8 devices in a mesh: data: 1 (over z), fsdp: 2 (over y), ep: 4 (over x, core).
Axes of the slice: x: 2, y: 2, z: 1, core: 2. Of those that a mesh axis runs over, the one named last changes fastest.
Arguments:
- tokens: bfloat16 [64, 512, 768], P(('data', 'fsdp', 'ep'))
- w_qkv: bfloat16 [768, 3, 12, 64], P('fsdp')
- w_out: bfloat16 [12, 64, 768], P(None, None, 'fsdp')
- w_gate: bfloat16 [8, 768, 3072], P('ep', 'fsdp')
- w_up: bfloat16 [8, 768, 3072], P('ep', 'fsdp')
- w_down: bfloat16 [8, 3072, 768], P('ep', None, 'fsdp')
- expert_idx: int32 [64, 512, 1], P(('data', 'fsdp', 'ep'))
- expert_slot: int32 [64, 512, 1], P(('data', 'fsdp', 'ep'))
- gate_wts: bfloat16 [64, 512, 1], P(('data', 'fsdp', 'ep'))
- d_out: bfloat16 [64, 512, 768], P(('data', 'fsdp', 'ep'))
Outputs:
- output 1: bfloat16 [64, 512, 768], P(('data', 'fsdp', 'ep'))
- output 2: bfloat16 [64, 512, 768], P(('data', 'fsdp', 'ep'))
- output 3: float32 [8, 768, 3072], P(('data', 'ep'), 'fsdp')
- output 4: float32 [8, 768, 3072], P(('data', 'ep'), 'fsdp')
- output 5: float32 [8, 3072, 768], P(('data', 'ep'), None, 'fsdp')
All inputs are finite; a program needn't handle non-finite values.
Results may differ from the reference program's by a relative error of at most 0.0149321.
Values are sent between devices in bfloat16 or wider.
A program may use at most 1 GiB of HBM per device.

```python
import jax
import jax.numpy as jnp
from jax import lax

SEQ_DEV = 8
SEQ_LEN = 512
D_MODEL = 768
D_FF = 3072
N_EXPERTS = 8
TOP_K = 1
N_HEADS = 12
HEAD_DIM = 64
FSDP_SIZE = 2
EP_SIZE = 4
CAPACITY = 640

GROUPS = FSDP_SIZE * EP_SIZE
TOK_DEV = SEQ_DEV * SEQ_LEN
N_BATCH = GROUPS * SEQ_DEV


def draw_routing(key):
    key_bias, key_hot, key_noise, key_order = jax.random.split(key, 4)
    n_assign = TOK_DEV * TOP_K
    expert_ids = jnp.arange(N_EXPERTS, dtype=jnp.int32)
    expert_bias = jax.random.randint(key_bias, (GROUPS, 1, N_EXPERTS), 0, 512, dtype=jnp.int32)
    hot_expert = jax.random.randint(key_hot, (GROUPS, 1, 1), 0, N_EXPERTS, dtype=jnp.int32)
    noise_int = jax.random.randint(key_noise, (GROUPS, TOK_DEV, N_EXPERTS), 0, 1024, dtype=jnp.int32)
    hot_bonus = jnp.where(expert_ids[None, None, :] == hot_expert, 2048, 0).astype(jnp.int32)
    scores = (noise_int + expert_bias + hot_bonus) * N_EXPERTS + expert_ids[None, None, :]
    chosen = lax.top_k(scores, TOP_K)[1].astype(jnp.int32)
    flat_ids = chosen.reshape(GROUPS, n_assign)
    priority = jax.vmap(lambda key_one: jax.random.permutation(key_one, n_assign))(jax.random.split(key_order, GROUPS)).astype(jnp.int32)
    sort_order = jnp.argsort(flat_ids * n_assign + priority, axis=1)
    sorted_ids = jnp.take_along_axis(flat_ids, sort_order, axis=1)
    counts = jax.vmap(lambda ids_one: jnp.bincount(ids_one, length=N_EXPERTS))(flat_ids).astype(jnp.int32)
    starts = jnp.cumsum(counts, axis=1) - counts
    rank_sorted = jnp.arange(n_assign, dtype=jnp.int32)[None, :] - jnp.take_along_axis(starts, sorted_ids, axis=1)
    slot_rank = jax.vmap(lambda order_one, rank_one: jnp.zeros((n_assign,), jnp.int32).at[order_one].set(rank_one))(sort_order, rank_sorted)
    slot_ids = jnp.where(slot_rank < CAPACITY, slot_rank, -1).astype(jnp.int32)
    return chosen.reshape(N_BATCH, SEQ_LEN, TOP_K), slot_ids.reshape(N_BATCH, SEQ_LEN, TOP_K)


def setup_inputs(seed: int = 0, part: int = 0) -> dict:
    part_key = jax.random.fold_in(jax.random.key(seed), part)
    key_tok, key_gate, key_dout, key_route = jax.random.split(part_key, 4)
    key_qkv, key_out, key_w1, key_w3, key_w2 = jax.random.split(jax.random.key(seed + 1), 5)
    tokens = jax.random.normal(key_tok, (N_BATCH, SEQ_LEN, D_MODEL), jnp.float32).astype(jnp.bfloat16)
    w_qkv = (jax.random.normal(key_qkv, (D_MODEL, 3, N_HEADS, HEAD_DIM), jnp.float32) * (1.5 * D_MODEL ** -0.5)).astype(jnp.bfloat16)
    w_out = (jax.random.normal(key_out, (N_HEADS, HEAD_DIM, D_MODEL), jnp.float32) * (N_HEADS * HEAD_DIM) ** -0.5).astype(jnp.bfloat16)
    w_gate = (jax.random.normal(key_w1, (N_EXPERTS, D_MODEL, D_FF), jnp.float32) * D_MODEL ** -0.5).astype(jnp.bfloat16)
    w_up = (jax.random.normal(key_w3, (N_EXPERTS, D_MODEL, D_FF), jnp.float32) * D_MODEL ** -0.5).astype(jnp.bfloat16)
    w_down = (jax.random.normal(key_w2, (N_EXPERTS, D_FF, D_MODEL), jnp.float32) * (1.5 * D_FF ** -0.5)).astype(jnp.bfloat16)
    expert_idx, expert_slot = draw_routing(key_route)
    gate_wts = jax.random.uniform(key_gate, (N_BATCH, SEQ_LEN, TOP_K), jnp.float32, 0.2, 1.0).astype(jnp.bfloat16)
    d_out = jax.random.normal(key_dout, (N_BATCH, SEQ_LEN, D_MODEL), jnp.float32).astype(jnp.bfloat16)
    return {'tokens': tokens, 'w_qkv': w_qkv, 'w_out': w_out, 'w_gate': w_gate, 'w_up': w_up, 'w_down': w_down, 'expert_idx': expert_idx, 'expert_slot': expert_slot, 'gate_wts': gate_wts, 'd_out': d_out}


def rms_norm(values):
    wide_vals = values.astype(jnp.float32)
    inv_rms = lax.rsqrt(jnp.mean(wide_vals * wide_vals, axis=-1, keepdims=True) + 1e-6)
    return (wide_vals * inv_rms).astype(jnp.bfloat16)


def attend_group(tok_grp, wqkv_f, wout_f):
    normed = rms_norm(tok_grp).astype(jnp.float32)
    qkv_all = jnp.einsum('bsd,dthe->bsthe', normed, wqkv_f).astype(jnp.bfloat16).astype(jnp.float32)
    scores = jnp.einsum('bqhe,bkhe->bhqk', qkv_all[:, :, 0], qkv_all[:, :, 1]) * (HEAD_DIM ** -0.5)
    causal = lax.broadcasted_iota(jnp.int32, (SEQ_LEN, SEQ_LEN), 0) >= lax.broadcasted_iota(jnp.int32, (SEQ_LEN, SEQ_LEN), 1)
    attn_probs = jax.nn.softmax(jnp.where(causal, scores, -1e30), axis=-1).astype(jnp.bfloat16).astype(jnp.float32)
    context = jnp.einsum('bhqk,bkhe->bqhe', attn_probs, qkv_all[:, :, 2]).astype(jnp.bfloat16).astype(jnp.float32)
    attn_proj = jnp.einsum('bqhe,hed->bqd', context, wout_f)
    return (tok_grp.astype(jnp.float32) + attn_proj).astype(jnp.bfloat16)


def moe_group(h_grp, idx_one, slot_one, gate_one, w1_f, w3_f, w2_f):
    n_assign = TOK_DEV * TOP_K
    h_tok = h_grp.reshape(TOK_DEV, D_MODEL)
    u_tok = rms_norm(h_tok)
    flat_slot = slot_one.reshape(n_assign)
    row_pos = jnp.where(flat_slot >= 0, idx_one.reshape(n_assign) * CAPACITY + flat_slot, N_EXPERTS * CAPACITY)
    src_assign = jnp.full((N_EXPERTS * CAPACITY,), n_assign, jnp.int32).at[row_pos].set(jnp.arange(n_assign, dtype=jnp.int32), mode='drop')
    disp_buf = jnp.take(u_tok, src_assign // TOP_K, axis=0, mode='fill', fill_value=0)
    disp_f = disp_buf.reshape(N_EXPERTS, CAPACITY, D_MODEL).astype(jnp.float32)
    act_a = jnp.einsum('ecd,edf->ecf', disp_f, w1_f)
    act_b = jnp.einsum('ecd,edf->ecf', disp_f, w3_f)
    gated_act = (jax.nn.silu(act_a) * act_b).astype(jnp.bfloat16).astype(jnp.float32)
    y_buf = jnp.einsum('ecf,efd->ecd', gated_act, w2_f).astype(jnp.bfloat16).reshape(N_EXPERTS * CAPACITY, D_MODEL)
    y_rows = jnp.take(y_buf, row_pos, axis=0, mode='fill', fill_value=0).reshape(TOK_DEV, TOP_K, D_MODEL)
    mixed_sum = jnp.sum(y_rows.astype(jnp.float32) * gate_one.reshape(TOK_DEV, TOP_K, 1).astype(jnp.float32), axis=1)
    return (h_tok.astype(jnp.float32) + mixed_sum).astype(jnp.bfloat16).reshape(SEQ_DEV, SEQ_LEN, D_MODEL)


def reference(tokens, w_qkv, w_out, w_gate, w_up, w_down, expert_idx, expert_slot, gate_wts, d_out):
    wqkv_f = w_qkv.astype(jnp.float32)
    wout_f = w_out.astype(jnp.float32)
    idx_grp = expert_idx.reshape(GROUPS, SEQ_DEV, SEQ_LEN, TOP_K)
    slot_grp = expert_slot.reshape(GROUPS, SEQ_DEV, SEQ_LEN, TOP_K)
    gate_grp = gate_wts.reshape(GROUPS, SEQ_DEV, SEQ_LEN, TOP_K)

    def forward(tok_in, w1_f, w3_f, w2_f):
        def one_group(args_grp):
            tok_grp, idx_one, slot_one, gate_one = args_grp
            h_grp = attend_group(tok_grp, wqkv_f, wout_f)
            return moe_group(h_grp, idx_one, slot_one, gate_one, w1_f, w3_f, w2_f)
        group_outs = lax.map(jax.checkpoint(one_group), (tok_in.reshape(GROUPS, SEQ_DEV, SEQ_LEN, D_MODEL), idx_grp, slot_grp, gate_grp))
        return group_outs.reshape(N_BATCH, SEQ_LEN, D_MODEL)

    layer_out, pullback = jax.vjp(forward, tokens, w_gate.astype(jnp.float32), w_up.astype(jnp.float32), w_down.astype(jnp.float32))
    d_tokens, dw_gate, dw_up, dw_down = pullback(d_out)
    return layer_out, d_tokens, dw_gate, dw_up, dw_down
```

```python
import functools

import jax
import jax.numpy as jnp
from jax import lax
from jax.experimental import pallas as pl
from jax.experimental.pallas import tpu as pltpu
from jax.sharding import PartitionSpec as P

F32 = jnp.float32
BF16 = jnp.bfloat16
TILE = 128
CHUNK_TILES = 5
CHUNK = TILE * CHUNK_TILES
PASS_TILES = 20
FF_STEP = 512
GROUP = ('fsdp', 'ep')
NN = (((1,), (0,)), ((), ()))
NT = (((1,), (1,)), ((), ()))
TN = (((0,), (0,)), ((), ()))


def mm(lhs, rhs, dims=NN):
    return lax.dot_general(lhs, rhs, dims, preferred_element_type=F32)


def params(limit_mib=60):
    return pltpu.CompilerParams(vmem_limit_bytes=limit_mib * 1024 * 1024)


ANY = pl.BlockSpec(memory_space=pl.ANY)
SMEM = pl.BlockSpec(memory_space=pltpu.SMEM)
VMEM = pl.BlockSpec(memory_space=pltpu.VMEM)


def rms_norm(values):
    wide_vals = values.astype(F32)
    inv_rms = lax.rsqrt(jnp.mean(wide_vals * wide_vals, axis=-1, keepdims=True) + 1e-6)
    return (wide_vals * inv_rms).astype(BF16)


def attention_block(tok_seq, w_qkv, w_out):
    seq_len = tok_seq.shape[1]
    head_dim = w_qkv.shape[3]
    normed = rms_norm(tok_seq)
    qkv_all = jnp.einsum('bsd,dthe->tbshe', normed, w_qkv, preferred_element_type=F32).astype(BF16)
    scores = jnp.einsum('bqhe,bkhe->bhqk', qkv_all[0], qkv_all[1], preferred_element_type=F32) * (head_dim ** -0.5)
    causal = lax.broadcasted_iota(jnp.int32, (seq_len, seq_len), 0) >= lax.broadcasted_iota(jnp.int32, (seq_len, seq_len), 1)
    attn_probs = jax.nn.softmax(jnp.where(causal, scores, -1e30), axis=-1).astype(BF16)
    context = jnp.einsum('bhqk,bkhe->bqhe', attn_probs, qkv_all[2], preferred_element_type=F32).astype(BF16)
    attn_proj = jnp.einsum('crif,ife->cre', context, w_out, preferred_element_type=F32)
    return (tok_seq.astype(F32) + attn_proj).astype(BF16)


def route_kernel(n_exp, idx_ref, slot_ref, pos_ref, cnt_ref):
    idx, kept = idx_ref[...], slot_ref[...] >= 0
    rows, lanes = idx.shape
    upper = (lax.broadcasted_iota(jnp.int32, (lanes, lanes), 0) <= lax.broadcasted_iota(jnp.int32, (lanes, lanes), 1)).astype(F32).astype(BF16)
    lower = (lax.broadcasted_iota(jnp.int32, (rows, rows), 1) < lax.broadcasted_iota(jnp.int32, (rows, rows), 0)).astype(F32).astype(BF16)
    ones = jnp.ones((lanes, lanes), BF16)
    lane = lax.broadcasted_iota(jnp.int32, (1, lanes), 1)
    pos = jnp.full((rows, lanes), -1.0, F32)
    cnt = jnp.zeros((1, lanes), F32)
    off = jnp.zeros((1, 1), F32)
    for e in range(n_exp):
        mask = jnp.logical_and(idx == e, kept)
        wide = jnp.where(mask, 1.0, 0.0)
        mask_b = wide.astype(BF16)
        inside = mm(mask_b, upper)
        before = mm(lower, mm(mask_b, ones).astype(BF16))
        count = jnp.sum(jnp.sum(wide, axis=1, keepdims=True), axis=0, keepdims=True)
        pos = jnp.where(mask, off + before + inside - 1.0, pos)
        cnt = jnp.where(lane == e, count, cnt)
        off = off + jnp.floor((count + (TILE - 1.0)) * (1.0 / TILE)) * TILE
    pos_ref[...] = pos.astype(jnp.int32)
    cnt_ref[...] = cnt.astype(jnp.int32)


def route(idx, slot, n_exp):
    n = idx.size
    shape = (n // 128, 128)
    return pl.pallas_call(
        functools.partial(route_kernel, n_exp),
        out_shape=(jax.ShapeDtypeStruct(shape, jnp.int32), jax.ShapeDtypeStruct((1, 128), jnp.int32)),
        in_specs=[VMEM, VMEM],
        out_specs=(VMEM, VMEM),
        name='route',
    )(idx.reshape(shape), slot.reshape(shape))


PACK_STEP = 1024


def pack_kernel(weighted, c_ref, pos_ref, gate_ref, x_ref, out_ref, acc_ref):
    k = pl.program_id(0)
    row = lax.broadcasted_iota(jnp.int32, (CHUNK, PACK_STEP), 0) + c_ref[0] * CHUNK
    hit = row == pos_ref[pl.ds(k, 1), :]
    value = gate_ref[pl.ds(k, 1), :] if weighted else 1.0
    part = mm(jnp.where(hit, value, 0.0).astype(BF16), x_ref[...])

    @pl.when(k == 0)
    def _():
        acc_ref[...] = part

    @pl.when(k > 0)
    def _():
        acc_ref[...] += part

    @pl.when(k == pl.num_programs(0) - 1)
    def _():
        out_ref[...] = acc_ref[...].astype(BF16)


def pack(chunk, pos, gate, x, weighted):
    n, width = x.shape
    steps = n // PACK_STEP
    return pl.pallas_call(
        functools.partial(pack_kernel, weighted),
        grid=(steps,),
        out_shape=jax.ShapeDtypeStruct((CHUNK, width), BF16),
        in_specs=[SMEM, pl.BlockSpec((steps, PACK_STEP), lambda k: (0, 0)), pl.BlockSpec((steps, PACK_STEP), lambda k: (0, 0)), pl.BlockSpec((PACK_STEP, width), lambda k: (k, 0))],
        out_specs=pl.BlockSpec((CHUNK, width), lambda k: (0, 0)),
        scratch_shapes=[pltpu.VMEM((CHUNK, width), F32)],
        compiler_params=params(),
        cost_estimate=pl.CostEstimate(flops=2 * CHUNK * n * width, bytes_accessed=2 * n * width, transcendentals=0),
        name='pack',
    )(chunk.reshape(1), pos.reshape(steps, PACK_STEP), gate, x)


UNPACK_STEP = 512


def unpack_kernel(weighted, n_ref, pos_ref, gate_ref, *refs):
    if weighted:
        h_ref, first_ref, more_ref, out_ref, buf, acc, sem = refs
    else:
        first_ref, more_ref, out_ref, buf, acc, sem = refs
    k = pl.program_id(0)
    pos = pos_ref[pl.ds(k, 1), :]
    row = lax.broadcasted_iota(jnp.int32, (CHUNK, UNPACK_STEP), 0)
    value = gate_ref[pl.ds(k, 1), :] if weighted else 1.0

    def gathered(base, rows):
        return mm(jnp.where(row + base == pos, value, 0.0).astype(BF16), rows, TN)

    acc[...] = gathered(0, first_ref[...])

    def more(c, carry):
        copy = pltpu.make_async_copy(more_ref.at[c - 1], buf, sem)
        copy.start()
        copy.wait()
        acc[...] += gathered(c * CHUNK, buf[...])
        return carry

    lax.fori_loop(1, n_ref[0], more, 0)
    total = acc[...]
    if weighted:
        total = h_ref[...].astype(F32) + total
    out_ref[...] = total.astype(BF16)


def unpack(n_chunks, pos, gate, h, first, more):
    weighted = h is not None
    n = pos.size
    width = first.shape[1]
    steps = n // UNPACK_STEP
    small = pl.BlockSpec((steps, UNPACK_STEP), lambda k: (0, 0))
    rows = pl.BlockSpec((UNPACK_STEP, width), lambda k: (k, 0))
    return pl.pallas_call(
        functools.partial(unpack_kernel, weighted),
        grid=(steps,),
        out_shape=jax.ShapeDtypeStruct((n, width), BF16),
        in_specs=[SMEM, small, small] + ([rows] if weighted else []) + [pl.BlockSpec((CHUNK, width), lambda k: (0, 0)), ANY],
        out_specs=rows,
        scratch_shapes=[pltpu.VMEM((CHUNK, width), BF16), pltpu.VMEM((UNPACK_STEP, width), F32), pltpu.SemaphoreType.DMA],
        compiler_params=params(),
        cost_estimate=pl.CostEstimate(flops=2 * CHUNK * n * width, bytes_accessed=4 * n * width, transcendentals=0),
        name='unpack',
    )(n_chunks.reshape(1), pos.reshape(steps, UNPACK_STEP), gate.reshape(steps, UNPACK_STEP), *([h] if weighted else []), first, more)


def experts_kernel(back, n_src, cnt_ref, prm_ref, u_hbm, dy_hbm, w1_hbm, w3_hbm, w2_hbm, r1_hbm, r3_hbm, r2_hbm, i1, i3, i2, *refs):
    if back:
        o1, o3, o2, y_hbm, du_hbm = refs[:5]
        scratch = refs[5:]
        y_acc, du_acc, stage, zero, row_sem = scratch[-5:]
        scratch = scratch[:-5]
    else:
        o1, o3, o2 = refs[:3]
        scratch = refs[3:]
    u_s, dy_s, ut_s, dyt_s, w1_s, w3_s, w2_s, d1_s, d3_s, d2_s, d2t_s, lst, load_sem, w_sem, d_sem = scratch
    expert, local, half, chunk, add_first = prm_ref[0], prm_ref[1], prm_ref[2], prm_ref[3], prm_ref[4]
    width = u_s.shape[1]
    hw = width // 2
    ff = w1_hbm.shape[2]
    n_ff = ff // FF_STEP
    first_tile = chunk * CHUNK_TILES
    own_rows = pl.ds(pl.multiple_of(half * hw, hw), hw)
    got_rows = pl.ds(pl.multiple_of((1 - half) * hw, hw), hw)

    if back:
        def unmark(t, carry):
            lst[1, t] = 0
            return carry

        lax.fori_loop(0, n_src * CHUNK_TILES, unmark, 0)
    total = jnp.int32(0)
    for s in range(n_src):
        off, own = jnp.int32(0), jnp.int32(0)
        for e in range(n_src):
            tiles = (cnt_ref[s, e] + (TILE - 1)) // TILE
            off = off + jnp.where(e < expert, tiles, 0)
            own = own + jnp.where(e == expert, tiles, 0)
        lo = jnp.clip(off - first_tile, 0, CHUNK_TILES)
        hi = jnp.clip(off + own - first_tile, 0, CHUNK_TILES)

        def note(j, t, s=s):
            lst[0, t] = s * CHUNK_TILES + j
            if back:
                lst[1, s * CHUNK_TILES + j] = 1
            return t + 1

        total = lax.fori_loop(lo, hi, note, total)

    def tile_of(ref, t):
        return ref.at[t // CHUNK_TILES, pl.ds(pl.multiple_of((t % CHUNK_TILES) * TILE, TILE), TILE), :]

    if back:
        zero[...] = jnp.zeros_like(zero)

        def clear(t, n):
            @pl.when(lst[1, t] == 0)
            def _():
                pltpu.make_async_copy(zero, tile_of(y_hbm, t), row_sem).start()
                pltpu.make_async_copy(zero, tile_of(du_hbm, t), row_sem).start()

            return n

        lax.fori_loop(0, n_src * CHUNK_TILES, clear, 0)

    def weights(f, slot):
        cols = pl.ds(pl.multiple_of(f * FF_STEP, FF_STEP), FF_STEP)
        pairs = [
            (w1_hbm.at[local, :, cols], w1_s.at[slot, own_rows, :]),
            (r1_hbm.at[:, cols], w1_s.at[slot, got_rows, :]),
            (w3_hbm.at[local, :, cols], w3_s.at[slot, own_rows, :]),
            (r3_hbm.at[:, cols], w3_s.at[slot, got_rows, :]),
            (w2_hbm.at[local, cols, :], w2_s.at[slot, :, own_rows]),
            (r2_hbm.at[cols, :], w2_s.at[slot, :, got_rows]),
        ]
        return [pltpu.make_async_copy(src, dst, w_sem.at[slot, i]) for i, (src, dst) in enumerate(pairs)]

    def grads(f, slot, ins):
        cols = pl.ds(pl.multiple_of(f * FF_STEP, FF_STEP), FF_STEP)
        hbm = (i1, i3, i2) if ins else (o1, o3, o2)
        pairs = [
            (hbm[0].at[local, :, cols], d1_s.at[slot]),
            (hbm[1].at[local, :, cols], d3_s.at[slot]),
            (hbm[2].at[local, cols, :], d2_s.at[slot]),
        ]
        if not ins:
            pairs = [(b, a) for a, b in pairs]
        return [pltpu.make_async_copy(src, dst, d_sem.at[slot, i]) for i, (src, dst) in enumerate(pairs)]

    def one_pass(p, carry):
        for cp in weights(0, 0):
            cp.start()
        n_tiles = jnp.clip(total - p * PASS_TILES, 0, PASS_TILES)
        n_blk = (n_tiles + (CHUNK_TILES - 1)) // CHUNK_TILES

        def rows_at(k):
            return pl.ds(pl.multiple_of(k * TILE, TILE), TILE)

        def load(k, carry):
            t = lst[0, p * PASS_TILES + k]
            pltpu.make_async_copy(tile_of(u_hbm, t), u_s.at[rows_at(k), :], load_sem).start()
            pltpu.make_async_copy(tile_of(dy_hbm, t), dy_s.at[rows_at(k), :], load_sem).start()
            return carry

        lax.fori_loop(0, n_tiles, load, 0)

        def fill(k, carry):
            u_s[rows_at(k), :] = jnp.zeros((TILE, width), BF16)
            dy_s[rows_at(k), :] = jnp.zeros((TILE, width), BF16)
            return carry

        lax.fori_loop(n_tiles, n_blk * CHUNK_TILES, fill, 0)

        def loaded(k, carry):
            pltpu.make_async_copy(tile_of(u_hbm, 0), u_s.at[rows_at(k), :], load_sem).wait()
            pltpu.make_async_copy(tile_of(dy_hbm, 0), dy_s.at[rows_at(k), :], load_sem).wait()
            return carry

        lax.fori_loop(0, n_tiles, loaded, 0)

        def flip(k, carry):
            ut_s[:, rows_at(k)] = u_s[rows_at(k), own_rows].T
            dyt_s[:, rows_at(k)] = dy_s[rows_at(k), own_rows].T
            return carry

        lax.fori_loop(0, n_blk * CHUNK_TILES, flip, 0)
        add = jnp.logical_or(p > 0, add_first > 0)

        def step(f, carry):
            slot = f % 2

            @pl.when(f + 1 < n_ff)
            def _():
                for cp in weights(f + 1, 1 - slot):
                    cp.start()

            @pl.when(f >= 2)
            def _():
                for cp in grads(f - 2, slot, False):
                    cp.wait()

            for cp in weights(f, slot):
                cp.wait()

            d1_s[slot] = jnp.zeros((hw, FF_STEP), F32)
            d3_s[slot] = jnp.zeros((hw, FF_STEP), F32)
            d2t_s[...] = jnp.zeros((hw, FF_STEP), F32)

            @pl.when(add)
            def _():
                for cp in grads(f, slot, True):
                    cp.start()
                for cp in grads(f, slot, True):
                    cp.wait()
                d2t_s[...] = d2_s[slot].T

            def block(b, carry):
                rows = pl.ds(pl.multiple_of(b * CHUNK, CHUNK), CHUNK)
                w1, w3, w2 = w1_s[slot], w3_s[slot], w2_s[slot]
                u, dy = u_s[rows, :], dy_s[rows, :]
                act_a = mm(u, w1)
                act_b = mm(u, w3)
                d_g = mm(dy, w2, NT)
                sig = 0.5 * jnp.tanh(0.5 * act_a) + 0.5
                silu = act_a * sig
                g = (silu * act_b).astype(BF16)
                d_b = (d_g * silu).astype(BF16)
                d_a = (d_g * act_b * (sig + silu * (1.0 - sig))).astype(BF16)
                if back:
                    y = mm(g, w2)
                    du = mm(d_a, w1, NT) + mm(d_b, w3, NT)

                    @pl.when(f == 0)
                    def _():
                        y_acc[rows, :] = y
                        du_acc[rows, :] = du

                    @pl.when(f > 0)
                    def _():
                        y_acc[rows, :] += y
                        du_acc[rows, :] += du

                d1_s[slot] += mm(ut_s[:, rows], d_a)
                d3_s[slot] += mm(ut_s[:, rows], d_b)
                d2t_s[...] += mm(dyt_s[:, rows], g)
                return carry

            lax.fori_loop(0, n_blk, block, 0)
            d2_s[slot] = d2t_s[...].T
            for cp in grads(f, slot, False):
                cp.start()
            return carry

        lax.fori_loop(0, n_ff, step, 0)
        if back:
            def put(k, carry):
                t = lst[0, p * PASS_TILES + k]
                stage[0, rows_at(k), :] = y_acc[rows_at(k), :].astype(BF16)
                stage[1, rows_at(k), :] = du_acc[rows_at(k), :].astype(BF16)
                pltpu.make_async_copy(stage.at[0, rows_at(k), :], tile_of(y_hbm, t), row_sem).start()
                pltpu.make_async_copy(stage.at[1, rows_at(k), :], tile_of(du_hbm, t), row_sem).start()
                return carry

            lax.fori_loop(0, n_tiles, put, 0)

            def done(k, carry):
                pltpu.make_async_copy(zero, tile_of(y_hbm, 0), row_sem).wait()
                pltpu.make_async_copy(zero, tile_of(du_hbm, 0), row_sem).wait()
                return carry

            lax.fori_loop(0, n_tiles, done, 0)
        for f in (n_ff - 2, n_ff - 1):
            for cp in grads(f, f % 2, False):
                cp.wait()
        return carry

    n_pass = jnp.maximum((total + (PASS_TILES - 1)) // PASS_TILES, 1)
    lax.fori_loop(0, n_pass, one_pass, 0)
    if back:
        def cleared(t, carry):
            pltpu.make_async_copy(zero, tile_of(y_hbm, 0), row_sem).wait()
            pltpu.make_async_copy(zero, tile_of(du_hbm, 0), row_sem).wait()
            return carry

        lax.fori_loop(0, n_src * CHUNK_TILES - total, cleared, 0)


def experts(back, counts, prm, u_all, dy_all, own, got, dws):
    n_src, _, width = u_all.shape
    hw = width // 2
    ff = own[0].shape[2]
    rows = PASS_TILES * TILE
    scratch = [
        pltpu.VMEM((rows, width), BF16),
        pltpu.VMEM((rows, width), BF16),
        pltpu.VMEM((hw, rows), BF16),
        pltpu.VMEM((hw, rows), BF16),
        pltpu.VMEM((2, width, FF_STEP), BF16),
        pltpu.VMEM((2, width, FF_STEP), BF16),
        pltpu.VMEM((2, FF_STEP, width), BF16),
        pltpu.VMEM((2, hw, FF_STEP), F32),
        pltpu.VMEM((2, hw, FF_STEP), F32),
        pltpu.VMEM((2, FF_STEP, hw), F32),
        pltpu.VMEM((hw, FF_STEP), F32),
        pltpu.SMEM((2, n_src * CHUNK_TILES), jnp.int32),
        pltpu.SemaphoreType.DMA,
        pltpu.SemaphoreType.DMA((2, 6)),
        pltpu.SemaphoreType.DMA((2, 3)),
    ]
    outs = [jax.ShapeDtypeStruct(d.shape, d.dtype) for d in dws]
    if back:
        outs += [jax.ShapeDtypeStruct(u_all.shape, BF16)] * 2
        scratch += [
            pltpu.VMEM((rows, width), F32),
            pltpu.VMEM((rows, width), F32),
            pltpu.VMEM((2, rows, width), BF16),
            pltpu.VMEM((TILE, width), BF16),
            pltpu.SemaphoreType.DMA,
        ]
    units = 7.5 if back else 4.5
    return pl.pallas_call(
        functools.partial(experts_kernel, back, n_src),
        out_shape=tuple(outs),
        in_specs=[SMEM, SMEM] + [ANY] * 11,
        out_specs=tuple([ANY] * len(outs)),
        scratch_shapes=scratch,
        input_output_aliases={10: 0, 11: 1, 12: 2},
        compiler_params=params(),
        cost_estimate=pl.CostEstimate(flops=int(units * 2 * 2 * CHUNK * width * ff), bytes_accessed=30 * 2**20, transcendentals=0),
        name='experts_back' if back else 'experts_grad',
    )(counts, prm, u_all, dy_all, *own, *got, *dws)


def unset_kernel(*refs):
    pass


def unset(*shapes):
    outs = tuple(jax.ShapeDtypeStruct(s, d) for s, d in shapes)
    return pl.pallas_call(unset_kernel, out_shape=outs, out_specs=tuple([ANY] * len(outs)), name='unset')()


def solution(mesh):
    n_dev = mesh.shape['fsdp'] * mesh.shape['ep']
    tok_spec = P(('data', 'fsdp', 'ep'))
    in_specs = (tok_spec, P('fsdp'), P(None, None, 'fsdp'), P('ep', 'fsdp'), P('ep', 'fsdp'), P('ep', None, 'fsdp'), tok_spec, tok_spec, tok_spec, tok_spec)
    out_specs = (tok_spec, tok_spec, P(('data', 'ep'), 'fsdp'), P(('data', 'ep'), 'fsdp'), P(('data', 'ep'), None, 'fsdp'))

    def device_fn(tokens, w_qkv, w_out, w_gate, w_up, w_down, expert_idx, expert_slot, gate_wts, d_out):
        n_seq, seq_len, d_model = tokens.shape
        n_tok = n_seq * seq_len
        n_exp = n_dev
        half = lax.axis_index('fsdp').astype(jnp.int32)
        col = lax.axis_index('ep').astype(jnp.int32)
        swap = [(0, 1), (1, 0)]
        own = (w_gate, w_up, w_down)

        def other(local):
            return [lax.ppermute(lax.dynamic_index_in_dim(w, local, 0, keepdims=False), 'fsdp', swap) for w in own]

        qkv_full = lax.all_gather(w_qkv, 'fsdp', axis=0, tiled=True)
        out_full = lax.all_gather(w_out, 'fsdp', axis=2, tiled=True)
        pos, cnt = route(expert_idx, expert_slot, n_exp)
        counts = lax.all_gather(cnt[0], GROUP)
        got_mine = other(1 - half)
        gate = gate_wts.reshape(n_tok // PACK_STEP, PACK_STEP).astype(F32)
        dout_tok = d_out.reshape(n_tok, d_model)
        zero = jnp.int32(0)
        dy_all = lax.all_gather(pack(zero, pos, gate, dout_tok, True), GROUP)
        got_rest = other(half)

        h_seq, attn_pullback = jax.vjp(lambda tok_in: attention_block(tok_in, qkv_full, out_full), tokens)
        h_tok = h_seq.reshape(n_tok, d_model)
        u_tok, norm_pullback = jax.vjp(rms_norm, h_tok)
        u_all = lax.all_gather(pack(zero, pos, gate, u_tok, False), GROUP)

        tiles = (counts[:, :n_exp] + (TILE - 1)) // TILE
        n_chunks = jnp.max((jnp.sum(tiles, axis=1) + (CHUNK_TILES - 1)) // CHUNK_TILES)
        max_more = (n_tok + n_exp * (TILE - 1)) // CHUNK

        def prm(local, chunk, add):
            return jnp.stack([2 * col + local, local, half, chunk, add]).astype(jnp.int32)

        dws = unset(*[(w.shape, F32) for w in own])
        more_y, more_du = unset(*[((max_more, CHUNK, d_model), BF16)] * 2)
        *dws, y_all, du_all = experts(True, counts, prm(half, zero, zero), u_all, dy_all, own, got_mine, dws)
        first_du = lax.psum_scatter(du_all, GROUP, scatter_dimension=0)
        first_y = lax.psum_scatter(y_all, GROUP, scatter_dimension=0)

        def fetch(c):
            return lax.all_gather(pack(c, pos, gate, u_tok, False), GROUP), lax.all_gather(pack(c, pos, gate, dout_tok, True), GROUP)

        def more_back(state):
            c, d1, d3, d2, ys, dus = state
            u_c, dy_c = fetch(c)
            d1, d3, d2, y_c, du_c = experts(True, counts, prm(half, c, jnp.int32(1)), u_c, dy_c, own, got_mine, (d1, d3, d2))
            y_c = lax.psum_scatter(y_c, GROUP, scatter_dimension=0)
            du_c = lax.psum_scatter(du_c, GROUP, scatter_dimension=0)
            ys = lax.dynamic_update_index_in_dim(ys, y_c, c - 1, 0)
            dus = lax.dynamic_update_index_in_dim(dus, du_c, c - 1, 0)
            return c + 1, d1, d3, d2, ys, dus

        def more_grad(state):
            c, d1, d3, d2 = state
            u_c, dy_c = fetch(c)
            d1, d3, d2 = experts(False, counts, prm(1 - half, c, jnp.int32(1)), u_c, dy_c, own, got_rest, (d1, d3, d2))
            return c + 1, d1, d3, d2

        _, *dws, more_y, more_du = lax.while_loop(lambda s: s[0] < n_chunks, more_back, (jnp.int32(1), *dws, more_y, more_du))
        layer_out = unpack(n_chunks, pos, gate, h_tok, first_y, more_y).reshape(n_seq, seq_len, d_model)
        d_u = unpack(n_chunks, pos, gate, None, first_du, more_du)
        d_h_norm = norm_pullback(d_u)[0]
        d_h = (dout_tok.astype(F32) + d_h_norm.astype(F32)).astype(BF16).reshape(n_seq, seq_len, d_model)
        d_tokens = attn_pullback(d_h)[0]

        dws = experts(False, counts, prm(1 - half, zero, zero), u_all, dy_all, own, got_rest, dws)
        _, *dws = lax.while_loop(lambda s: s[0] < n_chunks, more_grad, (jnp.int32(1), *dws))
        return layer_out, d_tokens, *dws

    return jax.shard_map(device_fn, mesh=mesh, in_specs=in_specs, out_specs=out_specs, check_vma=False)
```

```python
import functools

import jax
import jax.numpy as jnp
from jax import lax
from jax.experimental import pallas as pl
from jax.experimental.pallas import tpu as pltpu
from jax.sharding import PartitionSpec as P


F32 = jnp.float32
BF16 = jnp.bfloat16
TILE = 128
CHUNK_TILES = 5
CHUNK = TILE * CHUNK_TILES
PASS_TILES = 20
FF_STEP = 512
GROUP = ('fsdp', 'ep')
NN = (((1,), (0,)), ((), ()))
NT = (((1,), (1,)), ((), ()))
TN = (((0,), (0,)), ((), ()))


def mm(lhs, rhs, dims=NN):
    return lax.dot_general(lhs, rhs, dims, preferred_element_type=F32)


def params(limit_mib=60):
    return pltpu.CompilerParams(vmem_limit_bytes=limit_mib * 1024 * 1024)


ANY = pl.BlockSpec(memory_space=pl.ANY)
SMEM = pl.BlockSpec(memory_space=pltpu.SMEM)
VMEM = pl.BlockSpec(memory_space=pltpu.VMEM)


def route_kernel(n_exp, idx_ref, slot_ref, pos_ref, cnt_ref):
    idx, kept = idx_ref[...], slot_ref[...] >= 0
    rows, lanes = idx.shape
    upper = (lax.broadcasted_iota(jnp.int32, (lanes, lanes), 0) <= lax.broadcasted_iota(jnp.int32, (lanes, lanes), 1)).astype(F32).astype(BF16)
    lower = (lax.broadcasted_iota(jnp.int32, (rows, rows), 1) < lax.broadcasted_iota(jnp.int32, (rows, rows), 0)).astype(F32).astype(BF16)
    ones = jnp.ones((lanes, lanes), BF16)
    lane = lax.broadcasted_iota(jnp.int32, (1, lanes), 1)
    pos = jnp.full((rows, lanes), -1.0, F32)
    cnt = jnp.zeros((1, lanes), F32)
    off = jnp.zeros((1, 1), F32)
    for e in range(n_exp):
        mask = jnp.logical_and(idx == e, kept)
        wide = jnp.where(mask, 1.0, 0.0)
        mask_b = wide.astype(BF16)
        inside = mm(mask_b, upper)
        before = mm(lower, mm(mask_b, ones).astype(BF16))
        count = jnp.sum(jnp.sum(wide, axis=1, keepdims=True), axis=0, keepdims=True)
        pos = jnp.where(mask, off + before + inside - 1.0, pos)
        cnt = jnp.where(lane == e, count, cnt)
        off = off + jnp.floor((count + (TILE - 1.0)) * (1.0 / TILE)) * TILE
    pos_ref[...] = pos.astype(jnp.int32)
    cnt_ref[...] = cnt.astype(jnp.int32)


def route(idx, slot, n_exp):
    n = idx.size
    shape = (n // 128, 128)
    return pl.pallas_call(
        functools.partial(route_kernel, n_exp),
        out_shape=(jax.ShapeDtypeStruct(shape, jnp.int32), jax.ShapeDtypeStruct((1, 128), jnp.int32)),
        in_specs=[VMEM, VMEM],
        out_specs=(VMEM, VMEM),
        name='route',
    )(idx.reshape(shape), slot.reshape(shape))


PACK_STEP = 1024


def pack_kernel(weighted, c_ref, cnt_ref, pos_ref, gate_ref, x_ref, out_ref, acc_ref):
    k = pl.program_id(0)
    row = lax.broadcasted_iota(jnp.int32, (CHUNK, PACK_STEP), 0) + c_ref[0] * CHUNK
    hit = row == pos_ref[pl.ds(k, 1), :]
    value = gate_ref[pl.ds(k, 1), :] if weighted else 1.0
    part = mm(jnp.where(hit, value, 0.0).astype(BF16), x_ref[...])

    @pl.when(k == 0)
    def _():
        acc_ref[...] = part

    @pl.when(k > 0)
    def _():
        acc_ref[...] += part

    @pl.when(k == pl.num_programs(0) - 1)
    def _():
        out_ref[...] = acc_ref[...].astype(BF16)


def pack(chunk, counts, pos, gate, x, weighted):
    n, width = x.shape
    steps = n // PACK_STEP
    return pl.pallas_call(
        functools.partial(pack_kernel, weighted),
        grid=(steps,),
        out_shape=jax.ShapeDtypeStruct((CHUNK, width), BF16),
        in_specs=[SMEM, ANY, pl.BlockSpec((steps, PACK_STEP), lambda k: (0, 0)), pl.BlockSpec((steps, PACK_STEP), lambda k: (0, 0)), pl.BlockSpec((PACK_STEP, width), lambda k: (k, 0))],
        out_specs=pl.BlockSpec((CHUNK, width), lambda k: (0, 0)),
        scratch_shapes=[pltpu.VMEM((CHUNK, width), F32)],
        compiler_params=params(),
        cost_estimate=pl.CostEstimate(flops=2 * CHUNK * n * width, bytes_accessed=2 * n * width, transcendentals=0),
        name='pack',
    )(chunk.reshape(1), counts, pos.reshape(steps, PACK_STEP), gate, x)


UNPACK_STEP = 512


def unpack_kernel(weighted, n_ref, pos_ref, gate_ref, *refs):
    if weighted:
        h_ref, first_ref, more_ref, out_ref, buf, acc, sem = refs
    else:
        first_ref, more_ref, out_ref, buf, acc, sem = refs
    k = pl.program_id(0)
    pos = pos_ref[pl.ds(k, 1), :]
    row = lax.broadcasted_iota(jnp.int32, (CHUNK, UNPACK_STEP), 0)
    value = gate_ref[pl.ds(k, 1), :] if weighted else 1.0

    def gathered(base, rows):
        return mm(jnp.where(row + base == pos, value, 0.0).astype(BF16), rows, TN)

    acc[...] = gathered(0, first_ref[...])

    def more(c, carry):
        copy = pltpu.make_async_copy(more_ref.at[c - 1], buf, sem)
        copy.start()
        copy.wait()
        acc[...] += gathered(c * CHUNK, buf[...])
        return carry

    lax.fori_loop(1, n_ref[0], more, 0)
    total = acc[...]
    if weighted:
        total = h_ref[...].astype(F32) + total
    out_ref[...] = total.astype(BF16)


def unpack(n_chunks, pos, gate, h, first, more):
    weighted = h is not None
    n = pos.size
    width = first.shape[1]
    steps = n // UNPACK_STEP
    small = pl.BlockSpec((steps, UNPACK_STEP), lambda k: (0, 0))
    rows = pl.BlockSpec((UNPACK_STEP, width), lambda k: (k, 0))
    return pl.pallas_call(
        functools.partial(unpack_kernel, weighted),
        grid=(steps,),
        out_shape=jax.ShapeDtypeStruct((n, width), BF16),
        in_specs=[SMEM, small, small] + ([rows] if weighted else []) + [pl.BlockSpec((CHUNK, width), lambda k: (0, 0)), ANY],
        out_specs=rows,
        scratch_shapes=[pltpu.VMEM((CHUNK, width), BF16), pltpu.VMEM((UNPACK_STEP, width), F32), pltpu.SemaphoreType.DMA],
        compiler_params=params(),
        cost_estimate=pl.CostEstimate(flops=2 * CHUNK * n * width, bytes_accessed=4 * n * width, transcendentals=0),
        name='unpack',
    )(n_chunks.reshape(1), pos.reshape(steps, UNPACK_STEP), gate.reshape(steps, UNPACK_STEP), *([h] if weighted else []), first, more)


QUERY_BLOCK = 256


def load_attention_weights(w_hbm, wqkv, wo, sem):
    n_dev, rows, _ = w_hbm.shape
    wide, hw = wqkv.shape[1], wo.shape[2]
    n_col = n_dev // 2
    copies = []
    for i in range(n_dev):
        copies.append(pltpu.make_async_copy(w_hbm.at[i, :, pl.ds(0, wide)], wqkv.at[pl.ds(i * rows, rows), :], sem))
        for j in range(2):
            dst = wo.at[i // n_col, pl.ds((i % n_col * 2 + j) * rows, rows), :]
            copies.append(pltpu.make_async_copy(w_hbm.at[i, :, pl.ds(wide + j * hw, hw)], dst, sem))
    for cp in copies:
        cp.start()
    for cp in copies:
        cp.wait()


def inv_rms_of(wide_vals):
    return lax.rsqrt(jnp.mean(wide_vals * wide_vals, axis=-1, keepdims=True) + 1e-6)


def head_lanes(shape, axis, head):
    lane = lax.broadcasted_iota(jnp.int32, shape, axis)
    return lane < 64 if head == 0 else lane >= 64


def causal_tail(values, fill):
    n, k = values.shape
    tail = values[:, k - n :]
    keep = lax.broadcasted_iota(jnp.int32, (n, n), 0) >= lax.broadcasted_iota(jnp.int32, (n, n), 1)
    tail = jnp.where(keep, tail, fill)
    return tail if k == n else jnp.concatenate([values[:, : k - n], tail], axis=1)


def attn_fwd_kernel(pos_ref, w_hbm, x_ref, h_ref, u_ref, qkv_ref, ctx_ref, lse_ref, pack_ref, wqkv, wo, acc, sem):
    i = pl.program_id(0)
    width = x_ref.shape[1]
    hw = width // 2
    seq = x_ref.shape[0]

    @pl.when(i == 0)
    def _():
        load_attention_weights(w_hbm, wqkv, wo, sem)

    x = x_ref[...].astype(F32)
    normed = (x * inv_rms_of(x)).astype(BF16)
    for t in range(3):
        cols = slice(t * width, (t + 1) * width)
        qkv_ref[:, cols] = mm(normed, wqkv[:, cols]).astype(BF16)
    for pair in range(width // 128):
        lanes = slice(pair * 128, (pair + 1) * 128)
        q = qkv_ref[:, lanes] * jnp.asarray(0.125, BF16)
        k = qkv_ref[:, width + pair * 128 : width + (pair + 1) * 128]
        v = qkv_ref[:, 2 * width + pair * 128 : 2 * width + (pair + 1) * 128]
        for j in range(seq // QUERY_BLOCK):
            rows = slice(j * QUERY_BLOCK, (j + 1) * QUERY_BLOCK)
            keys = slice(0, (j + 1) * QUERY_BLOCK)
            outs = []
            for head in range(2):
                qm = jnp.where(head_lanes((QUERY_BLOCK, 128), 1, head), q[rows], jnp.zeros((), BF16))
                s = causal_tail(mm(qm, k[keys], NT), -1e30)
                top = jnp.max(s, axis=1, keepdims=True)
                e = jnp.exp(s - top)
                total = jnp.sum(e, axis=1, keepdims=True)
                outs.append(mm((e * (1.0 / total)).astype(BF16), v[keys]))
                lse_ref[rows, pair * 2 + head : pair * 2 + head + 1] = top + jnp.log(total)
            ctx_ref[rows, lanes] = jnp.where(head_lanes((QUERY_BLOCK, 128), 1, 0), outs[0], outs[1]).astype(BF16)
    ctx = ctx_ref[...]
    for f in range(2):
        cols = slice(f * hw, (f + 1) * hw)
        h_ref[:, cols] = (x_ref[:, cols].astype(F32) + mm(ctx, wo[f])).astype(BF16)
    h = h_ref[...].astype(F32)
    u = (h * inv_rms_of(h)).astype(BF16)
    u_ref[...] = u
    hit = lax.broadcasted_iota(jnp.int32, (CHUNK, seq), 0) == pos_ref[pl.ds(i, 1), :]
    part = mm(jnp.where(hit, 1.0, 0.0).astype(BF16), u)

    @pl.when(i == 0)
    def _():
        acc[...] = part

    @pl.when(i > 0)
    def _():
        acc[...] += part

    @pl.when(i == pl.num_programs(0) - 1)
    def _():
        pack_ref[...] = acc[...].astype(BF16)


def attn_fwd(pos, w_all, x, n_seq):
    n, width = x.shape
    seq = n // n_seq
    rows = pl.BlockSpec((seq, width), lambda i: (i, 0))
    return pl.pallas_call(
        attn_fwd_kernel,
        grid=(n_seq,),
        out_shape=(
            jax.ShapeDtypeStruct((n, width), BF16),
            jax.ShapeDtypeStruct((n, width), BF16),
            jax.ShapeDtypeStruct((n, 3 * width), BF16),
            jax.ShapeDtypeStruct((n, width), BF16),
            jax.ShapeDtypeStruct((n, 128), F32),
            jax.ShapeDtypeStruct((CHUNK, width), BF16),
        ),
        in_specs=[pl.BlockSpec((n_seq, seq), lambda i: (0, 0)), ANY, rows],
        out_specs=(rows, rows, pl.BlockSpec((seq, 3 * width), lambda i: (i, 0)), rows, pl.BlockSpec((seq, 128), lambda i: (i, 0)), pl.BlockSpec((CHUNK, width), lambda i: (0, 0))),
        scratch_shapes=[pltpu.VMEM((width, 3 * width), BF16), pltpu.VMEM((2, width, width // 2), BF16), pltpu.VMEM((CHUNK, width), F32), pltpu.SemaphoreType.DMA],
        compiler_params=params(),
        cost_estimate=pl.CostEstimate(flops=30 * 10**9, bytes_accessed=50 * 2**20, transcendentals=0),
        name='attn_fwd',
    )(pos.reshape(n_seq, seq), w_all, x)


def norm_back(grad, wide_vals):
    inv = inv_rms_of(wide_vals)
    return inv * (grad - wide_vals * (inv * inv * jnp.mean(grad * wide_vals, axis=-1, keepdims=True)))


def attn_bwd_kernel(n_ref, pos_ref, first_ref, more_hbm, w_hbm, x_ref, h_ref, dout_ref, qkv_ref, ctx_ref, lse_ref, dx_ref, wqkv, wo, dqkv, dctx, dh, buf, sem):
    i = pl.program_id(0)
    seq, width = x_ref.shape
    hw = width // 2

    @pl.when(i == 0)
    def _():
        load_attention_weights(w_hbm, wqkv, wo, sem)

    pos = pos_ref[pl.ds(i, 1), :]
    row = lax.broadcasted_iota(jnp.int32, (CHUNK, seq), 0)

    def gathered(base, rows):
        return mm(jnp.where(row + base == pos, 1.0, 0.0).astype(BF16), rows, TN)

    dh[...] = gathered(0, first_ref[...])

    def more(c, carry):
        copy = pltpu.make_async_copy(more_hbm.at[c - 1], buf, sem)
        copy.start()
        copy.wait()
        dh[...] += gathered(c * CHUNK, buf[...])
        return carry

    lax.fori_loop(1, n_ref[0], more, 0)
    dh[...] = dout_ref[...].astype(F32) + norm_back(dh[...], h_ref[...].astype(F32))
    dh_b = dh[...].astype(BF16)
    dctx[...] = (mm(dh_b[:, :hw], wo[0], NT) + mm(dh_b[:, hw:], wo[1], NT)).astype(BF16)
    zero = jnp.zeros((), BF16)
    for pair in range(width // 128):
        lanes = slice(pair * 128, (pair + 1) * 128)
        k_lanes = slice(width + pair * 128, width + (pair + 1) * 128)
        v_lanes = slice(2 * width + pair * 128, 2 * width + (pair + 1) * 128)
        q = qkv_ref[:, lanes] * jnp.asarray(0.125, BF16)
        k, v = qkv_ref[:, k_lanes], qkv_ref[:, v_lanes]
        do = dctx[:, lanes]
        q_t, do_t = q.T, do.T
        prod = do.astype(F32) * ctx_ref[:, lanes].astype(F32)
        dk_t = [jnp.zeros((128, QUERY_BLOCK), F32) for _ in range(seq // QUERY_BLOCK)]
        dv_t = list(dk_t)
        for j in range(seq // QUERY_BLOCK):
            rows = slice(j * QUERY_BLOCK, (j + 1) * QUERY_BLOCK)
            keys = slice(0, (j + 1) * QUERY_BLOCK)
            dqs = []
            for head in range(2):
                mine = head_lanes((QUERY_BLOCK, 128), 1, head)
                mine_t = head_lanes((128, QUERY_BLOCK), 0, head)
                qm, dom = jnp.where(mine, q[rows], zero), jnp.where(mine, do[rows], zero)
                delta = jnp.sum(jnp.where(mine, prod[rows], 0.0), axis=1, keepdims=True)
                lse = lse_ref[rows, pair * 2 + head : pair * 2 + head + 1]
                p = jnp.exp(causal_tail(mm(qm, k[keys], NT) - lse, -1e30))
                dp = mm(dom, v[keys], NT)
                ds = (p * (dp - delta)).astype(BF16)
                pb = p.astype(BF16)
                dqs.append(mm(ds, k[keys]))
                qm_t, dom_t = jnp.where(mine_t, q_t[:, rows], zero), jnp.where(mine_t, do_t[:, rows], zero)
                dk_part, dv_part = mm(qm_t, ds), mm(dom_t, pb)
                for c in range(j + 1):
                    cols = slice(c * QUERY_BLOCK, (c + 1) * QUERY_BLOCK)
                    dk_t[c] = dk_t[c] + dk_part[:, cols]
                    dv_t[c] = dv_t[c] + dv_part[:, cols]
            dqkv[rows, lanes] = (jnp.where(head_lanes((QUERY_BLOCK, 128), 1, 0), dqs[0], dqs[1]) * 0.125).astype(BF16)
        for c in range(seq // QUERY_BLOCK):
            rows = slice(c * QUERY_BLOCK, (c + 1) * QUERY_BLOCK)
            dqkv[rows, k_lanes] = dk_t[c].astype(BF16).T
            dqkv[rows, v_lanes] = dv_t[c].astype(BF16).T
    dn = mm(dqkv[...], wqkv[...], NT)
    dx_ref[...] = (dh[...] + norm_back(dn, x_ref[...].astype(F32))).astype(BF16)


def attn_bwd(n_chunks, pos, first, more, w_all, x, h, dout, qkv, ctx, lse, n_seq):
    n, width = x.shape
    seq = n // n_seq
    rows = pl.BlockSpec((seq, width), lambda i: (i, 0))
    return pl.pallas_call(
        attn_bwd_kernel,
        grid=(n_seq,),
        out_shape=jax.ShapeDtypeStruct((n, width), BF16),
        in_specs=[SMEM, pl.BlockSpec((n_seq, seq), lambda i: (0, 0)), pl.BlockSpec((CHUNK, width), lambda i: (0, 0)), ANY, ANY, rows, rows, rows, pl.BlockSpec((seq, 3 * width), lambda i: (i, 0)), rows, pl.BlockSpec((seq, 128), lambda i: (i, 0))],
        out_specs=rows,
        scratch_shapes=[
            pltpu.VMEM((width, 3 * width), BF16),
            pltpu.VMEM((2, width, width // 2), BF16),
            pltpu.VMEM((seq, 3 * width), BF16),
            pltpu.VMEM((seq, width), BF16),
            pltpu.VMEM((seq, width), F32),
            pltpu.VMEM((CHUNK, width), BF16),
            pltpu.SemaphoreType.DMA,
        ],
        compiler_params=params(),
        cost_estimate=pl.CostEstimate(flops=50 * 10**9, bytes_accessed=60 * 2**20, transcendentals=0),
        name='attn_bwd',
    )(n_chunks.reshape(1), pos.reshape(n_seq, seq), first, more, w_all, x, h, dout, qkv, ctx, lse)


def experts_kernel(back, n_src, cnt_ref, prm_ref, u_hbm, dy_hbm, w1_hbm, w3_hbm, w2_hbm, r1_hbm, r3_hbm, r2_hbm, i1, i3, i2, *refs):
    if back:
        o1, o3, o2, y_hbm, du_hbm = refs[:5]
        scratch = refs[5:]
        y_acc, du_acc, stage, zero, row_sem = scratch[-5:]
        scratch = scratch[:-5]
    else:
        o1, o3, o2 = refs[:3]
        scratch = refs[3:]
    u_s, dy_s, ut_s, dyt_s, w1_s, w3_s, w2_s, d1_s, d3_s, d2_s, d2t_s, lst, load_sem, w_sem, d_sem = scratch
    expert, local, half, chunk, add_first = prm_ref[0], prm_ref[1], prm_ref[2], prm_ref[3], prm_ref[4]
    width = u_s.shape[1]
    hw = width // 2
    ff = w1_hbm.shape[2]
    n_ff = ff // FF_STEP
    first_tile = chunk * CHUNK_TILES
    own_rows = pl.ds(pl.multiple_of(half * hw, hw), hw)
    got_rows = pl.ds(pl.multiple_of((1 - half) * hw, hw), hw)

    if back:
        def unmark(t, carry):
            lst[1, t] = 0
            return carry

        lax.fori_loop(0, n_src * CHUNK_TILES, unmark, 0)
    total = jnp.int32(0)
    for s in range(n_src):
        off, own = jnp.int32(0), jnp.int32(0)
        for e in range(n_src):
            tiles = (cnt_ref[s, e] + (TILE - 1)) // TILE
            off = off + jnp.where(e < expert, tiles, 0)
            own = own + jnp.where(e == expert, tiles, 0)
        lo = jnp.clip(off - first_tile, 0, CHUNK_TILES)
        hi = jnp.clip(off + own - first_tile, 0, CHUNK_TILES)

        def note(j, t, s=s):
            lst[0, t] = s * CHUNK_TILES + j
            if back:
                lst[1, s * CHUNK_TILES + j] = 1
            return t + 1

        total = lax.fori_loop(lo, hi, note, total)

    def tile_of(ref, t):
        return ref.at[t // CHUNK_TILES, pl.ds(pl.multiple_of((t % CHUNK_TILES) * TILE, TILE), TILE), :]

    if back:
        zero[...] = jnp.zeros_like(zero)

        def clear(t, n):
            @pl.when(lst[1, t] == 0)
            def _():
                pltpu.make_async_copy(zero, tile_of(y_hbm, t), row_sem).start()
                pltpu.make_async_copy(zero, tile_of(du_hbm, t), row_sem).start()

            return n

        lax.fori_loop(0, n_src * CHUNK_TILES, clear, 0)

    def weights(f, slot):
        cols = pl.ds(pl.multiple_of(f * FF_STEP, FF_STEP), FF_STEP)
        pairs = [
            (w1_hbm.at[local, :, cols], w1_s.at[slot, own_rows, :]),
            (r1_hbm.at[:, cols], w1_s.at[slot, got_rows, :]),
            (w3_hbm.at[local, :, cols], w3_s.at[slot, own_rows, :]),
            (r3_hbm.at[:, cols], w3_s.at[slot, got_rows, :]),
            (w2_hbm.at[local, cols, :], w2_s.at[slot, :, own_rows]),
            (r2_hbm.at[cols, :], w2_s.at[slot, :, got_rows]),
        ]
        return [pltpu.make_async_copy(src, dst, w_sem.at[slot, i]) for i, (src, dst) in enumerate(pairs)]

    def grads(f, slot, ins):
        cols = pl.ds(pl.multiple_of(f * FF_STEP, FF_STEP), FF_STEP)
        hbm = (i1, i3, i2) if ins else (o1, o3, o2)
        pairs = [
            (hbm[0].at[local, :, cols], d1_s.at[slot]),
            (hbm[1].at[local, :, cols], d3_s.at[slot]),
            (hbm[2].at[local, cols, :], d2_s.at[slot]),
        ]
        if not ins:
            pairs = [(b, a) for a, b in pairs]
        return [pltpu.make_async_copy(src, dst, d_sem.at[slot, i]) for i, (src, dst) in enumerate(pairs)]

    def one_pass(p, carry):
        for cp in weights(0, 0):
            cp.start()
        n_tiles = jnp.clip(total - p * PASS_TILES, 0, PASS_TILES)
        n_blk = (n_tiles + (CHUNK_TILES - 1)) // CHUNK_TILES

        def rows_at(k):
            return pl.ds(pl.multiple_of(k * TILE, TILE), TILE)

        def load(k, carry):
            t = lst[0, p * PASS_TILES + k]
            pltpu.make_async_copy(tile_of(u_hbm, t), u_s.at[rows_at(k), :], load_sem).start()
            pltpu.make_async_copy(tile_of(dy_hbm, t), dy_s.at[rows_at(k), :], load_sem).start()
            return carry

        lax.fori_loop(0, n_tiles, load, 0)

        def fill(k, carry):
            u_s[rows_at(k), :] = jnp.zeros((TILE, width), BF16)
            dy_s[rows_at(k), :] = jnp.zeros((TILE, width), BF16)
            return carry

        lax.fori_loop(n_tiles, n_blk * CHUNK_TILES, fill, 0)

        def loaded(k, carry):
            pltpu.make_async_copy(tile_of(u_hbm, 0), u_s.at[rows_at(k), :], load_sem).wait()
            pltpu.make_async_copy(tile_of(dy_hbm, 0), dy_s.at[rows_at(k), :], load_sem).wait()
            return carry

        lax.fori_loop(0, n_tiles, loaded, 0)

        def flip(k, carry):
            ut_s[:, rows_at(k)] = u_s[rows_at(k), own_rows].T
            dyt_s[:, rows_at(k)] = dy_s[rows_at(k), own_rows].T
            return carry

        lax.fori_loop(0, n_blk * CHUNK_TILES, flip, 0)
        add = jnp.logical_or(p > 0, add_first > 0)

        def step(f, carry):
            slot = f % 2

            @pl.when(f + 1 < n_ff)
            def _():
                for cp in weights(f + 1, 1 - slot):
                    cp.start()

            @pl.when(f >= 2)
            def _():
                for cp in grads(f - 2, slot, False):
                    cp.wait()

            for cp in weights(f, slot):
                cp.wait()

            d1_s[slot] = jnp.zeros((hw, FF_STEP), F32)
            d3_s[slot] = jnp.zeros((hw, FF_STEP), F32)
            d2t_s[...] = jnp.zeros((hw, FF_STEP), F32)

            @pl.when(add)
            def _():
                for cp in grads(f, slot, True):
                    cp.start()
                for cp in grads(f, slot, True):
                    cp.wait()
                d2t_s[...] = d2_s[slot].T

            def block(b, carry):
                rows = pl.ds(pl.multiple_of(b * CHUNK, CHUNK), CHUNK)
                w1, w3, w2 = w1_s[slot], w3_s[slot], w2_s[slot]
                u, dy = u_s[rows, :], dy_s[rows, :]
                act_a = mm(u, w1)
                act_b = mm(u, w3)
                d_g = mm(dy, w2, NT)
                sig = 0.5 * jnp.tanh(0.5 * act_a) + 0.5
                silu = act_a * sig
                g = (silu * act_b).astype(BF16)
                d_b = (d_g * silu).astype(BF16)
                d_a = (d_g * act_b * (sig + silu * (1.0 - sig))).astype(BF16)
                if back:
                    y = mm(g, w2)
                    du = mm(d_a, w1, NT) + mm(d_b, w3, NT)

                    @pl.when(f == 0)
                    def _():
                        y_acc[rows, :] = y
                        du_acc[rows, :] = du

                    @pl.when(f > 0)
                    def _():
                        y_acc[rows, :] += y
                        du_acc[rows, :] += du

                d1_s[slot] += mm(ut_s[:, rows], d_a)
                d3_s[slot] += mm(ut_s[:, rows], d_b)
                d2t_s[...] += mm(dyt_s[:, rows], g)
                return carry

            lax.fori_loop(0, n_blk, block, 0)
            d2_s[slot] = d2t_s[...].T
            for cp in grads(f, slot, False):
                cp.start()
            return carry

        lax.fori_loop(0, n_ff, step, 0)
        if back:
            def put(k, carry):
                t = lst[0, p * PASS_TILES + k]
                stage[0, rows_at(k), :] = y_acc[rows_at(k), :].astype(BF16)
                stage[1, rows_at(k), :] = du_acc[rows_at(k), :].astype(BF16)
                pltpu.make_async_copy(stage.at[0, rows_at(k), :], tile_of(y_hbm, t), row_sem).start()
                pltpu.make_async_copy(stage.at[1, rows_at(k), :], tile_of(du_hbm, t), row_sem).start()
                return carry

            lax.fori_loop(0, n_tiles, put, 0)

            def done(k, carry):
                pltpu.make_async_copy(zero, tile_of(y_hbm, 0), row_sem).wait()
                pltpu.make_async_copy(zero, tile_of(du_hbm, 0), row_sem).wait()
                return carry

            lax.fori_loop(0, n_tiles, done, 0)
        for f in (n_ff - 2, n_ff - 1):
            for cp in grads(f, f % 2, False):
                cp.wait()
        return carry

    n_pass = jnp.maximum((total + (PASS_TILES - 1)) // PASS_TILES, 1)
    lax.fori_loop(0, n_pass, one_pass, 0)
    if back:
        def cleared(t, carry):
            pltpu.make_async_copy(zero, tile_of(y_hbm, 0), row_sem).wait()
            pltpu.make_async_copy(zero, tile_of(du_hbm, 0), row_sem).wait()
            return carry

        lax.fori_loop(0, n_src * CHUNK_TILES - total, cleared, 0)


def experts(back, counts, prm, u_all, dy_all, own, got, dws):
    n_src, _, width = u_all.shape
    hw = width // 2
    ff = own[0].shape[2]
    rows = PASS_TILES * TILE
    scratch = [
        pltpu.VMEM((rows, width), BF16),
        pltpu.VMEM((rows, width), BF16),
        pltpu.VMEM((hw, rows), BF16),
        pltpu.VMEM((hw, rows), BF16),
        pltpu.VMEM((2, width, FF_STEP), BF16),
        pltpu.VMEM((2, width, FF_STEP), BF16),
        pltpu.VMEM((2, FF_STEP, width), BF16),
        pltpu.VMEM((2, hw, FF_STEP), F32),
        pltpu.VMEM((2, hw, FF_STEP), F32),
        pltpu.VMEM((2, FF_STEP, hw), F32),
        pltpu.VMEM((hw, FF_STEP), F32),
        pltpu.SMEM((2, n_src * CHUNK_TILES), jnp.int32),
        pltpu.SemaphoreType.DMA,
        pltpu.SemaphoreType.DMA((2, 6)),
        pltpu.SemaphoreType.DMA((2, 3)),
    ]
    outs = [jax.ShapeDtypeStruct(d.shape, d.dtype) for d in dws]
    if back:
        outs += [jax.ShapeDtypeStruct(u_all.shape, BF16)] * 2
        scratch += [
            pltpu.VMEM((rows, width), F32),
            pltpu.VMEM((rows, width), F32),
            pltpu.VMEM((2, rows, width), BF16),
            pltpu.VMEM((TILE, width), BF16),
            pltpu.SemaphoreType.DMA,
        ]
    units = 7.5 if back else 4.5
    return pl.pallas_call(
        functools.partial(experts_kernel, back, n_src),
        out_shape=tuple(outs),
        in_specs=[SMEM, SMEM] + [ANY] * 11,
        out_specs=tuple([ANY] * len(outs)),
        scratch_shapes=scratch,
        input_output_aliases={10: 0, 11: 1, 12: 2},
        compiler_params=params(),
        cost_estimate=pl.CostEstimate(flops=int(units * 2 * 2 * CHUNK * width * ff), bytes_accessed=30 * 2**20, transcendentals=0),
        name='experts_back' if back else 'experts_grad',
    )(counts, prm, u_all, dy_all, *own, *got, *dws)


def unset_kernel(*refs):
    pass


def unset(*shapes):
    outs = tuple(jax.ShapeDtypeStruct(s, d) for s, d in shapes)
    return pl.pallas_call(unset_kernel, out_shape=outs, out_specs=tuple([ANY] * len(outs)), name='unset')()


def solution(mesh):
    n_dev = mesh.shape['fsdp'] * mesh.shape['ep']
    tok_spec = P(('data', 'fsdp', 'ep'))
    in_specs = (tok_spec, P('fsdp'), P(None, None, 'fsdp'), P('ep', 'fsdp'), P('ep', 'fsdp'), P('ep', None, 'fsdp'), tok_spec, tok_spec, tok_spec, tok_spec)
    out_specs = (tok_spec, tok_spec, P(('data', 'ep'), 'fsdp'), P(('data', 'ep'), 'fsdp'), P(('data', 'ep'), None, 'fsdp'))

    def device_fn(tokens, w_qkv, w_out, w_gate, w_up, w_down, expert_idx, expert_slot, gate_wts, d_out):
        n_seq, seq_len, d_model = tokens.shape
        n_tok = n_seq * seq_len
        n_exp = n_dev
        half = lax.axis_index('fsdp').astype(jnp.int32)
        col = lax.axis_index('ep').astype(jnp.int32)
        swap = [(0, 1), (1, 0)]
        own = (w_gate, w_up, w_down)

        def other(local):
            got = []
            for w in own:
                piece = lax.dynamic_index_in_dim(w, local, 0, keepdims=False)
                got.append(lax.ppermute(piece, 'fsdp', swap))
            return got

        n_col = mesh.shape['ep']
        hw = w_qkv.shape[0]
        eighth = hw // n_col
        qkv_part = lax.dynamic_slice_in_dim(w_qkv.reshape(hw, 3 * d_model), col * eighth, eighth, 0)
        out_part = lax.dynamic_slice_in_dim(w_out.reshape(d_model, hw), col * 2 * eighth, 2 * eighth, 0)
        w_part = jnp.concatenate([qkv_part, out_part[:eighth], out_part[eighth:]], axis=1)
        w_all = lax.all_gather(w_part, GROUP)
        x_tok = tokens.reshape(n_tok, d_model)
        pos, cnt = route(expert_idx, expert_slot, n_exp)
        counts = lax.all_gather(cnt[0], GROUP)
        got_mine = other(1 - half)
        gate = gate_wts.reshape(n_tok // PACK_STEP, PACK_STEP).astype(F32)
        dout_tok = d_out.reshape(n_tok, d_model)
        zero = jnp.int32(0)
        dy_all = lax.all_gather(pack(zero, counts, pos, gate, dout_tok, True), GROUP)
        got_rest = other(half)

        h_tok, u_tok, qkv, ctx, lse, u_pack = attn_fwd(pos, w_all, x_tok, n_seq)
        u_all = lax.all_gather(u_pack, GROUP)

        tiles = (counts[:, :n_exp] + (TILE - 1)) // TILE
        n_chunks = jnp.max((jnp.sum(tiles, axis=1) + (CHUNK_TILES - 1)) // CHUNK_TILES)
        max_more = (n_tok + n_exp * (TILE - 1)) // CHUNK

        def prm(local, chunk, add):
            return jnp.stack([2 * col + local, local, half, chunk, add]).astype(jnp.int32)

        dws = unset(*[(w.shape, F32) for w in own])
        more_y, more_du = unset(*[((max_more, CHUNK, d_model), BF16)] * 2)
        *dws, y_all, du_all = experts(True, counts, prm(half, zero, zero), u_all, dy_all, own, got_mine, dws)
        first_du = lax.psum_scatter(du_all, GROUP, scatter_dimension=0)
        first_y = lax.psum_scatter(y_all, GROUP, scatter_dimension=0)

        def fetch(c):
            return lax.all_gather(pack(c, counts, pos, gate, u_tok, False), GROUP), lax.all_gather(pack(c, counts, pos, gate, dout_tok, True), GROUP)

        def more_back(state):
            c, d1, d3, d2, ys, dus = state
            u_c, dy_c = fetch(c)
            d1, d3, d2, y_c, du_c = experts(True, counts, prm(half, c, jnp.int32(1)), u_c, dy_c, own, got_mine, (d1, d3, d2))
            y_c = lax.psum_scatter(y_c, GROUP, scatter_dimension=0)
            du_c = lax.psum_scatter(du_c, GROUP, scatter_dimension=0)
            ys = lax.dynamic_update_index_in_dim(ys, y_c, c - 1, 0)
            dus = lax.dynamic_update_index_in_dim(dus, du_c, c - 1, 0)
            return c + 1, d1, d3, d2, ys, dus

        def more_grad(state):
            c, d1, d3, d2 = state
            u_c, dy_c = fetch(c)
            d1, d3, d2 = experts(False, counts, prm(1 - half, c, jnp.int32(1)), u_c, dy_c, own, got_rest, (d1, d3, d2))
            return c + 1, d1, d3, d2

        _, *dws, more_y, more_du = lax.while_loop(lambda s: s[0] < n_chunks, more_back, (jnp.int32(1), *dws, more_y, more_du))
        layer_out = unpack(n_chunks, pos, gate, h_tok, first_y, more_y).reshape(n_seq, seq_len, d_model)
        d_tokens = attn_bwd(n_chunks, pos, first_du, more_du, w_all, x_tok, h_tok, dout_tok, qkv, ctx, lse, n_seq).reshape(n_seq, seq_len, d_model)

        dws = experts(False, counts, prm(1 - half, zero, zero), u_all, dy_all, own, got_rest, dws)
        _, *dws = lax.while_loop(lambda s: s[0] < n_chunks, more_grad, (jnp.int32(1), *dws))
        return layer_out, d_tokens, *dws

    return jax.shard_map(device_fn, mesh=mesh, in_specs=in_specs, out_specs=out_specs, check_vma=False)
```

```python
import functools

import jax
import jax.numpy as jnp
from jax import lax
from jax.experimental import pallas as pl
from jax.experimental.pallas import tpu as pltpu
from jax.sharding import PartitionSpec as P


F32 = jnp.float32
BF16 = jnp.bfloat16
TILE = 128
CHUNK_TILES = 5
CHUNK = TILE * CHUNK_TILES
PASS_TILES = 20
FF_STEP = 512
N_PARTS = 3
GROUP = ('fsdp', 'ep')
NN = (((1,), (0,)), ((), ()))
NT = (((1,), (1,)), ((), ()))
TN = (((0,), (0,)), ((), ()))


def mm(lhs, rhs, dims=NN):
    return lax.dot_general(lhs, rhs, dims, preferred_element_type=F32)


def params(limit_mib=60):
    return pltpu.CompilerParams(vmem_limit_bytes=limit_mib * 1024 * 1024)


ANY = pl.BlockSpec(memory_space=pl.ANY)
SMEM = pl.BlockSpec(memory_space=pltpu.SMEM)
VMEM = pl.BlockSpec(memory_space=pltpu.VMEM)


def route_kernel(n_exp, idx_ref, slot_ref, pos_ref, cnt_ref):
    idx, kept = idx_ref[...], slot_ref[...] >= 0
    rows, lanes = idx.shape
    upper = (lax.broadcasted_iota(jnp.int32, (lanes, lanes), 0) <= lax.broadcasted_iota(jnp.int32, (lanes, lanes), 1)).astype(F32).astype(BF16)
    lower = (lax.broadcasted_iota(jnp.int32, (rows, rows), 1) < lax.broadcasted_iota(jnp.int32, (rows, rows), 0)).astype(F32).astype(BF16)
    ones = jnp.ones((lanes, lanes), BF16)
    lane = lax.broadcasted_iota(jnp.int32, (1, lanes), 1)
    pos = jnp.full((rows, lanes), -1.0, F32)
    cnt = jnp.zeros((1, lanes), F32)
    off = jnp.zeros((1, 1), F32)
    for e in range(n_exp):
        mask = jnp.logical_and(idx == e, kept)
        wide = jnp.where(mask, 1.0, 0.0)
        mask_b = wide.astype(BF16)
        inside = mm(mask_b, upper)
        before = mm(lower, mm(mask_b, ones).astype(BF16))
        count = jnp.sum(jnp.sum(wide, axis=1, keepdims=True), axis=0, keepdims=True)
        pos = jnp.where(mask, off + before + inside - 1.0, pos)
        cnt = jnp.where(lane == e, count, cnt)
        off = off + jnp.floor((count + (TILE - 1.0)) * (1.0 / TILE)) * TILE
    pos_ref[...] = pos.astype(jnp.int32)
    cnt_ref[...] = cnt.astype(jnp.int32)


def route(idx, slot, n_exp):
    n = idx.size
    shape = (n // 128, 128)
    return pl.pallas_call(
        functools.partial(route_kernel, n_exp),
        out_shape=(jax.ShapeDtypeStruct(shape, jnp.int32), jax.ShapeDtypeStruct((1, 128), jnp.int32)),
        in_specs=[VMEM, VMEM],
        out_specs=(VMEM, VMEM),
        name='route',
    )(idx.reshape(shape), slot.reshape(shape))


PACK_STEP = 1024


def pack_kernel(weighted, c_ref, cnt_ref, pos_ref, gate_ref, x_ref, out_ref, acc_ref):
    k = pl.program_id(0)
    row = lax.broadcasted_iota(jnp.int32, (CHUNK, PACK_STEP), 0) + c_ref[0] * CHUNK
    hit = row == pos_ref[pl.ds(k, 1), :]
    value = gate_ref[pl.ds(k, 1), :] if weighted else 1.0
    part = mm(jnp.where(hit, value, 0.0).astype(BF16), x_ref[...])

    @pl.when(k == 0)
    def _():
        acc_ref[...] = part

    @pl.when(k > 0)
    def _():
        acc_ref[...] += part

    @pl.when(k == pl.num_programs(0) - 1)
    def _():
        out_ref[...] = acc_ref[...].astype(BF16)


def pack(chunk, counts, pos, gate, x, weighted):
    n, width = x.shape
    steps = n // PACK_STEP
    return pl.pallas_call(
        functools.partial(pack_kernel, weighted),
        grid=(steps,),
        out_shape=jax.ShapeDtypeStruct((CHUNK, width), BF16),
        in_specs=[SMEM, ANY, pl.BlockSpec((steps, PACK_STEP), lambda k: (0, 0)), pl.BlockSpec((steps, PACK_STEP), lambda k: (0, 0)), pl.BlockSpec((PACK_STEP, width), lambda k: (k, 0))],
        out_specs=pl.BlockSpec((CHUNK, width), lambda k: (0, 0)),
        scratch_shapes=[pltpu.VMEM((CHUNK, width), F32)],
        compiler_params=params(),
        cost_estimate=pl.CostEstimate(flops=2 * CHUNK * n * width, bytes_accessed=2 * n * width, transcendentals=0),
        name='pack',
    )(chunk.reshape(1), counts, pos.reshape(steps, PACK_STEP), gate, x)


UNPACK_STEP = 512


def unpack_kernel(weighted, n_ref, pos_ref, gate_ref, *refs):
    if weighted:
        h_ref, first_ref, more_ref, out_ref, buf, acc, sem = refs
    else:
        first_ref, more_ref, out_ref, buf, acc, sem = refs
    k = pl.program_id(0)
    pos = pos_ref[pl.ds(k, 1), :]
    row = lax.broadcasted_iota(jnp.int32, (CHUNK, UNPACK_STEP), 0)
    value = gate_ref[pl.ds(k, 1), :] if weighted else 1.0

    def gathered(base, rows):
        return mm(jnp.where(row + base == pos, value, 0.0).astype(BF16), rows, TN)

    acc[...] = gathered(0, first_ref[...])

    def more(c, carry):
        copy = pltpu.make_async_copy(more_ref.at[c - 1], buf, sem)
        copy.start()
        copy.wait()
        acc[...] += gathered(c * CHUNK, buf[...])
        return carry

    lax.fori_loop(1, n_ref[0], more, 0)
    total = acc[...]
    if weighted:
        total = h_ref[...].astype(F32) + total
    out_ref[...] = total.astype(BF16)


def unpack(n_chunks, pos, gate, h, first, more):
    weighted = h is not None
    n = pos.size
    width = first.shape[1]
    steps = n // UNPACK_STEP
    small = pl.BlockSpec((steps, UNPACK_STEP), lambda k: (0, 0))
    rows = pl.BlockSpec((UNPACK_STEP, width), lambda k: (k, 0))
    return pl.pallas_call(
        functools.partial(unpack_kernel, weighted),
        grid=(steps,),
        out_shape=jax.ShapeDtypeStruct((n, width), BF16),
        in_specs=[SMEM, small, small] + ([rows] if weighted else []) + [pl.BlockSpec((CHUNK, width), lambda k: (0, 0)), ANY],
        out_specs=rows,
        scratch_shapes=[pltpu.VMEM((CHUNK, width), BF16), pltpu.VMEM((UNPACK_STEP, width), F32), pltpu.SemaphoreType.DMA],
        compiler_params=params(),
        cost_estimate=pl.CostEstimate(flops=2 * CHUNK * n * width, bytes_accessed=4 * n * width, transcendentals=0),
        name='unpack',
    )(n_chunks.reshape(1), pos.reshape(steps, UNPACK_STEP), gate.reshape(steps, UNPACK_STEP), *([h] if weighted else []), first, more)


QUERY_BLOCK = 256


def load_attention_weights(w_hbm, wqkv, wo, sem):
    n_dev, rows, _ = w_hbm.shape
    wide, hw = wqkv.shape[1], wo.shape[2]
    n_col = n_dev // 2
    copies = []
    for i in range(n_dev):
        copies.append(pltpu.make_async_copy(w_hbm.at[i, :, pl.ds(0, wide)], wqkv.at[pl.ds(i * rows, rows), :], sem))
        for j in range(2):
            dst = wo.at[i // n_col, pl.ds((i % n_col * 2 + j) * rows, rows), :]
            copies.append(pltpu.make_async_copy(w_hbm.at[i, :, pl.ds(wide + j * hw, hw)], dst, sem))
    for cp in copies:
        cp.start()
    for cp in copies:
        cp.wait()


def inv_rms_of(wide_vals):
    return lax.rsqrt(jnp.mean(wide_vals * wide_vals, axis=-1, keepdims=True) + 1e-6)


def head_lanes(shape, axis, head):
    lane = lax.broadcasted_iota(jnp.int32, shape, axis)
    return lane < 64 if head == 0 else lane >= 64


def causal_tail(values, fill):
    n, k = values.shape
    tail = values[:, k - n :]
    keep = lax.broadcasted_iota(jnp.int32, (n, n), 0) >= lax.broadcasted_iota(jnp.int32, (n, n), 1)
    tail = jnp.where(keep, tail, fill)
    return tail if k == n else jnp.concatenate([values[:, : k - n], tail], axis=1)


def attn_fwd_kernel(pos_ref, w_hbm, x_ref, h_ref, u_ref, qkv_ref, ctx_ref, p0_ref, p1_ref, pack_ref, wqkv, wo, acc, sem):
    i = pl.program_id(0)
    width = x_ref.shape[1]
    hw = width // 2
    seq = x_ref.shape[0]

    @pl.when(i == 0)
    def _():
        load_attention_weights(w_hbm, wqkv, wo, sem)

    x = x_ref[...].astype(F32)
    normed = (x * inv_rms_of(x)).astype(BF16)
    for t in range(3):
        cols = slice(t * width, (t + 1) * width)
        qkv_ref[:, cols] = mm(normed, wqkv[:, cols]).astype(BF16)
    for pair in range(width // 128):
        lanes = slice(pair * 128, (pair + 1) * 128)
        q = qkv_ref[:, lanes] * jnp.asarray(0.125, BF16)
        k = qkv_ref[:, width + pair * 128 : width + (pair + 1) * 128]
        v = qkv_ref[:, 2 * width + pair * 128 : 2 * width + (pair + 1) * 128]
        for j in range(seq // QUERY_BLOCK):
            rows = slice(j * QUERY_BLOCK, (j + 1) * QUERY_BLOCK)
            keys = slice(0, (j + 1) * QUERY_BLOCK)
            outs = []
            for head in range(2):
                qm = jnp.where(head_lanes((QUERY_BLOCK, 128), 1, head), q[rows], jnp.zeros((), BF16))
                s = causal_tail(mm(qm, k[keys], NT), -1e30)
                top = jnp.max(s, axis=1, keepdims=True)
                e = jnp.exp(s - top)
                total = jnp.sum(e, axis=1, keepdims=True)
                p = (e * (1.0 / total)).astype(BF16)
                (p0_ref, p1_ref)[j][0, pair * 2 + head] = p
                outs.append(mm(p, v[keys]))
            ctx_ref[rows, lanes] = jnp.where(head_lanes((QUERY_BLOCK, 128), 1, 0), outs[0], outs[1]).astype(BF16)
    ctx = ctx_ref[...]
    for f in range(2):
        cols = slice(f * hw, (f + 1) * hw)
        h_ref[:, cols] = (x_ref[:, cols].astype(F32) + mm(ctx, wo[f])).astype(BF16)
    h = h_ref[...].astype(F32)
    u = (h * inv_rms_of(h)).astype(BF16)
    u_ref[...] = u
    hit = lax.broadcasted_iota(jnp.int32, (CHUNK, seq), 0) == pos_ref[pl.ds(i, 1), :]
    part = mm(jnp.where(hit, 1.0, 0.0).astype(BF16), u)

    @pl.when(i == 0)
    def _():
        acc[...] = part

    @pl.when(i > 0)
    def _():
        acc[...] += part

    @pl.when(i == pl.num_programs(0) - 1)
    def _():
        pack_ref[...] = acc[...].astype(BF16)


def probs_shapes(n_seq, width):
    return [jax.ShapeDtypeStruct((n_seq, width // 64, QUERY_BLOCK, (j + 1) * QUERY_BLOCK), BF16) for j in range(2)]


def probs_specs(width):
    return [pl.BlockSpec((1, width // 64, QUERY_BLOCK, (j + 1) * QUERY_BLOCK), lambda i: (i, 0, 0, 0)) for j in range(2)]


def attn_fwd(pos, w_all, x, n_seq):
    n, width = x.shape
    seq = n // n_seq
    rows = pl.BlockSpec((seq, width), lambda i: (i, 0))
    return pl.pallas_call(
        attn_fwd_kernel,
        grid=(n_seq,),
        out_shape=(
            jax.ShapeDtypeStruct((n, width), BF16),
            jax.ShapeDtypeStruct((n, width), BF16),
            jax.ShapeDtypeStruct((n, 3 * width), BF16),
            jax.ShapeDtypeStruct((n, width), BF16),
            *probs_shapes(n_seq, width),
            jax.ShapeDtypeStruct((CHUNK, width), BF16),
        ),
        in_specs=[pl.BlockSpec((n_seq, seq), lambda i: (0, 0)), ANY, rows],
        out_specs=(rows, rows, pl.BlockSpec((seq, 3 * width), lambda i: (i, 0)), rows, *probs_specs(width), pl.BlockSpec((CHUNK, width), lambda i: (0, 0))),
        scratch_shapes=[pltpu.VMEM((width, 3 * width), BF16), pltpu.VMEM((2, width, width // 2), BF16), pltpu.VMEM((CHUNK, width), F32), pltpu.SemaphoreType.DMA],
        compiler_params=params(),
        cost_estimate=pl.CostEstimate(flops=30 * 10**9, bytes_accessed=50 * 2**20, transcendentals=0),
        name='attn_fwd',
    )(pos.reshape(n_seq, seq), w_all, x)


def norm_back(grad, wide_vals):
    inv = inv_rms_of(wide_vals)
    return inv * (grad - wide_vals * (inv * inv * jnp.mean(grad * wide_vals, axis=-1, keepdims=True)))


def attn_bwd_kernel(n_ref, pos_ref, first_ref, more_hbm, w_hbm, x_ref, h_ref, dout_ref, qkv_ref, ctx_ref, p0_ref, p1_ref, dx_ref, wqkv, wo, dqkv, dctx, dh, buf, sem):
    i = pl.program_id(0)
    seq, width = x_ref.shape
    hw = width // 2

    @pl.when(i == 0)
    def _():
        load_attention_weights(w_hbm, wqkv, wo, sem)

    pos = pos_ref[pl.ds(i, 1), :]
    row = lax.broadcasted_iota(jnp.int32, (CHUNK, seq), 0)

    def gathered(base, rows):
        return mm(jnp.where(row + base == pos, 1.0, 0.0).astype(BF16), rows, TN)

    dh[...] = gathered(0, first_ref[...])

    def more(c, carry):
        copy = pltpu.make_async_copy(more_hbm.at[c - 1], buf, sem)
        copy.start()
        copy.wait()
        dh[...] += gathered(c * CHUNK, buf[...])
        return carry

    lax.fori_loop(1, n_ref[0], more, 0)
    dh[...] = dout_ref[...].astype(F32) + norm_back(dh[...], h_ref[...].astype(F32))
    dh_b = dh[...].astype(BF16)
    dctx[...] = (mm(dh_b[:, :hw], wo[0], NT) + mm(dh_b[:, hw:], wo[1], NT)).astype(BF16)
    zero = jnp.zeros((), BF16)
    for pair in range(width // 128):
        lanes = slice(pair * 128, (pair + 1) * 128)
        k_lanes = slice(width + pair * 128, width + (pair + 1) * 128)
        v_lanes = slice(2 * width + pair * 128, 2 * width + (pair + 1) * 128)
        q = qkv_ref[:, lanes] * jnp.asarray(0.125, BF16)
        k, v = qkv_ref[:, k_lanes], qkv_ref[:, v_lanes]
        do = dctx[:, lanes]
        q_t, do_t = q.T, do.T
        prod = do.astype(F32) * ctx_ref[:, lanes].astype(F32)
        dk_t = [jnp.zeros((128, QUERY_BLOCK), F32) for _ in range(seq // QUERY_BLOCK)]
        dv_t = list(dk_t)
        for j in range(seq // QUERY_BLOCK):
            rows = slice(j * QUERY_BLOCK, (j + 1) * QUERY_BLOCK)
            keys = slice(0, (j + 1) * QUERY_BLOCK)
            dqs = []
            for head in range(2):
                mine = head_lanes((QUERY_BLOCK, 128), 1, head)
                mine_t = head_lanes((128, QUERY_BLOCK), 0, head)
                dom = jnp.where(mine, do[rows], zero)
                delta = jnp.sum(jnp.where(mine, prod[rows], 0.0), axis=1, keepdims=True)
                pb = (p0_ref, p1_ref)[j][0, pair * 2 + head]
                dp = mm(dom, v[keys], NT)
                ds = (pb.astype(F32) * (dp - delta)).astype(BF16)
                dqs.append(mm(ds, k[keys]))
                qm_t, dom_t = jnp.where(mine_t, q_t[:, rows], zero), jnp.where(mine_t, do_t[:, rows], zero)
                dk_part, dv_part = mm(qm_t, ds), mm(dom_t, pb)
                for c in range(j + 1):
                    cols = slice(c * QUERY_BLOCK, (c + 1) * QUERY_BLOCK)
                    dk_t[c] = dk_t[c] + dk_part[:, cols]
                    dv_t[c] = dv_t[c] + dv_part[:, cols]
            dqkv[rows, lanes] = (jnp.where(head_lanes((QUERY_BLOCK, 128), 1, 0), dqs[0], dqs[1]) * 0.125).astype(BF16)
        for c in range(seq // QUERY_BLOCK):
            rows = slice(c * QUERY_BLOCK, (c + 1) * QUERY_BLOCK)
            dqkv[rows, k_lanes] = dk_t[c].astype(BF16).T
            dqkv[rows, v_lanes] = dv_t[c].astype(BF16).T
    dn = mm(dqkv[...], wqkv[...], NT)
    dx_ref[...] = (dh[...] + norm_back(dn, x_ref[...].astype(F32))).astype(BF16)


def attn_bwd(n_chunks, pos, first, more, w_all, x, h, dout, qkv, ctx, probs, n_seq):
    n, width = x.shape
    seq = n // n_seq
    rows = pl.BlockSpec((seq, width), lambda i: (i, 0))
    return pl.pallas_call(
        attn_bwd_kernel,
        grid=(n_seq,),
        out_shape=jax.ShapeDtypeStruct((n, width), BF16),
        in_specs=[SMEM, pl.BlockSpec((n_seq, seq), lambda i: (0, 0)), pl.BlockSpec((CHUNK, width), lambda i: (0, 0)), ANY, ANY, rows, rows, rows, pl.BlockSpec((seq, 3 * width), lambda i: (i, 0)), rows, *probs_specs(width)],
        out_specs=rows,
        scratch_shapes=[
            pltpu.VMEM((width, 3 * width), BF16),
            pltpu.VMEM((2, width, width // 2), BF16),
            pltpu.VMEM((seq, 3 * width), BF16),
            pltpu.VMEM((seq, width), BF16),
            pltpu.VMEM((seq, width), F32),
            pltpu.VMEM((CHUNK, width), BF16),
            pltpu.SemaphoreType.DMA,
        ],
        compiler_params=params(),
        cost_estimate=pl.CostEstimate(flops=50 * 10**9, bytes_accessed=60 * 2**20, transcendentals=0),
        name='attn_bwd',
    )(n_chunks.reshape(1), pos.reshape(n_seq, seq), first, more, w_all, x, h, dout, qkv, ctx, *probs)


def experts_kernel(back, first, last, f_base, n_src, cnt_ref, prm_ref, u_hbm, dy_hbm, w1_hbm, w3_hbm, w2_hbm, r13_hbm, r2_hbm, i1, i3, i2, *refs):
    if back:
        o1, o3, o2, y_part, du_part = refs[2:7]
        scratch = refs[7:]
        if last:
            (y_hbm, du_hbm), scratch = scratch[:2], scratch[2:]
        y_acc, du_acc, stage, zero, row_sem, part_sem = scratch[-6:]
        scratch = scratch[:-6]
    else:
        o1, o3, o2 = refs[:3]
        scratch = refs[3:]
    u_s, dy_s, ut_s, dyt_s, w1_s, w3_s, w2_s, d1_s, d3_s, d2_s, d2t_s, lst, load_sem, w_sem, d_sem = scratch
    expert, local, half, chunk, add_first = prm_ref[0], prm_ref[1], prm_ref[2], prm_ref[3], prm_ref[4]
    width = u_s.shape[1]
    hw = width // 2
    n_ff = r2_hbm.shape[0] // FF_STEP
    first_tile = chunk * CHUNK_TILES
    own_rows = pl.ds(pl.multiple_of(half * hw, hw), hw)
    got_rows = pl.ds(pl.multiple_of((1 - half) * hw, hw), hw)

    if back and last:
        def unmark(t, carry):
            lst[1, t] = 0
            return carry

        lax.fori_loop(0, n_src * CHUNK_TILES, unmark, 0)
    total = jnp.int32(0)
    for s in range(n_src):
        off, own = jnp.int32(0), jnp.int32(0)
        for e in range(n_src):
            tiles = (cnt_ref[s, e] + (TILE - 1)) // TILE
            off = off + jnp.where(e < expert, tiles, 0)
            own = own + jnp.where(e == expert, tiles, 0)
        lo = jnp.clip(off - first_tile, 0, CHUNK_TILES)
        hi = jnp.clip(off + own - first_tile, 0, CHUNK_TILES)

        def note(j, t, s=s):
            lst[0, t] = s * CHUNK_TILES + j
            if back and last:
                lst[1, s * CHUNK_TILES + j] = 1
            return t + 1

        total = lax.fori_loop(lo, hi, note, total)

    def tile_of(ref, t):
        return ref.at[t // CHUNK_TILES, pl.ds(pl.multiple_of((t % CHUNK_TILES) * TILE, TILE), TILE), :]

    if back and last:
        zero[...] = jnp.zeros_like(zero)

        def clear(t, n):
            @pl.when(lst[1, t] == 0)
            def _():
                pltpu.make_async_copy(zero, tile_of(y_hbm, t), row_sem).start()
                pltpu.make_async_copy(zero, tile_of(du_hbm, t), row_sem).start()

            return n

        lax.fori_loop(0, n_src * CHUNK_TILES, clear, 0)

    def weights(f, slot):
        cols = pl.ds(pl.multiple_of(f_base + f * FF_STEP, FF_STEP), FF_STEP)
        part = pl.ds(pl.multiple_of(f * FF_STEP, FF_STEP), FF_STEP)
        pairs = [
            (w1_hbm.at[local, :, cols], w1_s.at[slot, own_rows, :]),
            (r13_hbm.at[pl.ds(0, hw), part], w1_s.at[slot, got_rows, :]),
            (w3_hbm.at[local, :, cols], w3_s.at[slot, own_rows, :]),
            (r13_hbm.at[pl.ds(hw, hw), part], w3_s.at[slot, got_rows, :]),
            (w2_hbm.at[local, cols, :], w2_s.at[slot, :, own_rows]),
            (r2_hbm.at[part, :], w2_s.at[slot, :, got_rows]),
        ]
        return [pltpu.make_async_copy(src, dst, w_sem.at[slot, i]) for i, (src, dst) in enumerate(pairs)]

    def grads(f, slot, ins):
        cols = pl.ds(pl.multiple_of(f_base + f * FF_STEP, FF_STEP), FF_STEP)
        hbm = (i1, i3, i2) if ins else (o1, o3, o2)
        pairs = [
            (hbm[0].at[local, :, cols], d1_s.at[slot]),
            (hbm[1].at[local, :, cols], d3_s.at[slot]),
            (hbm[2].at[local, cols, :], d2_s.at[slot]),
        ]
        if not ins:
            pairs = [(b, a) for a, b in pairs]
        return [pltpu.make_async_copy(src, dst, d_sem.at[slot, i]) for i, (src, dst) in enumerate(pairs)]

    def one_pass(p, carry):
        for cp in weights(0, 0):
            cp.start()
        n_tiles = jnp.clip(total - p * PASS_TILES, 0, PASS_TILES)
        n_blk = (n_tiles + (CHUNK_TILES - 1)) // CHUNK_TILES

        def rows_at(k):
            return pl.ds(pl.multiple_of(k * TILE, TILE), TILE)

        def load(k, carry):
            t = lst[0, p * PASS_TILES + k]
            pltpu.make_async_copy(tile_of(u_hbm, t), u_s.at[rows_at(k), :], load_sem).start()
            pltpu.make_async_copy(tile_of(dy_hbm, t), dy_s.at[rows_at(k), :], load_sem).start()
            return carry

        lax.fori_loop(0, n_tiles, load, 0)

        def partial_sums(b, out):
            rows = pl.ds(pl.multiple_of(b * CHUNK, CHUNK), CHUNK)
            hbm_rows = pl.ds(pl.multiple_of((p * (PASS_TILES // CHUNK_TILES) + b) * CHUNK, CHUNK), CHUNK)
            pairs = [(y_acc.at[rows, :], y_part.at[hbm_rows, :]), (du_acc.at[rows, :], du_part.at[hbm_rows, :])]
            return [pltpu.make_async_copy(*(pair if out else pair[::-1]), part_sem) for pair in pairs]

        def each_block(out, action):
            def go(b, carry):
                for cp in partial_sums(b, out):
                    getattr(cp, action)()
                return carry

            lax.fori_loop(0, n_blk, go, 0)

        if back and not first:
            each_block(False, 'start')

        def fill(k, carry):
            u_s[rows_at(k), :] = jnp.zeros((TILE, width), BF16)
            dy_s[rows_at(k), :] = jnp.zeros((TILE, width), BF16)
            return carry

        lax.fori_loop(n_tiles, n_blk * CHUNK_TILES, fill, 0)

        def loaded(k, carry):
            pltpu.make_async_copy(tile_of(u_hbm, 0), u_s.at[rows_at(k), :], load_sem).wait()
            pltpu.make_async_copy(tile_of(dy_hbm, 0), dy_s.at[rows_at(k), :], load_sem).wait()
            return carry

        lax.fori_loop(0, n_tiles, loaded, 0)

        def flip(k, carry):
            ut_s[:, rows_at(k)] = u_s[rows_at(k), own_rows].T
            dyt_s[:, rows_at(k)] = dy_s[rows_at(k), own_rows].T
            return carry

        lax.fori_loop(0, n_blk * CHUNK_TILES, flip, 0)
        if back and not first:
            each_block(False, 'wait')
        add = jnp.logical_or(p > 0, add_first > 0)

        def step(f, carry):
            slot = f % 2

            @pl.when(f + 1 < n_ff)
            def _():
                for cp in weights(f + 1, 1 - slot):
                    cp.start()

            @pl.when(f >= 2)
            def _():
                for cp in grads(f - 2, slot, False):
                    cp.wait()

            for cp in weights(f, slot):
                cp.wait()

            d1_s[slot] = jnp.zeros((hw, FF_STEP), F32)
            d3_s[slot] = jnp.zeros((hw, FF_STEP), F32)
            d2t_s[...] = jnp.zeros((hw, FF_STEP), F32)

            @pl.when(add)
            def _():
                for cp in grads(f, slot, True):
                    cp.start()
                for cp in grads(f, slot, True):
                    cp.wait()
                d2t_s[...] = d2_s[slot].T

            def block(b, carry):
                rows = pl.ds(pl.multiple_of(b * CHUNK, CHUNK), CHUNK)
                w1, w3, w2 = w1_s[slot], w3_s[slot], w2_s[slot]
                u, dy = u_s[rows, :], dy_s[rows, :]
                act_a = mm(u, w1)
                act_b = mm(u, w3)
                d_g = mm(dy, w2, NT)
                sig = 0.5 * jnp.tanh(0.5 * act_a) + 0.5
                silu = act_a * sig
                g = (silu * act_b).astype(BF16)
                d_b = (d_g * silu).astype(BF16)
                d_a = (d_g * act_b * (sig + silu * (1.0 - sig))).astype(BF16)
                if back:
                    y = mm(g, w2)
                    du = mm(d_a, w1, NT) + mm(d_b, w3, NT)

                    if first:
                        @pl.when(f == 0)
                        def _():
                            y_acc[rows, :] = y
                            du_acc[rows, :] = du

                        @pl.when(f > 0)
                        def _():
                            y_acc[rows, :] += y
                            du_acc[rows, :] += du
                    else:
                        y_acc[rows, :] += y
                        du_acc[rows, :] += du

                d1_s[slot] += mm(ut_s[:, rows], d_a)
                d3_s[slot] += mm(ut_s[:, rows], d_b)
                d2t_s[...] += mm(dyt_s[:, rows], g)
                return carry

            lax.fori_loop(0, n_blk, block, 0)
            d2_s[slot] = d2t_s[...].T
            for cp in grads(f, slot, False):
                cp.start()
            return carry

        lax.fori_loop(0, n_ff, step, 0)
        if back and not last:
            each_block(True, 'start')
            each_block(True, 'wait')
        if back and last:
            def put(k, carry):
                t = lst[0, p * PASS_TILES + k]
                stage[0, rows_at(k), :] = y_acc[rows_at(k), :].astype(BF16)
                stage[1, rows_at(k), :] = du_acc[rows_at(k), :].astype(BF16)
                pltpu.make_async_copy(stage.at[0, rows_at(k), :], tile_of(y_hbm, t), row_sem).start()
                pltpu.make_async_copy(stage.at[1, rows_at(k), :], tile_of(du_hbm, t), row_sem).start()
                return carry

            lax.fori_loop(0, n_tiles, put, 0)

            def done(k, carry):
                pltpu.make_async_copy(zero, tile_of(y_hbm, 0), row_sem).wait()
                pltpu.make_async_copy(zero, tile_of(du_hbm, 0), row_sem).wait()
                return carry

            lax.fori_loop(0, n_tiles, done, 0)
        for f in (n_ff - 2, n_ff - 1):
            for cp in grads(f, f % 2, False):
                cp.wait()
        return carry

    n_pass = jnp.maximum((total + (PASS_TILES - 1)) // PASS_TILES, 1)
    lax.fori_loop(0, n_pass, one_pass, 0)
    if back and last:
        def cleared(t, carry):
            pltpu.make_async_copy(zero, tile_of(y_hbm, 0), row_sem).wait()
            pltpu.make_async_copy(zero, tile_of(du_hbm, 0), row_sem).wait()
            return carry

        lax.fori_loop(0, n_src * CHUNK_TILES - total, cleared, 0)


def experts(back, part, n_parts, counts, prm, u_all, dy_all, own, got, dws, sums=()):
    n_src, _, width = u_all.shape
    first, last = part == 0, part == n_parts - 1
    hw = width // 2
    ff = got[1].shape[0]
    rows = PASS_TILES * TILE
    scratch = [
        pltpu.VMEM((rows, width), BF16),
        pltpu.VMEM((rows, width), BF16),
        pltpu.VMEM((hw, rows), BF16),
        pltpu.VMEM((hw, rows), BF16),
        pltpu.VMEM((2, width, FF_STEP), BF16),
        pltpu.VMEM((2, width, FF_STEP), BF16),
        pltpu.VMEM((2, FF_STEP, width), BF16),
        pltpu.VMEM((2, hw, FF_STEP), F32),
        pltpu.VMEM((2, hw, FF_STEP), F32),
        pltpu.VMEM((2, FF_STEP, hw), F32),
        pltpu.VMEM((hw, FF_STEP), F32),
        pltpu.SMEM((2, n_src * CHUNK_TILES), jnp.int32),
        pltpu.SemaphoreType.DMA,
        pltpu.SemaphoreType.DMA((2, 6)),
        pltpu.SemaphoreType.DMA((2, 3)),
    ]
    outs = [jax.ShapeDtypeStruct(d.shape, d.dtype) for d in (*dws, *sums)]
    n_alias = len(outs)
    if back and last:
        outs += [jax.ShapeDtypeStruct(u_all.shape, BF16)] * 2
    if back:
        scratch += [
            pltpu.VMEM((rows, width), F32),
            pltpu.VMEM((rows, width), F32),
            pltpu.VMEM((2, rows, width), BF16),
            pltpu.VMEM((TILE, width), BF16),
            pltpu.SemaphoreType.DMA,
            pltpu.SemaphoreType.DMA,
        ]
    units = 7.5 if back else 4.5
    return pl.pallas_call(
        functools.partial(experts_kernel, back, first, last, part * ff, n_src),
        out_shape=tuple(outs),
        in_specs=[SMEM, SMEM] + [ANY] * (7 + n_alias),
        out_specs=tuple([ANY] * len(outs)),
        scratch_shapes=scratch,
        input_output_aliases={9 + i: i for i in range(n_alias)},
        compiler_params=params(),
        cost_estimate=pl.CostEstimate(flops=int(units * 2 * 2 * CHUNK * width * ff), bytes_accessed=10 * 2**20, transcendentals=0),
    )(counts, prm, u_all, dy_all, *own, *got, *dws, *sums)


def unset_kernel(*refs):
    pass


def unset(*shapes):
    outs = tuple(jax.ShapeDtypeStruct(s, d) for s, d in shapes)
    return pl.pallas_call(unset_kernel, out_shape=outs, out_specs=tuple([ANY] * len(outs)), name='unset')()


def solution(mesh):
    n_dev = mesh.shape['fsdp'] * mesh.shape['ep']
    tok_spec = P(('data', 'fsdp', 'ep'))
    in_specs = (tok_spec, P('fsdp'), P(None, None, 'fsdp'), P('ep', 'fsdp'), P('ep', 'fsdp'), P('ep', None, 'fsdp'), tok_spec, tok_spec, tok_spec, tok_spec)
    out_specs = (tok_spec, tok_spec, P(('data', 'ep'), 'fsdp'), P(('data', 'ep'), 'fsdp'), P(('data', 'ep'), None, 'fsdp'))

    def device_fn(tokens, w_qkv, w_out, w_gate, w_up, w_down, expert_idx, expert_slot, gate_wts, d_out):
        n_seq, seq_len, d_model = tokens.shape
        n_tok = n_seq * seq_len
        n_exp = n_dev
        half = lax.axis_index('fsdp').astype(jnp.int32)
        col = lax.axis_index('ep').astype(jnp.int32)
        swap = [(0, 1), (1, 0)]
        own = (w_gate, w_up, w_down)

        def other(local):
            got = []
            gate, up, down = [lax.dynamic_index_in_dim(w, local, 0, keepdims=False) for w in own]
            size = down.shape[0] // N_PARTS
            for r in range(N_PARTS):
                cols = slice(r * size, (r + 1) * size)
                both = lax.ppermute(jnp.concatenate([gate[:, cols], up[:, cols]], axis=0), 'fsdp', swap)
                got.append((both, lax.ppermute(down[cols], 'fsdp', swap)))
            return got

        def back(chunk, add, u_c, dy_c, dws):
            sums = unset(*[((n_dev * CHUNK, d_model), F32)] * 2)
            for r in range(N_PARTS):
                *state, = experts(True, r, N_PARTS, counts, prm(half, chunk, add), u_c, dy_c, own, got_mine[r], dws, sums)
                dws, sums = state[:3], state[3:5]
            return dws, state[5], state[6]

        def grad_part(r, chunk, add, u_c, dy_c, dws):
            return experts(False, r, N_PARTS, counts, prm(1 - half, chunk, add), u_c, dy_c, own, got_rest[r], dws)

        def prm(local, chunk, add):
            return jnp.stack([2 * col + local, local, half, chunk, add]).astype(jnp.int32)

        n_col = mesh.shape['ep']
        hw = w_qkv.shape[0]
        eighth = hw // n_col
        qkv_part = lax.dynamic_slice_in_dim(w_qkv.reshape(hw, 3 * d_model), col * eighth, eighth, 0)
        out_part = lax.dynamic_slice_in_dim(w_out.reshape(d_model, hw), col * 2 * eighth, 2 * eighth, 0)
        w_part = jnp.concatenate([qkv_part, out_part[:eighth], out_part[eighth:]], axis=1)
        w_all = lax.all_gather(w_part, GROUP)
        x_tok = tokens.reshape(n_tok, d_model)
        pos, cnt = route(expert_idx, expert_slot, n_exp)
        counts = lax.all_gather(cnt[0], GROUP)
        got_mine = other(1 - half)
        gate = gate_wts.reshape(n_tok // PACK_STEP, PACK_STEP).astype(F32)
        dout_tok = d_out.reshape(n_tok, d_model)
        zero = jnp.int32(0)
        dy_all = lax.all_gather(pack(zero, counts, pos, gate, dout_tok, True), GROUP)
        got_rest = other(half)

        h_tok, u_tok, qkv, ctx, *probs, u_pack = attn_fwd(pos, w_all, x_tok, n_seq)
        u_all = lax.all_gather(u_pack, GROUP)

        tiles = (counts[:, :n_exp] + (TILE - 1)) // TILE
        n_chunks = jnp.max((jnp.sum(tiles, axis=1) + (CHUNK_TILES - 1)) // CHUNK_TILES)
        max_more = (n_tok + n_exp * (TILE - 1)) // CHUNK

        dws = unset(*[(w.shape, F32) for w in own])
        more_y, more_du = unset(*[((max_more, CHUNK, d_model), BF16)] * 2)
        dws, y_all, du_all = back(zero, zero, u_all, dy_all, dws)
        first_du = lax.psum_scatter(du_all, GROUP, scatter_dimension=0)

        first_y = lax.psum_scatter(y_all, GROUP, scatter_dimension=0)

        def fetch(c):
            return lax.all_gather(pack(c, counts, pos, gate, u_tok, False), GROUP), lax.all_gather(pack(c, counts, pos, gate, dout_tok, True), GROUP)

        def more_back(state):
            c, d1, d3, d2, ys, dus = state
            u_c, dy_c = fetch(c)
            (d1, d3, d2), y_c, du_c = back(c, jnp.int32(1), u_c, dy_c, (d1, d3, d2))
            y_c = lax.psum_scatter(y_c, GROUP, scatter_dimension=0)
            du_c = lax.psum_scatter(du_c, GROUP, scatter_dimension=0)
            ys = lax.dynamic_update_index_in_dim(ys, y_c, c - 1, 0)
            dus = lax.dynamic_update_index_in_dim(dus, du_c, c - 1, 0)
            return c + 1, d1, d3, d2, ys, dus

        def more_grad(state):
            c, d1, d3, d2 = state
            u_c, dy_c = fetch(c)
            dws = (d1, d3, d2)
            for r in range(N_PARTS):
                dws = grad_part(r, c, jnp.int32(1), u_c, dy_c, dws)
            return (c + 1, *dws)

        _, *dws, more_y, more_du = lax.while_loop(lambda s: s[0] < n_chunks, more_back, (jnp.int32(1), *dws, more_y, more_du))
        layer_out = unpack(n_chunks, pos, gate, h_tok, first_y, more_y).reshape(n_seq, seq_len, d_model)
        d_tokens = attn_bwd(n_chunks, pos, first_du, more_du, w_all, x_tok, h_tok, dout_tok, qkv, ctx, probs, n_seq).reshape(n_seq, seq_len, d_model)

        for r in range(N_PARTS):
            dws = grad_part(r, zero, zero, u_all, dy_all, dws)
        _, *dws = lax.while_loop(lambda s: s[0] < n_chunks, more_grad, (jnp.int32(1), *dws))
        return layer_out, d_tokens, *dws

    return jax.shard_map(device_fn, mesh=mesh, in_specs=in_specs, out_specs=out_specs, check_vma=False)
```

```python
import functools

import jax
import jax.numpy as jnp
from jax import lax
from jax.experimental import pallas as pl
from jax.experimental.pallas import tpu as pltpu
from jax.sharding import PartitionSpec as P


F32 = jnp.float32
BF16 = jnp.bfloat16
TILE = 128
CHUNK_TILES = 5
CHUNK = TILE * CHUNK_TILES
PASS_TILES = 20
FF_STEP = 512
N_PARTS = 3
GROUP = ('fsdp', 'ep')
MESH = pl.DeviceIdType.MESH
NN = (((1,), (0,)), ((), ()))
NT = (((1,), (1,)), ((), ()))
TN = (((0,), (0,)), ((), ()))


def mm(lhs, rhs, dims=NN):
    return lax.dot_general(lhs, rhs, dims, preferred_element_type=F32)


def params(limit_mib=60):
    return pltpu.CompilerParams(vmem_limit_bytes=limit_mib * 1024 * 1024)


ANY = pl.BlockSpec(memory_space=pl.ANY)
SMEM = pl.BlockSpec(memory_space=pltpu.SMEM)
VMEM = pl.BlockSpec(memory_space=pltpu.VMEM)


def route_kernel(n_exp, idx_ref, slot_ref, pos_ref, cnt_ref):
    idx, kept = idx_ref[...], slot_ref[...] >= 0
    rows, lanes = idx.shape
    upper = (lax.broadcasted_iota(jnp.int32, (lanes, lanes), 0) <= lax.broadcasted_iota(jnp.int32, (lanes, lanes), 1)).astype(F32).astype(BF16)
    lower = (lax.broadcasted_iota(jnp.int32, (rows, rows), 1) < lax.broadcasted_iota(jnp.int32, (rows, rows), 0)).astype(F32).astype(BF16)
    ones = jnp.ones((lanes, lanes), BF16)
    lane = lax.broadcasted_iota(jnp.int32, (1, lanes), 1)
    pos = jnp.full((rows, lanes), -1.0, F32)
    cnt = jnp.zeros((1, lanes), F32)
    off = jnp.zeros((1, 1), F32)
    for e in range(n_exp):
        mask = jnp.logical_and(idx == e, kept)
        wide = jnp.where(mask, 1.0, 0.0)
        mask_b = wide.astype(BF16)
        inside = mm(mask_b, upper)
        before = mm(lower, mm(mask_b, ones).astype(BF16))
        count = jnp.sum(jnp.sum(wide, axis=1, keepdims=True), axis=0, keepdims=True)
        pos = jnp.where(mask, off + before + inside - 1.0, pos)
        cnt = jnp.where(lane == e, count, cnt)
        off = off + jnp.floor((count + (TILE - 1.0)) * (1.0 / TILE)) * TILE
    pos_ref[...] = pos.astype(jnp.int32)
    cnt_ref[...] = cnt.astype(jnp.int32)


def route(idx, slot, n_exp):
    n = idx.size
    shape = (n // 128, 128)
    return pl.pallas_call(
        functools.partial(route_kernel, n_exp),
        out_shape=(jax.ShapeDtypeStruct(shape, jnp.int32), jax.ShapeDtypeStruct((1, 128), jnp.int32)),
        in_specs=[VMEM, VMEM],
        out_specs=(VMEM, VMEM),
        name='route',
    )(idx.reshape(shape), slot.reshape(shape))


PACK_STEP = 1024


def pack_kernel(weighted, c_ref, pos_ref, gate_ref, x_ref, out_ref, acc_ref):
    k = pl.program_id(0)
    row = lax.broadcasted_iota(jnp.int32, (CHUNK, PACK_STEP), 0) + c_ref[0] * CHUNK
    hit = row == pos_ref[pl.ds(k, 1), :]
    value = gate_ref[pl.ds(k, 1), :] if weighted else 1.0
    part = mm(jnp.where(hit, value, 0.0).astype(BF16), x_ref[...])

    @pl.when(k == 0)
    def _():
        acc_ref[...] = part

    @pl.when(k > 0)
    def _():
        acc_ref[...] += part

    @pl.when(k == pl.num_programs(0) - 1)
    def _():
        out_ref[...] = acc_ref[...].astype(BF16)


def pack(chunk, pos, gate, x, weighted):
    n, width = x.shape
    steps = n // PACK_STEP
    return pl.pallas_call(
        functools.partial(pack_kernel, weighted),
        grid=(steps,),
        out_shape=jax.ShapeDtypeStruct((CHUNK, width), BF16),
        in_specs=[SMEM, pl.BlockSpec((steps, PACK_STEP), lambda k: (0, 0)), pl.BlockSpec((steps, PACK_STEP), lambda k: (0, 0)), pl.BlockSpec((PACK_STEP, width), lambda k: (k, 0))],
        out_specs=pl.BlockSpec((CHUNK, width), lambda k: (0, 0)),
        scratch_shapes=[pltpu.VMEM((CHUNK, width), F32)],
        compiler_params=params(),
        cost_estimate=pl.CostEstimate(flops=2 * CHUNK * n * width, bytes_accessed=2 * n * width, transcendentals=0),
        name='pack',
    )(chunk.reshape(1), pos.reshape(steps, PACK_STEP), gate, x)


UNPACK_STEP = 512


def unpack_kernel(weighted, n_ref, pos_ref, gate_ref, *refs):
    if weighted:
        h_ref, first_ref, more_ref, out_ref, buf, acc, sem = refs
    else:
        first_ref, more_ref, out_ref, buf, acc, sem = refs
    k = pl.program_id(0)
    pos = pos_ref[pl.ds(k, 1), :]
    row = lax.broadcasted_iota(jnp.int32, (CHUNK, UNPACK_STEP), 0)
    value = gate_ref[pl.ds(k, 1), :] if weighted else 1.0

    def gathered(base, rows):
        return mm(jnp.where(row + base == pos, value, 0.0).astype(BF16), rows, TN)

    acc[...] = gathered(0, first_ref[...])

    def more(c, carry):
        copy = pltpu.make_async_copy(more_ref.at[c - 1], buf, sem)
        copy.start()
        copy.wait()
        acc[...] += gathered(c * CHUNK, buf[...])
        return carry

    lax.fori_loop(1, n_ref[0], more, 0)
    total = acc[...]
    if weighted:
        total = h_ref[...].astype(F32) + total
    out_ref[...] = total.astype(BF16)


def unpack(n_chunks, pos, gate, h, first, more):
    weighted = h is not None
    n = pos.size
    width = first.shape[1]
    steps = n // UNPACK_STEP
    small = pl.BlockSpec((steps, UNPACK_STEP), lambda k: (0, 0))
    rows = pl.BlockSpec((UNPACK_STEP, width), lambda k: (k, 0))
    return pl.pallas_call(
        functools.partial(unpack_kernel, weighted),
        grid=(steps,),
        out_shape=jax.ShapeDtypeStruct((n, width), BF16),
        in_specs=[SMEM, small, small] + ([rows] if weighted else []) + [pl.BlockSpec((CHUNK, width), lambda k: (0, 0)), ANY],
        out_specs=rows,
        scratch_shapes=[pltpu.VMEM((CHUNK, width), BF16), pltpu.VMEM((UNPACK_STEP, width), F32), pltpu.SemaphoreType.DMA],
        compiler_params=params(),
        cost_estimate=pl.CostEstimate(flops=2 * CHUNK * n * width, bytes_accessed=4 * n * width, transcendentals=0),
        name='unpack',
    )(n_chunks.reshape(1), pos.reshape(steps, UNPACK_STEP), gate.reshape(steps, UNPACK_STEP), *([h] if weighted else []), first, more)


QUERY_BLOCK = 256


def peers():
    f, e = lax.axis_index('fsdp'), lax.axis_index('ep')
    core = e + 1 - 2 * (e % 2)
    return (f, e), (1 - f, e), (f, (e + 2) % 4), (f, core), (1 - f, (e + 2) % 4), (1 - f, core), (f, (core + 2) % 4), (1 - f, (core + 2) % 4)


def rank(dev):
    return dev[0] * 4 + dev[1]


def meet_neighbours():
    me, y, x, core, *_ = peers()
    barrier = pltpu.get_barrier_semaphore()
    for dev in (y, x, core):
        pl.semaphore_signal(barrier, inc=1, device_id={'fsdp': dev[0], 'ep': dev[1]}, device_id_type=MESH)
    pl.semaphore_wait(barrier, 3)


def remote(src, dst, dev, sems, i):
    return pltpu.make_async_remote_copy(src, dst, sems.at[0, i], sems.at[1, i], device_id={'fsdp': dev[0], 'ep': dev[1]}, device_id_type=MESH)


class Gather:
    def __init__(self, own, out, sems):
        me, y, x, core, xy, *_ = peers()

        def flow(i, src, owner, dev):
            return remote(src, out.at[rank(owner)], dev, sems, i)

        self.flows = [
            flow(0, own, me, y),
            flow(1, own, me, x),
            flow(2, own, me, core),
            flow(3, out.at[rank(y)], y, x),
            flow(4, out.at[rank(y)], y, core),
            flow(5, out.at[rank(x)], x, core),
            flow(6, out.at[rank(xy)], xy, core),
        ]
        self.local = pltpu.make_async_copy(own, out.at[rank(me)], sems.at[0, 7])

    def start(self):
        for i in range(3):
            self.flows[i].start()
        self.local.start()

    def forward_y(self):
        self.flows[0].wait_recv()
        self.flows[3].start()
        self.flows[4].start()

    def forward_x(self):
        self.flows[1].wait_recv()
        self.flows[5].start()

    def forward_xy(self):
        self.flows[3].wait_recv()
        self.flows[6].start()

    def finish(self):
        for i in (2, 4, 5, 6):
            self.flows[i].wait_recv()
        for flow in self.flows:
            flow.wait_send()
        self.local.wait()

    def run(self):
        self.start()
        self.forward_y()
        self.forward_x()
        self.forward_xy()
        self.finish()


def attention_weight_flows(wq_hbm, wo_hbm, wqkv, wo, sems):
    me, y, x, core, xy, _, _, _ = peers()
    hw = wq_hbm.shape[0]
    quarter = hw // 4

    def pieces(dev):
        return wqkv.at[pl.ds(dev[0] * hw + dev[1] * quarter, quarter), :], wo.at[dev[0], pl.ds(dev[1] * 2 * quarter, 2 * quarter), :]

    mine = wq_hbm.at[pl.ds(me[1] * quarter, quarter), :], wo_hbm.at[pl.ds(me[1] * 2 * quarter, 2 * quarter), :]
    flows = []
    for part in range(2):
        flows.append([
            remote(mine[part], pieces(me)[part], y, sems, part),
            remote(pieces(y)[part], pieces(y)[part], x, sems, 2 + part),
            remote(pieces(y)[part], pieces(y)[part], core, sems, 4 + part),
            remote(pieces(xy)[part], pieces(xy)[part], core, sems, 6 + part),
        ])
    return flows


def load_attention_weights(wqkv_hbm, wo_hbm, wqkv, wo, sems):
    copies = [pltpu.make_async_copy(wqkv_hbm, wqkv, sems.at[0]), pltpu.make_async_copy(wo_hbm, wo, sems.at[1])]
    for cp in copies:
        cp.start()
    for cp in copies:
        cp.wait()


class WeightPieces:
    def __init__(self, own, send, part, outs, sems, n):
        y = peers()[1]
        gate, up, down = own
        r13, r2 = outs
        hw, size = gate.shape[1], r2.shape[0]
        cols = pl.ds(part * size, size)
        step, step2 = hw // n, size // n
        self.pieces = []
        for i in range(n):
            rows = pl.ds(i * step, step)
            self.pieces.append([
                remote(gate.at[send, rows, cols], r13.at[rows, :], y, sems, 3 * i),
                remote(up.at[send, rows, cols], r13.at[pl.ds(hw + i * step, step), :], y, sems, 3 * i + 1),
                remote(down.at[send, pl.ds(part * size + i * step2, step2), :], r2.at[pl.ds(i * step2, step2), :], y, sems, 3 * i + 2),
            ])

    def start(self, i):
        for cp in self.pieces[i]:
            cp.start()

    def finish(self):
        for piece in self.pieces:
            for cp in piece:
                cp.wait()


def inv_rms_of(wide_vals):
    return lax.rsqrt(jnp.mean(wide_vals * wide_vals, axis=-1, keepdims=True) + 1e-6)


def head_lanes(shape, axis, head):
    lane = lax.broadcasted_iota(jnp.int32, shape, axis)
    return lane < 64 if head == 0 else lane >= 64


def causal_tail(values, fill):
    n, k = values.shape
    tail = values[:, k - n :]
    keep = lax.broadcasted_iota(jnp.int32, (n, n), 0) >= lax.broadcasted_iota(jnp.int32, (n, n), 1)
    tail = jnp.where(keep, tail, fill)
    return tail if k == n else jnp.concatenate([values[:, : k - n], tail], axis=1)


def attn_fwd_kernel(pos_ref, cnt_hbm, dy_hbm, wq_hbm, wo_hbm, gate_hbm, up_hbm, down_hbm, x_ref, *refs):
    h_ref, u_ref, qkv_ref, ctx_ref, p0_ref, p1_ref, wqkv_out, wo_out, cnt_all, dy_all, u_all, a0, b0, a1, b1 = refs[:15]
    wqkv, wo, acc, u_pack, sem_a, sem_c, sem_d, sem_u, sem_0, sem_1, sem_w = refs[15:]
    i = pl.program_id(0)
    width = x_ref.shape[1]
    hw = width // 2
    seq = x_ref.shape[0]
    me = peers()[0]
    own = gate_hbm, up_hbm, down_hbm
    counts, dys, us = Gather(cnt_hbm, cnt_all, sem_c), Gather(dy_hbm, dy_all, sem_d), Gather(u_pack, u_all, sem_u)
    part0 = WeightPieces(own, 1 - me[0], 0, (a0, b0), sem_0, 1)
    part1 = WeightPieces(own, 1 - me[0], 1, (a1, b1), sem_1, 4)
    flows = attention_weight_flows(wq_hbm, wo_hbm, wqkv, wo, sem_a)
    local = [
        pltpu.make_async_copy(wq_hbm, wqkv.at[pl.ds(me[0] * hw, hw), :], sem_w.at[0]),
        pltpu.make_async_copy(wo_hbm, wo.at[me[0]], sem_w.at[1]),
    ]
    keep = [pltpu.make_async_copy(wqkv, wqkv_out, sem_w.at[2]), pltpu.make_async_copy(wo, wo_out, sem_w.at[3])]

    @pl.when(i == 0)
    def _():
        meet_neighbours()
        for cps in flows:
            cps[0].start()
        for cp in local:
            cp.start()
        counts.start()
        for cps in flows:
            cps[0].wait_recv()
            cps[1].start()
            cps[2].start()
        dys.start()
        part0.start(0)
        for cps in flows:
            cps[1].wait_recv()
            cps[3].start()
        for cps in flows:
            cps[2].wait_recv()
            cps[3].wait_recv()
            for cp in cps:
                cp.wait_send()
        for cp in local:
            cp.wait()
        for cp in keep:
            cp.start()

    @pl.when(i == 2)
    def _():
        counts.forward_y()
        counts.forward_x()
        dys.forward_y()
        dys.forward_x()

    @pl.when(i == 4)
    def _():
        counts.forward_xy()
        dys.forward_xy()

    for n in range(4):
        @pl.when(i == 3 + n)
        def _(n=n):
            part1.start(n)

    x = x_ref[...].astype(F32)
    normed = (x * inv_rms_of(x)).astype(BF16)
    for t in range(3):
        cols = slice(t * width, (t + 1) * width)
        qkv_ref[:, cols] = mm(normed, wqkv[:, cols]).astype(BF16)
    for pair in range(width // 128):
        lanes = slice(pair * 128, (pair + 1) * 128)
        q = qkv_ref[:, lanes] * jnp.asarray(0.125, BF16)
        k = qkv_ref[:, width + pair * 128 : width + (pair + 1) * 128]
        v = qkv_ref[:, 2 * width + pair * 128 : 2 * width + (pair + 1) * 128]
        for j in range(seq // QUERY_BLOCK):
            rows = slice(j * QUERY_BLOCK, (j + 1) * QUERY_BLOCK)
            keys = slice(0, (j + 1) * QUERY_BLOCK)
            outs = []
            for head in range(2):
                qm = jnp.where(head_lanes((QUERY_BLOCK, 128), 1, head), q[rows], jnp.zeros((), BF16))
                s = causal_tail(mm(qm, k[keys], NT), -1e30)
                top = jnp.max(s, axis=1, keepdims=True)
                e = jnp.exp(s - top)
                total = jnp.sum(e, axis=1, keepdims=True)
                p = (e * (1.0 / total)).astype(BF16)
                (p0_ref, p1_ref)[j][0, pair * 2 + head] = p
                outs.append(mm(p, v[keys]))
            ctx_ref[rows, lanes] = jnp.where(head_lanes((QUERY_BLOCK, 128), 1, 0), outs[0], outs[1]).astype(BF16)
    ctx = ctx_ref[...]
    for f in range(2):
        cols = slice(f * hw, (f + 1) * hw)
        h_ref[:, cols] = (x_ref[:, cols].astype(F32) + mm(ctx, wo[f])).astype(BF16)
    h = h_ref[...].astype(F32)
    u = (h * inv_rms_of(h)).astype(BF16)
    u_ref[...] = u
    hit = lax.broadcasted_iota(jnp.int32, (CHUNK, seq), 0) == pos_ref[pl.ds(i, 1), :]
    part = mm(jnp.where(hit, 1.0, 0.0).astype(BF16), u)

    @pl.when(i == 0)
    def _():
        acc[...] = part

    @pl.when(i > 0)
    def _():
        acc[...] += part

    @pl.when(i == pl.num_programs(0) - 1)
    def _():
        u_pack[...] = acc[...].astype(BF16)
        us.run()
        counts.finish()
        dys.finish()
        part0.finish()
        part1.finish()
        for cp in keep:
            cp.wait()


def probs_shapes(n_seq, width):
    return [jax.ShapeDtypeStruct((n_seq, width // 64, QUERY_BLOCK, (j + 1) * QUERY_BLOCK), BF16) for j in range(2)]


def probs_specs(width):
    return [pl.BlockSpec((1, width // 64, QUERY_BLOCK, (j + 1) * QUERY_BLOCK), lambda i: (i, 0, 0, 0)) for j in range(2)]


def attn_fwd(pos, cnt, dy, wq, wo, own, x, n_seq):
    n, width = x.shape
    seq = n // n_seq
    hw = width // 2
    size = own[0].shape[2] // N_PARTS
    rows = pl.BlockSpec((seq, width), lambda i: (i, 0))
    part = [jax.ShapeDtypeStruct((width, size), BF16), jax.ShapeDtypeStruct((size, hw), BF16)]
    sems = lambda k: pltpu.SemaphoreType.DMA((2, k))
    h, u, qkv, ctx, p0, p1, *rest = pl.pallas_call(
        attn_fwd_kernel,
        grid=(n_seq,),
        out_shape=(
            jax.ShapeDtypeStruct((n, width), BF16),
            jax.ShapeDtypeStruct((n, width), BF16),
            jax.ShapeDtypeStruct((n, 3 * width), BF16),
            jax.ShapeDtypeStruct((n, width), BF16),
            *probs_shapes(n_seq, width),
            jax.ShapeDtypeStruct((width, 3 * width), BF16),
            jax.ShapeDtypeStruct((2, width, hw), BF16),
            jax.ShapeDtypeStruct((8, 1, 128), jnp.int32),
            jax.ShapeDtypeStruct((8, CHUNK, width), BF16),
            jax.ShapeDtypeStruct((8, CHUNK, width), BF16),
            *part,
            *part,
        ),
        in_specs=[pl.BlockSpec((n_seq, seq), lambda i: (0, 0))] + [ANY] * 7 + [rows],
        out_specs=(rows, rows, pl.BlockSpec((seq, 3 * width), lambda i: (i, 0)), rows, *probs_specs(width)) + (ANY,) * 9,
        scratch_shapes=[
            pltpu.VMEM((width, 3 * width), BF16),
            pltpu.VMEM((2, width, hw), BF16),
            pltpu.VMEM((CHUNK, width), F32),
            pltpu.VMEM((CHUNK, width), BF16),
            sems(8),
            sems(8),
            sems(8),
            sems(8),
            sems(3),
            sems(12),
            pltpu.SemaphoreType.DMA((4,)),
        ],
        compiler_params=pltpu.CompilerParams(vmem_limit_bytes=60 * 1024 * 1024, collective_id=0, has_side_effects=True),
        cost_estimate=pl.CostEstimate(flops=30 * 10**9, bytes_accessed=50 * 2**20, transcendentals=0),
        name='attn_fwd',
    )(pos.reshape(n_seq, seq), cnt, dy, wq, wo, *own, x)
    return (h, u, qkv, ctx, (p0, p1)), rest


def norm_back(grad, wide_vals):
    inv = inv_rms_of(wide_vals)
    return inv * (grad - wide_vals * (inv * inv * jnp.mean(grad * wide_vals, axis=-1, keepdims=True)))


def attn_bwd_kernel(n_ref, pos_ref, first_ref, more_hbm, wqkv_hbm, wo_hbm, x_ref, h_ref, dout_ref, qkv_ref, ctx_ref, p0_ref, p1_ref, dx_ref, wqkv, wo, dqkv, dctx, dh, buf, sem, w_sem):
    i = pl.program_id(0)
    seq, width = x_ref.shape
    hw = width // 2

    @pl.when(i == 0)
    def _():
        load_attention_weights(wqkv_hbm, wo_hbm, wqkv, wo, w_sem)

    pos = pos_ref[pl.ds(i, 1), :]
    row = lax.broadcasted_iota(jnp.int32, (CHUNK, seq), 0)

    def gathered(base, rows):
        return mm(jnp.where(row + base == pos, 1.0, 0.0).astype(BF16), rows, TN)

    dh[...] = gathered(0, first_ref[...])

    def more(c, carry):
        copy = pltpu.make_async_copy(more_hbm.at[c - 1], buf, sem)
        copy.start()
        copy.wait()
        dh[...] += gathered(c * CHUNK, buf[...])
        return carry

    lax.fori_loop(1, n_ref[0], more, 0)
    dh[...] = dout_ref[...].astype(F32) + norm_back(dh[...], h_ref[...].astype(F32))
    dh_b = dh[...].astype(BF16)
    dctx[...] = (mm(dh_b[:, :hw], wo[0], NT) + mm(dh_b[:, hw:], wo[1], NT)).astype(BF16)
    zero = jnp.zeros((), BF16)
    for pair in range(width // 128):
        lanes = slice(pair * 128, (pair + 1) * 128)
        k_lanes = slice(width + pair * 128, width + (pair + 1) * 128)
        v_lanes = slice(2 * width + pair * 128, 2 * width + (pair + 1) * 128)
        q = qkv_ref[:, lanes] * jnp.asarray(0.125, BF16)
        k, v = qkv_ref[:, k_lanes], qkv_ref[:, v_lanes]
        do = dctx[:, lanes]
        q_t, do_t = q.T, do.T
        prod = do.astype(F32) * ctx_ref[:, lanes].astype(F32)
        dk_t = [jnp.zeros((128, QUERY_BLOCK), F32) for _ in range(seq // QUERY_BLOCK)]
        dv_t = list(dk_t)
        for j in range(seq // QUERY_BLOCK):
            rows = slice(j * QUERY_BLOCK, (j + 1) * QUERY_BLOCK)
            keys = slice(0, (j + 1) * QUERY_BLOCK)
            dqs = []
            for head in range(2):
                mine = head_lanes((QUERY_BLOCK, 128), 1, head)
                mine_t = head_lanes((128, QUERY_BLOCK), 0, head)
                dom = jnp.where(mine, do[rows], zero)
                delta = jnp.sum(jnp.where(mine, prod[rows], 0.0), axis=1, keepdims=True)
                pb = (p0_ref, p1_ref)[j][0, pair * 2 + head]
                dp = mm(dom, v[keys], NT)
                ds = (pb.astype(F32) * (dp - delta)).astype(BF16)
                dqs.append(mm(ds, k[keys]))
                qm_t, dom_t = jnp.where(mine_t, q_t[:, rows], zero), jnp.where(mine_t, do_t[:, rows], zero)
                dk_part, dv_part = mm(qm_t, ds), mm(dom_t, pb)
                for c in range(j + 1):
                    cols = slice(c * QUERY_BLOCK, (c + 1) * QUERY_BLOCK)
                    dk_t[c] = dk_t[c] + dk_part[:, cols]
                    dv_t[c] = dv_t[c] + dv_part[:, cols]
            dqkv[rows, lanes] = (jnp.where(head_lanes((QUERY_BLOCK, 128), 1, 0), dqs[0], dqs[1]) * 0.125).astype(BF16)
        for c in range(seq // QUERY_BLOCK):
            rows = slice(c * QUERY_BLOCK, (c + 1) * QUERY_BLOCK)
            dqkv[rows, k_lanes] = dk_t[c].astype(BF16).T
            dqkv[rows, v_lanes] = dv_t[c].astype(BF16).T
    dn = mm(dqkv[...], wqkv[...], NT)
    dx_ref[...] = (dh[...] + norm_back(dn, x_ref[...].astype(F32))).astype(BF16)


def attn_bwd(n_chunks, pos, first, more, wqkv, wo, x, h, dout, qkv, ctx, probs, n_seq):
    n, width = x.shape
    seq = n // n_seq
    rows = pl.BlockSpec((seq, width), lambda i: (i, 0))
    return pl.pallas_call(
        attn_bwd_kernel,
        grid=(n_seq,),
        out_shape=jax.ShapeDtypeStruct((n, width), BF16),
        in_specs=[SMEM, pl.BlockSpec((n_seq, seq), lambda i: (0, 0)), pl.BlockSpec((CHUNK, width), lambda i: (0, 0)), ANY, ANY, ANY, rows, rows, rows, pl.BlockSpec((seq, 3 * width), lambda i: (i, 0)), rows, *probs_specs(width)],
        out_specs=rows,
        scratch_shapes=[
            pltpu.VMEM((width, 3 * width), BF16),
            pltpu.VMEM((2, width, width // 2), BF16),
            pltpu.VMEM((seq, 3 * width), BF16),
            pltpu.VMEM((seq, width), BF16),
            pltpu.VMEM((seq, width), F32),
            pltpu.VMEM((CHUNK, width), BF16),
            pltpu.SemaphoreType.DMA,
            pltpu.SemaphoreType.DMA((2,)),
        ],
        compiler_params=params(),
        cost_estimate=pl.CostEstimate(flops=50 * 10**9, bytes_accessed=60 * 2**20, transcendentals=0),
        name='attn_bwd',
    )(n_chunks.reshape(1), pos.reshape(n_seq, seq), first, more, wqkv, wo, x, h, dout, qkv, ctx, *probs)


def experts_kernel(back, first, last, f_base, n_src, cnt_ref, prm_ref, u_hbm, dy_hbm, w1_hbm, w3_hbm, w2_hbm, r13_hbm, r2_hbm, i1, i3, i2, *refs):
    if back:
        o1, o3, o2, y_part, du_part = refs[2:7]
        scratch = refs[7:]
        if last:
            (y_hbm, du_hbm), scratch = scratch[:2], scratch[2:]
        y_acc, du_acc, stage, zero, row_sem, part_sem = scratch[-6:]
        scratch = scratch[:-6]
    else:
        o1, o3, o2 = refs[:3]
        scratch = refs[3:]
    u_s, dy_s, ut_s, dyt_s, w1_s, w3_s, w2_s, d1_s, d3_s, d2_s, d2t_s, lst, load_sem, w_sem, d_sem = scratch
    expert, local, half, chunk, add_first = prm_ref[0], prm_ref[1], prm_ref[2], prm_ref[3], prm_ref[4]
    width = u_s.shape[1]
    hw = width // 2
    n_ff = r2_hbm.shape[0] // FF_STEP
    first_tile = chunk * CHUNK_TILES
    own_rows = pl.ds(pl.multiple_of(half * hw, hw), hw)
    got_rows = pl.ds(pl.multiple_of((1 - half) * hw, hw), hw)

    if back and last:
        def unmark(t, carry):
            lst[1, t] = 0
            return carry

        lax.fori_loop(0, n_src * CHUNK_TILES, unmark, 0)
    total = jnp.int32(0)
    for s in range(n_src):
        off, own = jnp.int32(0), jnp.int32(0)
        for e in range(n_src):
            tiles = (cnt_ref[s, e] + (TILE - 1)) // TILE
            off = off + jnp.where(e < expert, tiles, 0)
            own = own + jnp.where(e == expert, tiles, 0)
        lo = jnp.clip(off - first_tile, 0, CHUNK_TILES)
        hi = jnp.clip(off + own - first_tile, 0, CHUNK_TILES)

        def note(j, t, s=s):
            lst[0, t] = s * CHUNK_TILES + j
            if back and last:
                lst[1, s * CHUNK_TILES + j] = 1
            return t + 1

        total = lax.fori_loop(lo, hi, note, total)

    def tile_of(ref, t):
        return ref.at[t // CHUNK_TILES, pl.ds(pl.multiple_of((t % CHUNK_TILES) * TILE, TILE), TILE), :]

    if back and last:
        zero[...] = jnp.zeros_like(zero)

        def clear(t, n):
            @pl.when(lst[1, t] == 0)
            def _():
                pltpu.make_async_copy(zero, tile_of(y_hbm, t), row_sem).start()
                pltpu.make_async_copy(zero, tile_of(du_hbm, t), row_sem).start()

            return n

        lax.fori_loop(0, n_src * CHUNK_TILES, clear, 0)

    def weights(f, slot):
        cols = pl.ds(pl.multiple_of(f_base + f * FF_STEP, FF_STEP), FF_STEP)
        part = pl.ds(pl.multiple_of(f * FF_STEP, FF_STEP), FF_STEP)
        pairs = [
            (w1_hbm.at[local, :, cols], w1_s.at[slot, own_rows, :]),
            (r13_hbm.at[pl.ds(0, hw), part], w1_s.at[slot, got_rows, :]),
            (w3_hbm.at[local, :, cols], w3_s.at[slot, own_rows, :]),
            (r13_hbm.at[pl.ds(hw, hw), part], w3_s.at[slot, got_rows, :]),
            (w2_hbm.at[local, cols, :], w2_s.at[slot, :, own_rows]),
            (r2_hbm.at[part, :], w2_s.at[slot, :, got_rows]),
        ]
        return [pltpu.make_async_copy(src, dst, w_sem.at[slot, i]) for i, (src, dst) in enumerate(pairs)]

    def grads(f, slot, ins):
        cols = pl.ds(pl.multiple_of(f_base + f * FF_STEP, FF_STEP), FF_STEP)
        hbm = (i1, i3, i2) if ins else (o1, o3, o2)
        pairs = [
            (hbm[0].at[local, :, cols], d1_s.at[slot]),
            (hbm[1].at[local, :, cols], d3_s.at[slot]),
            (hbm[2].at[local, cols, :], d2_s.at[slot]),
        ]
        if not ins:
            pairs = [(b, a) for a, b in pairs]
        return [pltpu.make_async_copy(src, dst, d_sem.at[slot, i]) for i, (src, dst) in enumerate(pairs)]

    def one_pass(p, carry):
        for cp in weights(0, 0):
            cp.start()
        n_tiles = jnp.clip(total - p * PASS_TILES, 0, PASS_TILES)
        n_blk = (n_tiles + (CHUNK_TILES - 1)) // CHUNK_TILES

        def rows_at(k):
            return pl.ds(pl.multiple_of(k * TILE, TILE), TILE)

        def load(k, carry):
            t = lst[0, p * PASS_TILES + k]
            pltpu.make_async_copy(tile_of(u_hbm, t), u_s.at[rows_at(k), :], load_sem).start()
            pltpu.make_async_copy(tile_of(dy_hbm, t), dy_s.at[rows_at(k), :], load_sem).start()
            return carry

        lax.fori_loop(0, n_tiles, load, 0)

        def partial_sums(b, out):
            rows = pl.ds(pl.multiple_of(b * CHUNK, CHUNK), CHUNK)
            hbm_rows = pl.ds(pl.multiple_of((p * (PASS_TILES // CHUNK_TILES) + b) * CHUNK, CHUNK), CHUNK)
            pairs = [(y_acc.at[rows, :], y_part.at[hbm_rows, :]), (du_acc.at[rows, :], du_part.at[hbm_rows, :])]
            return [pltpu.make_async_copy(*(pair if out else pair[::-1]), part_sem) for pair in pairs]

        def each_block(out, action):
            def go(b, carry):
                for cp in partial_sums(b, out):
                    getattr(cp, action)()
                return carry

            lax.fori_loop(0, n_blk, go, 0)

        if back and not first:
            each_block(False, 'start')

        def fill(k, carry):
            u_s[rows_at(k), :] = jnp.zeros((TILE, width), BF16)
            dy_s[rows_at(k), :] = jnp.zeros((TILE, width), BF16)
            return carry

        lax.fori_loop(n_tiles, n_blk * CHUNK_TILES, fill, 0)

        def loaded(k, carry):
            pltpu.make_async_copy(tile_of(u_hbm, 0), u_s.at[rows_at(k), :], load_sem).wait()
            pltpu.make_async_copy(tile_of(dy_hbm, 0), dy_s.at[rows_at(k), :], load_sem).wait()
            return carry

        lax.fori_loop(0, n_tiles, loaded, 0)

        def flip(k, carry):
            ut_s[:, rows_at(k)] = u_s[rows_at(k), own_rows].T
            dyt_s[:, rows_at(k)] = dy_s[rows_at(k), own_rows].T
            return carry

        lax.fori_loop(0, n_blk * CHUNK_TILES, flip, 0)
        if back and not first:
            each_block(False, 'wait')
        add = jnp.logical_or(p > 0, add_first > 0)

        def step(f, carry):
            slot = f % 2

            @pl.when(f + 1 < n_ff)
            def _():
                for cp in weights(f + 1, 1 - slot):
                    cp.start()

            @pl.when(f >= 2)
            def _():
                for cp in grads(f - 2, slot, False):
                    cp.wait()

            for cp in weights(f, slot):
                cp.wait()

            d1_s[slot] = jnp.zeros((hw, FF_STEP), F32)
            d3_s[slot] = jnp.zeros((hw, FF_STEP), F32)
            d2t_s[...] = jnp.zeros((hw, FF_STEP), F32)

            @pl.when(add)
            def _():
                for cp in grads(f, slot, True):
                    cp.start()
                for cp in grads(f, slot, True):
                    cp.wait()
                d2t_s[...] = d2_s[slot].T

            def block(b, carry):
                rows = pl.ds(pl.multiple_of(b * CHUNK, CHUNK), CHUNK)
                w1, w3, w2 = w1_s[slot], w3_s[slot], w2_s[slot]
                u, dy = u_s[rows, :], dy_s[rows, :]
                act_a = mm(u, w1)
                act_b = mm(u, w3)
                d_g = mm(dy, w2, NT)
                sig = 0.5 * jnp.tanh(0.5 * act_a) + 0.5
                silu = act_a * sig
                g = (silu * act_b).astype(BF16)
                d_b = (d_g * silu).astype(BF16)
                d_a = (d_g * act_b * (sig + silu * (1.0 - sig))).astype(BF16)
                if back:
                    y = mm(g, w2)
                    du = mm(d_a, w1, NT) + mm(d_b, w3, NT)

                    if first:
                        @pl.when(f == 0)
                        def _():
                            y_acc[rows, :] = y
                            du_acc[rows, :] = du

                        @pl.when(f > 0)
                        def _():
                            y_acc[rows, :] += y
                            du_acc[rows, :] += du
                    else:
                        y_acc[rows, :] += y
                        du_acc[rows, :] += du

                d1_s[slot] += mm(ut_s[:, rows], d_a)
                d3_s[slot] += mm(ut_s[:, rows], d_b)
                d2t_s[...] += mm(dyt_s[:, rows], g)
                return carry

            lax.fori_loop(0, n_blk, block, 0)
            d2_s[slot] = d2t_s[...].T
            for cp in grads(f, slot, False):
                cp.start()
            return carry

        lax.fori_loop(0, n_ff, step, 0)
        if back and not last:
            each_block(True, 'start')
            each_block(True, 'wait')
        if back and last:
            def put(k, carry):
                t = lst[0, p * PASS_TILES + k]
                stage[0, rows_at(k), :] = y_acc[rows_at(k), :].astype(BF16)
                stage[1, rows_at(k), :] = du_acc[rows_at(k), :].astype(BF16)
                pltpu.make_async_copy(stage.at[0, rows_at(k), :], tile_of(y_hbm, t), row_sem).start()
                pltpu.make_async_copy(stage.at[1, rows_at(k), :], tile_of(du_hbm, t), row_sem).start()
                return carry

            lax.fori_loop(0, n_tiles, put, 0)

            def done(k, carry):
                pltpu.make_async_copy(zero, tile_of(y_hbm, 0), row_sem).wait()
                pltpu.make_async_copy(zero, tile_of(du_hbm, 0), row_sem).wait()
                return carry

            lax.fori_loop(0, n_tiles, done, 0)
        for f in (n_ff - 2, n_ff - 1):
            for cp in grads(f, f % 2, False):
                cp.wait()
        return carry

    n_pass = jnp.maximum((total + (PASS_TILES - 1)) // PASS_TILES, 1)
    lax.fori_loop(0, n_pass, one_pass, 0)
    if back and last:
        def cleared(t, carry):
            pltpu.make_async_copy(zero, tile_of(y_hbm, 0), row_sem).wait()
            pltpu.make_async_copy(zero, tile_of(du_hbm, 0), row_sem).wait()
            return carry

        lax.fori_loop(0, n_src * CHUNK_TILES - total, cleared, 0)


def experts(back, part, n_parts, counts, prm, u_all, dy_all, own, got, dws, sums=()):
    n_src, _, width = u_all.shape
    first, last = part == 0, part == n_parts - 1
    hw = width // 2
    ff = got[1].shape[0]
    rows = PASS_TILES * TILE
    scratch = [
        pltpu.VMEM((rows, width), BF16),
        pltpu.VMEM((rows, width), BF16),
        pltpu.VMEM((hw, rows), BF16),
        pltpu.VMEM((hw, rows), BF16),
        pltpu.VMEM((2, width, FF_STEP), BF16),
        pltpu.VMEM((2, width, FF_STEP), BF16),
        pltpu.VMEM((2, FF_STEP, width), BF16),
        pltpu.VMEM((2, hw, FF_STEP), F32),
        pltpu.VMEM((2, hw, FF_STEP), F32),
        pltpu.VMEM((2, FF_STEP, hw), F32),
        pltpu.VMEM((hw, FF_STEP), F32),
        pltpu.SMEM((2, n_src * CHUNK_TILES), jnp.int32),
        pltpu.SemaphoreType.DMA,
        pltpu.SemaphoreType.DMA((2, 6)),
        pltpu.SemaphoreType.DMA((2, 3)),
    ]
    outs = [jax.ShapeDtypeStruct(d.shape, d.dtype) for d in (*dws, *sums)]
    n_alias = len(outs)
    if back and last:
        outs += [jax.ShapeDtypeStruct(u_all.shape, BF16)] * 2
    if back:
        scratch += [
            pltpu.VMEM((rows, width), F32),
            pltpu.VMEM((rows, width), F32),
            pltpu.VMEM((2, rows, width), BF16),
            pltpu.VMEM((TILE, width), BF16),
            pltpu.SemaphoreType.DMA,
            pltpu.SemaphoreType.DMA,
        ]
    units = 7.5 if back else 4.5
    return pl.pallas_call(
        functools.partial(experts_kernel, back, first, last, part * ff, n_src),
        out_shape=tuple(outs),
        in_specs=[SMEM, SMEM] + [ANY] * (7 + n_alias),
        out_specs=tuple([ANY] * len(outs)),
        scratch_shapes=scratch,
        input_output_aliases={9 + i: i for i in range(n_alias)},
        compiler_params=params(),
        cost_estimate=pl.CostEstimate(flops=int(units * 2 * 2 * CHUNK * width * ff), bytes_accessed=10 * 2**20, transcendentals=0),
    )(counts, prm, u_all, dy_all, *own, *got, *dws, *sums)


def unset_kernel(*refs):
    pass


def unset(*shapes):
    outs = tuple(jax.ShapeDtypeStruct(s, d) for s, d in shapes)
    return pl.pallas_call(unset_kernel, out_shape=outs, out_specs=tuple([ANY] * len(outs)), name='unset')()


def solution(mesh):
    n_dev = mesh.shape['fsdp'] * mesh.shape['ep']
    tok_spec = P(('data', 'fsdp', 'ep'))
    in_specs = (tok_spec, P('fsdp'), P(None, None, 'fsdp'), P('ep', 'fsdp'), P('ep', 'fsdp'), P('ep', None, 'fsdp'), tok_spec, tok_spec, tok_spec, tok_spec)
    out_specs = (tok_spec, tok_spec, P(('data', 'ep'), 'fsdp'), P(('data', 'ep'), 'fsdp'), P(('data', 'ep'), None, 'fsdp'))

    def device_fn(tokens, w_qkv, w_out, w_gate, w_up, w_down, expert_idx, expert_slot, gate_wts, d_out):
        n_seq, seq_len, d_model = tokens.shape
        n_tok = n_seq * seq_len
        n_exp = n_dev
        half = lax.axis_index('fsdp').astype(jnp.int32)
        col = lax.axis_index('ep').astype(jnp.int32)
        swap = [(0, 1), (1, 0)]
        own = (w_gate, w_up, w_down)

        def other(local, r):
            gate, up, down = [lax.dynamic_index_in_dim(w, local, 0, keepdims=False) for w in own]
            size = down.shape[0] // N_PARTS
            cols = slice(r * size, (r + 1) * size)
            both = lax.ppermute(jnp.concatenate([gate[:, cols], up[:, cols]], axis=0), 'fsdp', swap)
            return both, lax.ppermute(down[cols], 'fsdp', swap)

        def back(chunk, add, u_c, dy_c, dws):
            sums = unset(*[((n_dev * CHUNK, d_model), F32)] * 2)
            for r in range(N_PARTS):
                *state, = experts(True, r, N_PARTS, counts, prm(half, chunk, add), u_c, dy_c, own, got_mine[r], dws, sums)
                dws, sums = state[:3], state[3:5]
            return dws, state[5], state[6]

        def grad_part(r, chunk, add, u_c, dy_c, dws):
            return experts(False, r, N_PARTS, counts, prm(1 - half, chunk, add), u_c, dy_c, own, got_rest[r], dws)

        def prm(local, chunk, add):
            return jnp.stack([2 * col + local, local, half, chunk, add]).astype(jnp.int32)

        x_tok = tokens.reshape(n_tok, d_model)
        dout_tok = d_out.reshape(n_tok, d_model)
        gate = gate_wts.reshape(n_tok // PACK_STEP, PACK_STEP).astype(F32)
        zero = jnp.int32(0)
        pos, cnt = route(expert_idx, expert_slot, n_exp)
        dy_pack = pack(zero, pos, gate, dout_tok, True)
        wq = w_qkv.reshape(d_model // 2, 3 * d_model)
        (h_tok, u_tok, qkv, ctx, probs), gathered = attn_fwd(pos, cnt, dy_pack, wq, w_out.reshape(d_model, d_model // 2), own, x_tok, n_seq)
        wqkv_full, wo_full, counts, dy_all, u_all, a0, b0, a1, b1 = gathered
        counts = counts.reshape(n_exp, 128)
        got_mine = [(a0, b0), (a1, b1), other(1 - half, 2)]
        got_rest = [other(half, r) for r in range(N_PARTS)]

        tiles = (counts[:, :n_exp] + (TILE - 1)) // TILE
        n_chunks = jnp.max((jnp.sum(tiles, axis=1) + (CHUNK_TILES - 1)) // CHUNK_TILES)
        max_more = (n_tok + n_exp * (TILE - 1)) // CHUNK

        dws = unset(*[(w.shape, F32) for w in own])
        more_y, more_du = unset(*[((max_more, CHUNK, d_model), BF16)] * 2)
        dws, y_all, du_all = back(zero, zero, u_all, dy_all, dws)
        first_du = lax.psum_scatter(du_all, GROUP, scatter_dimension=0)

        first_y = lax.psum_scatter(y_all, GROUP, scatter_dimension=0)

        def fetch(c):
            return lax.all_gather(pack(c, pos, gate, u_tok, False), GROUP), lax.all_gather(pack(c, pos, gate, dout_tok, True), GROUP)

        def more_back(state):
            c, d1, d3, d2, ys, dus = state
            u_c, dy_c = fetch(c)
            (d1, d3, d2), y_c, du_c = back(c, jnp.int32(1), u_c, dy_c, (d1, d3, d2))
            y_c = lax.psum_scatter(y_c, GROUP, scatter_dimension=0)
            du_c = lax.psum_scatter(du_c, GROUP, scatter_dimension=0)
            ys = lax.dynamic_update_index_in_dim(ys, y_c, c - 1, 0)
            dus = lax.dynamic_update_index_in_dim(dus, du_c, c - 1, 0)
            return c + 1, d1, d3, d2, ys, dus

        def more_grad(state):
            c, d1, d3, d2 = state
            u_c, dy_c = fetch(c)
            dws = (d1, d3, d2)
            for r in range(N_PARTS):
                dws = grad_part(r, c, jnp.int32(1), u_c, dy_c, dws)
            return (c + 1, *dws)

        _, *dws, more_y, more_du = lax.while_loop(lambda s: s[0] < n_chunks, more_back, (jnp.int32(1), *dws, more_y, more_du))
        layer_out = unpack(n_chunks, pos, gate, h_tok, first_y, more_y).reshape(n_seq, seq_len, d_model)
        d_tokens = attn_bwd(n_chunks, pos, first_du, more_du, wqkv_full, wo_full, x_tok, h_tok, dout_tok, qkv, ctx, probs, n_seq).reshape(n_seq, seq_len, d_model)

        for r in range(N_PARTS):
            dws = grad_part(r, zero, zero, u_all, dy_all, dws)
        _, *dws = lax.while_loop(lambda s: s[0] < n_chunks, more_grad, (jnp.int32(1), *dws))
        return layer_out, d_tokens, *dws

    return jax.shard_map(device_fn, mesh=mesh, in_specs=in_specs, out_specs=out_specs, check_vma=False)
```

```python
import functools

import jax
import jax.numpy as jnp
from jax import lax
from jax.experimental import pallas as pl
from jax.experimental.pallas import tpu as pltpu
from jax.sharding import PartitionSpec as P


F32 = jnp.float32
BF16 = jnp.bfloat16
TILE = 128
CHUNK_TILES = 5
CHUNK = TILE * CHUNK_TILES
PASS_TILES = 20
FF_STEP = 512
N_PARTS = 3
GROUP = ('fsdp', 'ep')
MESH = pl.DeviceIdType.MESH
NN = (((1,), (0,)), ((), ()))
NT = (((1,), (1,)), ((), ()))
TN = (((0,), (0,)), ((), ()))


def mm(lhs, rhs, dims=NN):
    return lax.dot_general(lhs, rhs, dims, preferred_element_type=F32)


def params(limit_mib=60):
    return pltpu.CompilerParams(vmem_limit_bytes=limit_mib * 1024 * 1024)


ANY = pl.BlockSpec(memory_space=pl.ANY)
SMEM = pl.BlockSpec(memory_space=pltpu.SMEM)
VMEM = pl.BlockSpec(memory_space=pltpu.VMEM)


def route_kernel(n_exp, idx_ref, slot_ref, pos_ref, cnt_ref):
    idx, kept = idx_ref[...], slot_ref[...] >= 0
    rows, lanes = idx.shape
    upper = (lax.broadcasted_iota(jnp.int32, (lanes, lanes), 0) <= lax.broadcasted_iota(jnp.int32, (lanes, lanes), 1)).astype(F32).astype(BF16)
    lower = (lax.broadcasted_iota(jnp.int32, (rows, rows), 1) < lax.broadcasted_iota(jnp.int32, (rows, rows), 0)).astype(F32).astype(BF16)
    ones = jnp.ones((lanes, lanes), BF16)
    lane = lax.broadcasted_iota(jnp.int32, (1, lanes), 1)
    pos = jnp.full((rows, lanes), -1.0, F32)
    cnt = jnp.zeros((1, lanes), F32)
    off = jnp.zeros((1, 1), F32)
    for e in range(n_exp):
        mask = jnp.logical_and(idx == e, kept)
        wide = jnp.where(mask, 1.0, 0.0)
        mask_b = wide.astype(BF16)
        inside = mm(mask_b, upper)
        before = mm(lower, mm(mask_b, ones).astype(BF16))
        count = jnp.sum(jnp.sum(wide, axis=1, keepdims=True), axis=0, keepdims=True)
        pos = jnp.where(mask, off + before + inside - 1.0, pos)
        cnt = jnp.where(lane == e, count, cnt)
        off = off + jnp.floor((count + (TILE - 1.0)) * (1.0 / TILE)) * TILE
    pos_ref[...] = pos.astype(jnp.int32)
    cnt_ref[...] = cnt.astype(jnp.int32)


def route(idx, slot, n_exp):
    n = idx.size
    shape = (n // 128, 128)
    return pl.pallas_call(
        functools.partial(route_kernel, n_exp),
        out_shape=(jax.ShapeDtypeStruct(shape, jnp.int32), jax.ShapeDtypeStruct((1, 128), jnp.int32)),
        in_specs=[VMEM, VMEM],
        out_specs=(VMEM, VMEM),
        name='route',
    )(idx.reshape(shape), slot.reshape(shape))


PACK_STEP = 1024


def pack_kernel(weighted, c_ref, pos_ref, gate_ref, x_ref, out_ref, acc_ref):
    k = pl.program_id(0)
    row = lax.broadcasted_iota(jnp.int32, (CHUNK, PACK_STEP), 0) + c_ref[0] * CHUNK
    hit = row == pos_ref[pl.ds(k, 1), :]
    value = gate_ref[pl.ds(k, 1), :] if weighted else 1.0
    part = mm(jnp.where(hit, value, 0.0).astype(BF16), x_ref[...])

    @pl.when(k == 0)
    def _():
        acc_ref[...] = part

    @pl.when(k > 0)
    def _():
        acc_ref[...] += part

    @pl.when(k == pl.num_programs(0) - 1)
    def _():
        out_ref[...] = acc_ref[...].astype(BF16)


def pack(chunk, pos, gate, x, weighted):
    n, width = x.shape
    steps = n // PACK_STEP
    return pl.pallas_call(
        functools.partial(pack_kernel, weighted),
        grid=(steps,),
        out_shape=jax.ShapeDtypeStruct((CHUNK, width), BF16),
        in_specs=[SMEM, pl.BlockSpec((steps, PACK_STEP), lambda k: (0, 0)), pl.BlockSpec((steps, PACK_STEP), lambda k: (0, 0)), pl.BlockSpec((PACK_STEP, width), lambda k: (k, 0))],
        out_specs=pl.BlockSpec((CHUNK, width), lambda k: (0, 0)),
        scratch_shapes=[pltpu.VMEM((CHUNK, width), F32)],
        compiler_params=params(),
        cost_estimate=pl.CostEstimate(flops=2 * CHUNK * n * width, bytes_accessed=2 * n * width, transcendentals=0),
        name='pack',
    )(chunk.reshape(1), pos.reshape(steps, PACK_STEP), gate, x)


UNPACK_STEP = 512


def unpack_kernel(weighted, n_ref, pos_ref, gate_ref, *refs):
    if weighted:
        h_ref, first_ref, more_ref, out_ref, buf, acc, sem = refs
    else:
        first_ref, more_ref, out_ref, buf, acc, sem = refs
    k = pl.program_id(0)
    pos = pos_ref[pl.ds(k, 1), :]
    row = lax.broadcasted_iota(jnp.int32, (CHUNK, UNPACK_STEP), 0)
    value = gate_ref[pl.ds(k, 1), :] if weighted else 1.0

    def gathered(base, rows):
        return mm(jnp.where(row + base == pos, value, 0.0).astype(BF16), rows, TN)

    acc[...] = gathered(0, first_ref[...])

    def more(c, carry):
        copy = pltpu.make_async_copy(more_ref.at[c - 1], buf, sem)
        copy.start()
        copy.wait()
        acc[...] += gathered(c * CHUNK, buf[...])
        return carry

    lax.fori_loop(1, n_ref[0], more, 0)
    total = acc[...]
    if weighted:
        total = h_ref[...].astype(F32) + total
    out_ref[...] = total.astype(BF16)


def unpack(n_chunks, pos, gate, h, first, more):
    weighted = h is not None
    n = pos.size
    width = first.shape[1]
    steps = n // UNPACK_STEP
    small = pl.BlockSpec((steps, UNPACK_STEP), lambda k: (0, 0))
    rows = pl.BlockSpec((UNPACK_STEP, width), lambda k: (k, 0))
    return pl.pallas_call(
        functools.partial(unpack_kernel, weighted),
        grid=(steps,),
        out_shape=jax.ShapeDtypeStruct((n, width), BF16),
        in_specs=[SMEM, small, small] + ([rows] if weighted else []) + [pl.BlockSpec((CHUNK, width), lambda k: (0, 0)), ANY],
        out_specs=rows,
        scratch_shapes=[pltpu.VMEM((CHUNK, width), BF16), pltpu.VMEM((UNPACK_STEP, width), F32), pltpu.SemaphoreType.DMA],
        compiler_params=params(),
        cost_estimate=pl.CostEstimate(flops=2 * CHUNK * n * width, bytes_accessed=4 * n * width, transcendentals=0),
        name='unpack',
    )(n_chunks.reshape(1), pos.reshape(steps, UNPACK_STEP), gate.reshape(steps, UNPACK_STEP), *([h] if weighted else []), first, more)


QUERY_BLOCK = 256
SOFT_ROWS = 64


def peers():
    f, e = lax.axis_index('fsdp'), lax.axis_index('ep')
    core = e + 1 - 2 * (e % 2)
    return (f, e), (1 - f, e), (f, (e + 2) % 4), (f, core), (1 - f, (e + 2) % 4), (1 - f, core), (f, (core + 2) % 4), (1 - f, (core + 2) % 4)


def rank(dev):
    return dev[0] * 4 + dev[1]


def meet_neighbours():
    me, y, x, core, *_ = peers()
    barrier = pltpu.get_barrier_semaphore()
    for dev in (y, x, core):
        pl.semaphore_signal(barrier, inc=1, device_id={'fsdp': dev[0], 'ep': dev[1]}, device_id_type=MESH)
    pl.semaphore_wait(barrier, 3)


def remote(src, dst, dev, sems, i):
    return pltpu.make_async_remote_copy(src, dst, sems.at[0, i], sems.at[1, i], device_id={'fsdp': dev[0], 'ep': dev[1]}, device_id_type=MESH)


class Gather:
    def __init__(self, own, out, sems):
        me, y, x, core, xy, *_ = peers()

        def flow(i, src, owner, dev):
            return remote(src, out.at[rank(owner)], dev, sems, i)

        self.flows = [
            flow(0, own, me, y),
            flow(1, own, me, x),
            flow(2, own, me, core),
            flow(3, out.at[rank(y)], y, x),
            flow(4, out.at[rank(y)], y, core),
            flow(5, out.at[rank(x)], x, core),
            flow(6, out.at[rank(xy)], xy, core),
        ]
        self.local = pltpu.make_async_copy(own, out.at[rank(me)], sems.at[0, 7])

    def start(self):
        for i in range(3):
            self.flows[i].start()
        self.local.start()

    def forward_y(self):
        self.flows[0].wait_recv()
        self.flows[3].start()
        self.flows[4].start()

    def forward_x(self):
        self.flows[1].wait_recv()
        self.flows[5].start()

    def forward_xy(self):
        self.flows[3].wait_recv()
        self.flows[6].start()

    def finish(self):
        for i in (2, 4, 5, 6):
            self.flows[i].wait_recv()
        for flow in self.flows:
            flow.wait_send()
        self.local.wait()

    def run(self):
        self.start()
        self.forward_y()
        self.forward_x()
        self.forward_xy()
        self.finish()


def attention_weight_flows(wq_hbm, wo_hbm, wqkv, wo, sems):
    me, y, x, core, xy, _, _, _ = peers()
    hw = wq_hbm.shape[0]
    quarter = hw // 4

    def pieces(dev):
        return wqkv.at[pl.ds(dev[0] * hw + dev[1] * quarter, quarter), :], wo.at[dev[0], pl.ds(dev[1] * 2 * quarter, 2 * quarter), :]

    mine = wq_hbm.at[pl.ds(me[1] * quarter, quarter), :], wo_hbm.at[pl.ds(me[1] * 2 * quarter, 2 * quarter), :]
    flows = []
    for part in range(2):
        flows.append([
            remote(mine[part], pieces(me)[part], y, sems, part),
            remote(pieces(y)[part], pieces(y)[part], x, sems, 2 + part),
            remote(pieces(y)[part], pieces(y)[part], core, sems, 4 + part),
            remote(pieces(xy)[part], pieces(xy)[part], core, sems, 6 + part),
        ])
    return flows


def load_attention_weights(wqkv_hbm, wo_hbm, wqkv, wo, sems):
    copies = [pltpu.make_async_copy(wqkv_hbm, wqkv, sems.at[0]), pltpu.make_async_copy(wo_hbm, wo, sems.at[1])]
    for cp in copies:
        cp.start()
    for cp in copies:
        cp.wait()


class WeightPieces:
    def __init__(self, own, send, part, outs, sems, n):
        y = peers()[1]
        gate, up, down = own
        r13, r2 = outs
        hw, size = gate.shape[1], r2.shape[0]
        cols = pl.ds(part * size, size)
        step, step2 = hw // n, size // n
        self.pieces = []
        for i in range(n):
            rows = pl.ds(i * step, step)
            self.pieces.append([
                remote(gate.at[send, rows, cols], r13.at[rows, :], y, sems, 3 * i),
                remote(up.at[send, rows, cols], r13.at[pl.ds(hw + i * step, step), :], y, sems, 3 * i + 1),
                remote(down.at[send, pl.ds(part * size + i * step2, step2), :], r2.at[pl.ds(i * step2, step2), :], y, sems, 3 * i + 2),
            ])

    def start(self, i):
        for cp in self.pieces[i]:
            cp.start()

    def finish(self):
        for piece in self.pieces:
            for cp in piece:
                cp.wait()


def inv_rms_of(wide_vals):
    return lax.rsqrt(jnp.mean(wide_vals * wide_vals, axis=-1, keepdims=True) + 1e-6)


def head_lanes(shape, axis, head):
    lane = lax.broadcasted_iota(jnp.int32, shape, axis)
    return lane < 64 if head == 0 else lane >= 64


def attn_fwd_kernel(pos_ref, cnt_hbm, dy_hbm, wq_hbm, wo_hbm, gate_hbm, up_hbm, down_hbm, x_ref, *refs):
    h_ref, u_ref, qkv_ref, ctx_ref, inv_ref, p0_ref, p1_ref, wqkv_out, wo_out, cnt_all, dy_all, u_all, a0, b0, a1, b1 = refs[:16]
    wqkv, wo, acc, u_pack, s_scr, bias, sem_a, sem_c, sem_d, sem_u, sem_0, sem_1, sem_w = refs[16:]
    i = pl.program_id(0)
    width = x_ref.shape[1]
    hw = width // 2
    seq = x_ref.shape[0]
    me = peers()[0]
    own = gate_hbm, up_hbm, down_hbm
    counts, dys, us = Gather(cnt_hbm, cnt_all, sem_c), Gather(dy_hbm, dy_all, sem_d), Gather(u_pack, u_all, sem_u)
    part0 = WeightPieces(own, 1 - me[0], 0, (a0, b0), sem_0, 1)
    part1 = WeightPieces(own, 1 - me[0], 1, (a1, b1), sem_1, 4)
    flows = attention_weight_flows(wq_hbm, wo_hbm, wqkv, wo, sem_a)
    local = [
        pltpu.make_async_copy(wq_hbm, wqkv.at[pl.ds(me[0] * hw, hw), :], sem_w.at[0]),
        pltpu.make_async_copy(wo_hbm, wo.at[me[0]], sem_w.at[1]),
    ]
    keep = [pltpu.make_async_copy(wqkv, wqkv_out, sem_w.at[2]), pltpu.make_async_copy(wo, wo_out, sem_w.at[3])]

    @pl.when(i == 0)
    def _():
        meet_neighbours()
        for cps in flows:
            cps[0].start()
        for cp in local:
            cp.start()
        counts.start()
        for cps in flows:
            cps[0].wait_recv()
            cps[1].start()
            cps[2].start()
        dys.start()
        part0.start(0)
        for cps in flows:
            cps[1].wait_recv()
            cps[3].start()
        for cps in flows:
            cps[2].wait_recv()
            cps[3].wait_recv()
            for cp in cps:
                cp.wait_send()
        for cp in local:
            cp.wait()
        for cp in keep:
            cp.start()
        acc[...] = jnp.zeros_like(acc)
        shape = (QUERY_BLOCK, QUERY_BLOCK)
        keep_it = lax.broadcasted_iota(jnp.int32, shape, 0) >= lax.broadcasted_iota(jnp.int32, shape, 1)
        bias[...] = jnp.where(keep_it, 0.0, -1e30)

    @pl.when(i == 2)
    def _():
        counts.forward_y()
        counts.forward_x()
        dys.forward_y()
        dys.forward_x()

    @pl.when(i == 4)
    def _():
        counts.forward_xy()
        dys.forward_xy()

    for n in range(4):
        @pl.when(i == 3 + n)
        def _(n=n):
            part1.start(n)

    x = x_ref[...].astype(F32)
    normed = (x * inv_rms_of(x)).astype(BF16)
    for t in range(3):
        cols = slice(t * width, (t + 1) * width)
        qkv_ref[:, cols] = mm(normed, wqkv[:, cols]).astype(BF16)
    units = [(pair, j, head) for pair in range(width // 128) for j in range(2) for head in range(2)]
    ones = jnp.ones((2 * QUERY_BLOCK, 128), BF16)

    def score(n):
        pair, j, head = units[n]
        rows = slice(j * QUERY_BLOCK, (j + 1) * QUERY_BLOCK)
        keys = slice(0, (j + 1) * QUERY_BLOCK)
        q = qkv_ref[rows, pair * 128 : (pair + 1) * 128] * jnp.asarray(0.125, BF16)
        q = jnp.where(head_lanes((QUERY_BLOCK, 128), 1, head), q, jnp.zeros((), BF16))
        k = qkv_ref[keys, width + pair * 128 : width + (pair + 1) * 128]
        s_scr[n % 2, :, keys] = mm(q, k, NT)

    def soften(n):
        pair, j, head = units[n]
        p_ref = (p0_ref, p1_ref)[j]
        base = j * QUERY_BLOCK
        for r in range(0, QUERY_BLOCK, SOFT_ROWS):
            rows = slice(r, r + SOFT_ROWS)
            end = (r + SOFT_ROWS + 127) // 128 * 128
            s = s_scr[n % 2, rows, base : base + end] + bias[rows, :end]
            if j:
                s = jnp.concatenate([s_scr[n % 2, rows, :base], s], axis=1)
            p_ref[0, pair * 2 + head, rows, : base + end] = jnp.exp(s - jnp.max(s, axis=1, keepdims=True)).astype(BF16)
            if end < QUERY_BLOCK:
                p_ref[0, pair * 2 + head, rows, base + end :] = jnp.zeros((SOFT_ROWS, QUERY_BLOCK - end), BF16)

    def weigh(n):
        pair, j, head = units[n]
        keys = slice(0, (j + 1) * QUERY_BLOCK)
        v = qkv_ref[keys, 2 * width + pair * 128 : 2 * width + (pair + 1) * 128]
        both = mm((p0_ref, p1_ref)[j][0, pair * 2 + head], jnp.concatenate([v, ones[keys]], axis=1))
        return both[:, :128], both[:, 128:]

    score(0)
    for n, (pair, j, head) in enumerate(units):
        if n + 1 < len(units):
            score(n + 1)
        soften(n)
        if head == 0:
            first_out = weigh(n)
        else:
            rows, lanes = slice(j * QUERY_BLOCK, (j + 1) * QUERY_BLOCK), slice(pair * 128, (pair + 1) * 128)
            out, total = weigh(n)
            left = head_lanes((QUERY_BLOCK, 128), 1, 0)
            inv = 1.0 / jnp.where(left, first_out[1], total)
            inv_ref[rows, lanes] = inv
            ctx_ref[rows, lanes] = (jnp.where(left, first_out[0], out) * inv).astype(BF16)
    ctx = ctx_ref[...]
    for f in range(2):
        cols = slice(f * hw, (f + 1) * hw)
        h_ref[:, cols] = (x_ref[:, cols].astype(F32) + mm(ctx, wo[f])).astype(BF16)
    h = h_ref[...].astype(F32)
    u = (h * inv_rms_of(h)).astype(BF16)
    u_ref[...] = u
    hit = lax.broadcasted_iota(jnp.int32, (CHUNK, seq), 0) == pos_ref[pl.ds(i, 1), :]
    acc[...] += mm(jnp.where(hit, 1.0, 0.0).astype(BF16), u)

    @pl.when(i == pl.num_programs(0) - 1)
    def _():
        u_pack[...] = acc[...].astype(BF16)
        us.run()
        counts.finish()
        dys.finish()
        part0.finish()
        part1.finish()
        for cp in keep:
            cp.wait()


def probs_shapes(n_seq, width):
    return [jax.ShapeDtypeStruct((n_seq, width // 64, QUERY_BLOCK, (j + 1) * QUERY_BLOCK), BF16) for j in range(2)]


def probs_specs(width):
    return [pl.BlockSpec((1, width // 64, QUERY_BLOCK, (j + 1) * QUERY_BLOCK), lambda i: (i, 0, 0, 0)) for j in range(2)]


def attn_fwd(pos, cnt, dy, wq, wo, own, x, n_seq):
    n, width = x.shape
    seq = n // n_seq
    hw = width // 2
    size = own[0].shape[2] // N_PARTS
    rows = pl.BlockSpec((seq, width), lambda i: (i, 0))
    part = [jax.ShapeDtypeStruct((width, size), BF16), jax.ShapeDtypeStruct((size, hw), BF16)]
    sems = lambda k: pltpu.SemaphoreType.DMA((2, k))
    h, u, qkv, ctx, inv, p0, p1, *rest = pl.pallas_call(
        attn_fwd_kernel,
        grid=(n_seq,),
        out_shape=(
            jax.ShapeDtypeStruct((n, width), BF16),
            jax.ShapeDtypeStruct((n, width), BF16),
            jax.ShapeDtypeStruct((n, 3 * width), BF16),
            jax.ShapeDtypeStruct((n, width), BF16),
            jax.ShapeDtypeStruct((n, width), F32),
            *probs_shapes(n_seq, width),
            jax.ShapeDtypeStruct((width, 3 * width), BF16),
            jax.ShapeDtypeStruct((2, width, hw), BF16),
            jax.ShapeDtypeStruct((8, 1, 128), jnp.int32),
            jax.ShapeDtypeStruct((8, CHUNK, width), BF16),
            jax.ShapeDtypeStruct((8, CHUNK, width), BF16),
            *part,
            *part,
        ),
        in_specs=[pl.BlockSpec((n_seq, seq), lambda i: (0, 0))] + [ANY] * 7 + [rows],
        out_specs=(rows, rows, pl.BlockSpec((seq, 3 * width), lambda i: (i, 0)), rows, rows, *probs_specs(width)) + (ANY,) * 9,
        scratch_shapes=[
            pltpu.VMEM((width, 3 * width), BF16),
            pltpu.VMEM((2, width, hw), BF16),
            pltpu.VMEM((CHUNK, width), F32),
            pltpu.VMEM((CHUNK, width), BF16),
            pltpu.VMEM((2, QUERY_BLOCK, seq), F32),
            pltpu.VMEM((QUERY_BLOCK, QUERY_BLOCK), F32),
            sems(8),
            sems(8),
            sems(8),
            sems(8),
            sems(3),
            sems(12),
            pltpu.SemaphoreType.DMA((4,)),
        ],
        compiler_params=pltpu.CompilerParams(vmem_limit_bytes=60 * 1024 * 1024, collective_id=0, has_side_effects=True),
        cost_estimate=pl.CostEstimate(flops=30 * 10**9, bytes_accessed=50 * 2**20, transcendentals=0),
        name='attn_fwd',
    )(pos.reshape(n_seq, seq), cnt, dy, wq, wo, *own, x)
    return (h, u, qkv, ctx, (inv, p0, p1)), rest


def norm_back(grad, wide_vals):
    inv = inv_rms_of(wide_vals)
    return inv * (grad - wide_vals * (inv * inv * jnp.mean(grad * wide_vals, axis=-1, keepdims=True)))


def attn_bwd_kernel(n_ref, pos_ref, first_ref, more_hbm, wqkv_hbm, wo_hbm, x_ref, h_ref, dout_ref, qkv_ref, ctx_ref, inv_ref, p0_ref, p1_ref, dx_ref, wqkv, wo, dqkv, dctx, dp_scr, ds_scr, dh, buf, sem, w_sem):
    i = pl.program_id(0)
    seq, width = x_ref.shape
    hw = width // 2

    @pl.when(i == 0)
    def _():
        load_attention_weights(wqkv_hbm, wo_hbm, wqkv, wo, w_sem)

    pos = pos_ref[pl.ds(i, 1), :]
    row = lax.broadcasted_iota(jnp.int32, (CHUNK, seq), 0)

    def gathered(base, rows):
        return mm(jnp.where(row + base == pos, 1.0, 0.0).astype(BF16), rows, TN)

    dh[...] = gathered(0, first_ref[...])

    def more(c, carry):
        copy = pltpu.make_async_copy(more_hbm.at[c - 1], buf, sem)
        copy.start()
        copy.wait()
        dh[...] += gathered(c * CHUNK, buf[...])
        return carry

    lax.fori_loop(1, n_ref[0], more, 0)
    dh[...] = dout_ref[...].astype(F32) + norm_back(dh[...], h_ref[...].astype(F32))
    dh_b = dh[...].astype(BF16)
    dctx[...] = ((mm(dh_b[:, :hw], wo[0], NT) + mm(dh_b[:, hw:], wo[1], NT)) * inv_ref[...]).astype(BF16)
    zero = jnp.zeros((), BF16)
    units = [(pair, j, head) for pair in range(width // 128) for j in range(2) for head in range(2)]

    def third(t, pair):
        return slice(t * width + pair * 128, t * width + (pair + 1) * 128)

    def block(j):
        return slice(j * QUERY_BLOCK, (j + 1) * QUERY_BLOCK), slice(0, (j + 1) * QUERY_BLOCK)

    def d_probs(n):
        pair, j, head = units[n]
        rows, keys = block(j)
        do = jnp.where(head_lanes((QUERY_BLOCK, 128), 1, head), dctx[rows, third(0, pair)], zero)
        dp_scr[n % 2, :, keys] = mm(do, qkv_ref[keys, third(2, pair)], NT)

    def d_scores(n):
        pair, j, head = units[n]
        for r in range(0, QUERY_BLOCK, SOFT_ROWS):
            rows, at = slice(r, r + SOFT_ROWS), slice(j * QUERY_BLOCK + r, j * QUERY_BLOCK + r + SOFT_ROWS)
            base = j * QUERY_BLOCK
            end = base + (r + SOFT_ROWS + 127) // 128 * 128
            prod = dctx[at, third(0, pair)].astype(F32) * ctx_ref[at, third(0, pair)].astype(F32)
            delta = jnp.sum(jnp.where(head_lanes((SOFT_ROWS, 128), 1, head), prod, 0.0), axis=1, keepdims=True)
            p = (p0_ref, p1_ref)[j][0, pair * 2 + head, rows, :end].astype(F32)
            ds_scr[n % 2, rows, :end] = (p * (dp_scr[n % 2, rows, :end] - delta)).astype(BF16)
            if end < base + QUERY_BLOCK:
                ds_scr[n % 2, rows, end : base + QUERY_BLOCK] = jnp.zeros((SOFT_ROWS, base + QUERY_BLOCK - end), BF16)

    d_probs(0)
    for n, (pair, j, head) in enumerate(units):
        if n + 1 < len(units):
            d_probs(n + 1)
        d_scores(n)
        rows, keys = block(j)
        if j == 0 and head == 0:
            q_t = (qkv_ref[:, third(0, pair)] * jnp.asarray(0.125, BF16)).T
            do_t = dctx[:, third(0, pair)].T
            dk_t = [jnp.zeros((128, QUERY_BLOCK), F32) for _ in range(2)]
            dv_t = list(dk_t)
        ds = ds_scr[n % 2, :, keys]
        dq = mm(ds, qkv_ref[keys, third(1, pair)])
        mine_t = head_lanes((128, QUERY_BLOCK), 0, head)
        dk_part = mm(jnp.where(mine_t, q_t[:, rows], zero), ds)
        dv_part = mm(jnp.where(mine_t, do_t[:, rows], zero), (p0_ref, p1_ref)[j][0, pair * 2 + head])
        for c in range(j + 1):
            dk_t[c] = dk_t[c] + dk_part[:, block(c)[0]]
            dv_t[c] = dv_t[c] + dv_part[:, block(c)[0]]
        if head == 0:
            first_dq = dq
        else:
            dqkv[rows, third(0, pair)] = (jnp.where(head_lanes((QUERY_BLOCK, 128), 1, 0), first_dq, dq) * 0.125).astype(BF16)
            if j == 1:
                for c in range(2):
                    dqkv[block(c)[0], third(1, pair)] = dk_t[c].astype(BF16).T
                    dqkv[block(c)[0], third(2, pair)] = dv_t[c].astype(BF16).T
    dn = mm(dqkv[...], wqkv[...], NT)
    dx_ref[...] = (dh[...] + norm_back(dn, x_ref[...].astype(F32))).astype(BF16)


def attn_bwd(n_chunks, pos, first, more, wqkv, wo, x, h, dout, qkv, ctx, probs, n_seq):
    n, width = x.shape
    seq = n // n_seq
    rows = pl.BlockSpec((seq, width), lambda i: (i, 0))
    return pl.pallas_call(
        attn_bwd_kernel,
        grid=(n_seq,),
        out_shape=jax.ShapeDtypeStruct((n, width), BF16),
        in_specs=[SMEM, pl.BlockSpec((n_seq, seq), lambda i: (0, 0)), pl.BlockSpec((CHUNK, width), lambda i: (0, 0)), ANY, ANY, ANY, rows, rows, rows, pl.BlockSpec((seq, 3 * width), lambda i: (i, 0)), rows, rows, *probs_specs(width)],
        out_specs=rows,
        scratch_shapes=[
            pltpu.VMEM((width, 3 * width), BF16),
            pltpu.VMEM((2, width, width // 2), BF16),
            pltpu.VMEM((seq, 3 * width), BF16),
            pltpu.VMEM((seq, width), BF16),
            pltpu.VMEM((2, QUERY_BLOCK, seq), F32),
            pltpu.VMEM((2, QUERY_BLOCK, seq), BF16),
            pltpu.VMEM((seq, width), F32),
            pltpu.VMEM((CHUNK, width), BF16),
            pltpu.SemaphoreType.DMA,
            pltpu.SemaphoreType.DMA((2,)),
        ],
        compiler_params=params(),
        cost_estimate=pl.CostEstimate(flops=50 * 10**9, bytes_accessed=60 * 2**20, transcendentals=0),
        name='attn_bwd',
    )(n_chunks.reshape(1), pos.reshape(n_seq, seq), first, more, wqkv, wo, x, h, dout, qkv, ctx, *probs)


def experts_kernel(back, first, last, f_base, n_src, cnt_ref, prm_ref, u_hbm, dy_hbm, w1_hbm, w3_hbm, w2_hbm, r13_hbm, r2_hbm, i1, i3, i2, *refs):
    if back:
        o1, o3, o2, y_part, du_part = refs[2:7]
        scratch = refs[7:]
        if last:
            (y_hbm, du_hbm), scratch = scratch[:2], scratch[2:]
        y_acc, du_acc, stage, zero, row_sem, part_sem = scratch[-6:]
        scratch = scratch[:-6]
    else:
        o1, o3, o2 = refs[:3]
        scratch = refs[3:]
    u_s, dy_s, ut_s, dyt_s, w1_s, w3_s, w2_s, d1_s, d3_s, d2_s, d2t_s, lst, load_sem, w_sem, d_sem = scratch
    expert, local, half, chunk, add_first = prm_ref[0], prm_ref[1], prm_ref[2], prm_ref[3], prm_ref[4]
    width = u_s.shape[1]
    hw = width // 2
    n_ff = r2_hbm.shape[0] // FF_STEP
    first_tile = chunk * CHUNK_TILES
    own_rows = pl.ds(pl.multiple_of(half * hw, hw), hw)
    got_rows = pl.ds(pl.multiple_of((1 - half) * hw, hw), hw)

    if back and last:
        def unmark(t, carry):
            lst[1, t] = 0
            return carry

        lax.fori_loop(0, n_src * CHUNK_TILES, unmark, 0)
    total = jnp.int32(0)
    for s in range(n_src):
        off, own = jnp.int32(0), jnp.int32(0)
        for e in range(n_src):
            tiles = (cnt_ref[s, e] + (TILE - 1)) // TILE
            off = off + jnp.where(e < expert, tiles, 0)
            own = own + jnp.where(e == expert, tiles, 0)
        lo = jnp.clip(off - first_tile, 0, CHUNK_TILES)
        hi = jnp.clip(off + own - first_tile, 0, CHUNK_TILES)

        def note(j, t, s=s):
            lst[0, t] = s * CHUNK_TILES + j
            if back and last:
                lst[1, s * CHUNK_TILES + j] = 1
            return t + 1

        total = lax.fori_loop(lo, hi, note, total)

    def tile_of(ref, t):
        return ref.at[t // CHUNK_TILES, pl.ds(pl.multiple_of((t % CHUNK_TILES) * TILE, TILE), TILE), :]

    if back and last:
        zero[...] = jnp.zeros_like(zero)

        def clear(t, n):
            @pl.when(lst[1, t] == 0)
            def _():
                pltpu.make_async_copy(zero, tile_of(y_hbm, t), row_sem).start()
                pltpu.make_async_copy(zero, tile_of(du_hbm, t), row_sem).start()

            return n

        lax.fori_loop(0, n_src * CHUNK_TILES, clear, 0)

    def weights(f, slot):
        cols = pl.ds(pl.multiple_of(f_base + f * FF_STEP, FF_STEP), FF_STEP)
        part = pl.ds(pl.multiple_of(f * FF_STEP, FF_STEP), FF_STEP)
        pairs = [
            (w1_hbm.at[local, :, cols], w1_s.at[slot, own_rows, :]),
            (r13_hbm.at[pl.ds(0, hw), part], w1_s.at[slot, got_rows, :]),
            (w3_hbm.at[local, :, cols], w3_s.at[slot, own_rows, :]),
            (r13_hbm.at[pl.ds(hw, hw), part], w3_s.at[slot, got_rows, :]),
            (w2_hbm.at[local, cols, :], w2_s.at[slot, :, own_rows]),
            (r2_hbm.at[part, :], w2_s.at[slot, :, got_rows]),
        ]
        return [pltpu.make_async_copy(src, dst, w_sem.at[slot, i]) for i, (src, dst) in enumerate(pairs)]

    def grads(f, slot, ins):
        cols = pl.ds(pl.multiple_of(f_base + f * FF_STEP, FF_STEP), FF_STEP)
        hbm = (i1, i3, i2) if ins else (o1, o3, o2)
        pairs = [
            (hbm[0].at[local, :, cols], d1_s.at[slot]),
            (hbm[1].at[local, :, cols], d3_s.at[slot]),
            (hbm[2].at[local, cols, :], d2_s.at[slot]),
        ]
        if not ins:
            pairs = [(b, a) for a, b in pairs]
        return [pltpu.make_async_copy(src, dst, d_sem.at[slot, i]) for i, (src, dst) in enumerate(pairs)]

    def one_pass(p, carry):
        for cp in weights(0, 0):
            cp.start()
        n_tiles = jnp.clip(total - p * PASS_TILES, 0, PASS_TILES)
        n_blk = (n_tiles + (CHUNK_TILES - 1)) // CHUNK_TILES

        def rows_at(k):
            return pl.ds(pl.multiple_of(k * TILE, TILE), TILE)

        def load(k, carry):
            t = lst[0, p * PASS_TILES + k]
            pltpu.make_async_copy(tile_of(u_hbm, t), u_s.at[rows_at(k), :], load_sem).start()
            pltpu.make_async_copy(tile_of(dy_hbm, t), dy_s.at[rows_at(k), :], load_sem).start()
            return carry

        lax.fori_loop(0, n_tiles, load, 0)

        def partial_sums(b, out):
            rows = pl.ds(pl.multiple_of(b * CHUNK, CHUNK), CHUNK)
            hbm_rows = pl.ds(pl.multiple_of((p * (PASS_TILES // CHUNK_TILES) + b) * CHUNK, CHUNK), CHUNK)
            pairs = [(y_acc.at[rows, :], y_part.at[hbm_rows, :]), (du_acc.at[rows, :], du_part.at[hbm_rows, :])]
            return [pltpu.make_async_copy(*(pair if out else pair[::-1]), part_sem) for pair in pairs]

        def each_block(out, action):
            def go(b, carry):
                for cp in partial_sums(b, out):
                    getattr(cp, action)()
                return carry

            lax.fori_loop(0, n_blk, go, 0)

        if back and not first:
            each_block(False, 'start')

        def fill(k, carry):
            u_s[rows_at(k), :] = jnp.zeros((TILE, width), BF16)
            dy_s[rows_at(k), :] = jnp.zeros((TILE, width), BF16)
            return carry

        lax.fori_loop(n_tiles, n_blk * CHUNK_TILES, fill, 0)

        def loaded(k, carry):
            pltpu.make_async_copy(tile_of(u_hbm, 0), u_s.at[rows_at(k), :], load_sem).wait()
            pltpu.make_async_copy(tile_of(dy_hbm, 0), dy_s.at[rows_at(k), :], load_sem).wait()
            return carry

        lax.fori_loop(0, n_tiles, loaded, 0)

        def flip(k, carry):
            ut_s[:, rows_at(k)] = u_s[rows_at(k), own_rows].T
            dyt_s[:, rows_at(k)] = dy_s[rows_at(k), own_rows].T
            return carry

        lax.fori_loop(0, n_blk * CHUNK_TILES, flip, 0)
        if back and not first:
            each_block(False, 'wait')
        add = jnp.logical_or(p > 0, add_first > 0)

        def step(f, carry):
            slot = f % 2

            @pl.when(f + 1 < n_ff)
            def _():
                for cp in weights(f + 1, 1 - slot):
                    cp.start()

            @pl.when(f >= 2)
            def _():
                for cp in grads(f - 2, slot, False):
                    cp.wait()

            for cp in weights(f, slot):
                cp.wait()

            d1_s[slot] = jnp.zeros((hw, FF_STEP), F32)
            d3_s[slot] = jnp.zeros((hw, FF_STEP), F32)
            d2t_s[...] = jnp.zeros((hw, FF_STEP), F32)

            @pl.when(add)
            def _():
                for cp in grads(f, slot, True):
                    cp.start()
                for cp in grads(f, slot, True):
                    cp.wait()
                d2t_s[...] = d2_s[slot].T

            def block(b, carry):
                rows = pl.ds(pl.multiple_of(b * CHUNK, CHUNK), CHUNK)
                w1, w3, w2 = w1_s[slot], w3_s[slot], w2_s[slot]
                u, dy = u_s[rows, :], dy_s[rows, :]
                act_a = mm(u, w1)
                act_b = mm(u, w3)
                d_g = mm(dy, w2, NT)
                sig = 0.5 * jnp.tanh(0.5 * act_a) + 0.5
                silu = act_a * sig
                g = (silu * act_b).astype(BF16)
                d_b = (d_g * silu).astype(BF16)
                d_a = (d_g * act_b * (sig + silu * (1.0 - sig))).astype(BF16)
                if back:
                    y = mm(g, w2)
                    du = mm(d_a, w1, NT) + mm(d_b, w3, NT)

                    if first:
                        @pl.when(f == 0)
                        def _():
                            y_acc[rows, :] = y
                            du_acc[rows, :] = du

                        @pl.when(f > 0)
                        def _():
                            y_acc[rows, :] += y
                            du_acc[rows, :] += du
                    else:
                        y_acc[rows, :] += y
                        du_acc[rows, :] += du

                d1_s[slot] += mm(ut_s[:, rows], d_a)
                d3_s[slot] += mm(ut_s[:, rows], d_b)
                d2t_s[...] += mm(dyt_s[:, rows], g)
                return carry

            lax.fori_loop(0, n_blk, block, 0)
            d2_s[slot] = d2t_s[...].T
            for cp in grads(f, slot, False):
                cp.start()
            return carry

        lax.fori_loop(0, n_ff, step, 0)
        if back and not last:
            each_block(True, 'start')
            each_block(True, 'wait')
        if back and last:
            def put(k, carry):
                t = lst[0, p * PASS_TILES + k]
                stage[0, rows_at(k), :] = y_acc[rows_at(k), :].astype(BF16)
                stage[1, rows_at(k), :] = du_acc[rows_at(k), :].astype(BF16)
                pltpu.make_async_copy(stage.at[0, rows_at(k), :], tile_of(y_hbm, t), row_sem).start()
                pltpu.make_async_copy(stage.at[1, rows_at(k), :], tile_of(du_hbm, t), row_sem).start()
                return carry

            lax.fori_loop(0, n_tiles, put, 0)

            def done(k, carry):
                pltpu.make_async_copy(zero, tile_of(y_hbm, 0), row_sem).wait()
                pltpu.make_async_copy(zero, tile_of(du_hbm, 0), row_sem).wait()
                return carry

            lax.fori_loop(0, n_tiles, done, 0)
        for f in (n_ff - 2, n_ff - 1):
            for cp in grads(f, f % 2, False):
                cp.wait()
        return carry

    n_pass = jnp.maximum((total + (PASS_TILES - 1)) // PASS_TILES, 1)
    lax.fori_loop(0, n_pass, one_pass, 0)
    if back and last:
        def cleared(t, carry):
            pltpu.make_async_copy(zero, tile_of(y_hbm, 0), row_sem).wait()
            pltpu.make_async_copy(zero, tile_of(du_hbm, 0), row_sem).wait()
            return carry

        lax.fori_loop(0, n_src * CHUNK_TILES - total, cleared, 0)


def experts(back, part, n_parts, counts, prm, u_all, dy_all, own, got, dws, sums=()):
    n_src, _, width = u_all.shape
    first, last = part == 0, part == n_parts - 1
    hw = width // 2
    ff = got[1].shape[0]
    rows = PASS_TILES * TILE
    scratch = [
        pltpu.VMEM((rows, width), BF16),
        pltpu.VMEM((rows, width), BF16),
        pltpu.VMEM((hw, rows), BF16),
        pltpu.VMEM((hw, rows), BF16),
        pltpu.VMEM((2, width, FF_STEP), BF16),
        pltpu.VMEM((2, width, FF_STEP), BF16),
        pltpu.VMEM((2, FF_STEP, width), BF16),
        pltpu.VMEM((2, hw, FF_STEP), F32),
        pltpu.VMEM((2, hw, FF_STEP), F32),
        pltpu.VMEM((2, FF_STEP, hw), F32),
        pltpu.VMEM((hw, FF_STEP), F32),
        pltpu.SMEM((2, n_src * CHUNK_TILES), jnp.int32),
        pltpu.SemaphoreType.DMA,
        pltpu.SemaphoreType.DMA((2, 6)),
        pltpu.SemaphoreType.DMA((2, 3)),
    ]
    outs = [jax.ShapeDtypeStruct(d.shape, d.dtype) for d in (*dws, *sums)]
    n_alias = len(outs)
    if back and last:
        outs += [jax.ShapeDtypeStruct(u_all.shape, BF16)] * 2
    if back:
        scratch += [
            pltpu.VMEM((rows, width), F32),
            pltpu.VMEM((rows, width), F32),
            pltpu.VMEM((2, rows, width), BF16),
            pltpu.VMEM((TILE, width), BF16),
            pltpu.SemaphoreType.DMA,
            pltpu.SemaphoreType.DMA,
        ]
    units = 7.5 if back else 4.5
    return pl.pallas_call(
        functools.partial(experts_kernel, back, first, last, part * ff, n_src),
        out_shape=tuple(outs),
        in_specs=[SMEM, SMEM] + [ANY] * (7 + n_alias),
        out_specs=tuple([ANY] * len(outs)),
        scratch_shapes=scratch,
        input_output_aliases={9 + i: i for i in range(n_alias)},
        compiler_params=params(),
        cost_estimate=pl.CostEstimate(flops=int(units * 2 * 2 * CHUNK * width * ff), bytes_accessed=10 * 2**20, transcendentals=0),
    )(counts, prm, u_all, dy_all, *own, *got, *dws, *sums)


def unset_kernel(*refs):
    pass


def unset(*shapes):
    outs = tuple(jax.ShapeDtypeStruct(s, d) for s, d in shapes)
    return pl.pallas_call(unset_kernel, out_shape=outs, out_specs=tuple([ANY] * len(outs)), name='unset')()


def solution(mesh):
    n_dev = mesh.shape['fsdp'] * mesh.shape['ep']
    tok_spec = P(('data', 'fsdp', 'ep'))
    in_specs = (tok_spec, P('fsdp'), P(None, None, 'fsdp'), P('ep', 'fsdp'), P('ep', 'fsdp'), P('ep', None, 'fsdp'), tok_spec, tok_spec, tok_spec, tok_spec)
    out_specs = (tok_spec, tok_spec, P(('data', 'ep'), 'fsdp'), P(('data', 'ep'), 'fsdp'), P(('data', 'ep'), None, 'fsdp'))

    def device_fn(tokens, w_qkv, w_out, w_gate, w_up, w_down, expert_idx, expert_slot, gate_wts, d_out):
        n_seq, seq_len, d_model = tokens.shape
        n_tok = n_seq * seq_len
        n_exp = n_dev
        half = lax.axis_index('fsdp').astype(jnp.int32)
        col = lax.axis_index('ep').astype(jnp.int32)
        swap = [(0, 1), (1, 0)]
        own = (w_gate, w_up, w_down)

        def other(local, r):
            gate, up, down = [lax.dynamic_index_in_dim(w, local, 0, keepdims=False) for w in own]
            size = down.shape[0] // N_PARTS
            cols = slice(r * size, (r + 1) * size)
            both = lax.ppermute(jnp.concatenate([gate[:, cols], up[:, cols]], axis=0), 'fsdp', swap)
            return both, lax.ppermute(down[cols], 'fsdp', swap)

        def back(chunk, add, u_c, dy_c, dws):
            sums = unset(*[((n_dev * CHUNK, d_model), F32)] * 2)
            for r in range(N_PARTS):
                *state, = experts(True, r, N_PARTS, counts, prm(half, chunk, add), u_c, dy_c, own, got_mine[r], dws, sums)
                dws, sums = state[:3], state[3:5]
            return dws, state[5], state[6]

        def grad_part(r, chunk, add, u_c, dy_c, dws):
            return experts(False, r, N_PARTS, counts, prm(1 - half, chunk, add), u_c, dy_c, own, got_rest[r], dws)

        def prm(local, chunk, add):
            return jnp.stack([2 * col + local, local, half, chunk, add]).astype(jnp.int32)

        x_tok = tokens.reshape(n_tok, d_model)
        dout_tok = d_out.reshape(n_tok, d_model)
        gate = gate_wts.reshape(n_tok // PACK_STEP, PACK_STEP).astype(F32)
        zero = jnp.int32(0)
        pos, cnt = route(expert_idx, expert_slot, n_exp)
        dy_pack = pack(zero, pos, gate, dout_tok, True)
        wq = w_qkv.reshape(d_model // 2, 3 * d_model)
        (h_tok, u_tok, qkv, ctx, probs), gathered = attn_fwd(pos, cnt, dy_pack, wq, w_out.reshape(d_model, d_model // 2), own, x_tok, n_seq)
        wqkv_full, wo_full, counts, dy_all, u_all, a0, b0, a1, b1 = gathered
        counts = counts.reshape(n_exp, 128)
        got_mine = [(a0, b0), (a1, b1), other(1 - half, 2)]
        got_rest = [other(half, r) for r in range(N_PARTS)]

        tiles = (counts[:, :n_exp] + (TILE - 1)) // TILE
        n_chunks = jnp.max((jnp.sum(tiles, axis=1) + (CHUNK_TILES - 1)) // CHUNK_TILES)
        max_more = (n_tok + n_exp * (TILE - 1)) // CHUNK

        dws = unset(*[(w.shape, F32) for w in own])
        more_y, more_du = unset(*[((max_more, CHUNK, d_model), BF16)] * 2)
        dws, y_all, du_all = back(zero, zero, u_all, dy_all, dws)
        first_du = lax.psum_scatter(du_all, GROUP, scatter_dimension=0)

        first_y = lax.psum_scatter(y_all, GROUP, scatter_dimension=0)

        def fetch(c):
            return lax.all_gather(pack(c, pos, gate, u_tok, False), GROUP), lax.all_gather(pack(c, pos, gate, dout_tok, True), GROUP)

        def more_back(state):
            c, d1, d3, d2, ys, dus = state
            u_c, dy_c = fetch(c)
            (d1, d3, d2), y_c, du_c = back(c, jnp.int32(1), u_c, dy_c, (d1, d3, d2))
            y_c = lax.psum_scatter(y_c, GROUP, scatter_dimension=0)
            du_c = lax.psum_scatter(du_c, GROUP, scatter_dimension=0)
            ys = lax.dynamic_update_index_in_dim(ys, y_c, c - 1, 0)
            dus = lax.dynamic_update_index_in_dim(dus, du_c, c - 1, 0)
            return c + 1, d1, d3, d2, ys, dus

        def more_grad(state):
            c, d1, d3, d2 = state
            u_c, dy_c = fetch(c)
            dws = (d1, d3, d2)
            for r in range(N_PARTS):
                dws = grad_part(r, c, jnp.int32(1), u_c, dy_c, dws)
            return (c + 1, *dws)

        _, *dws, more_y, more_du = lax.while_loop(lambda s: s[0] < n_chunks, more_back, (jnp.int32(1), *dws, more_y, more_du))
        layer_out = unpack(n_chunks, pos, gate, h_tok, first_y, more_y).reshape(n_seq, seq_len, d_model)
        d_tokens = attn_bwd(n_chunks, pos, first_du, more_du, wqkv_full, wo_full, x_tok, h_tok, dout_tok, qkv, ctx, probs, n_seq).reshape(n_seq, seq_len, d_model)

        for r in range(N_PARTS):
            dws = grad_part(r, zero, zero, u_all, dy_all, dws)
        _, *dws = lax.while_loop(lambda s: s[0] < n_chunks, more_grad, (jnp.int32(1), *dws))
        return layer_out, d_tokens, *dws

    return jax.shard_map(device_fn, mesh=mesh, in_specs=in_specs, out_specs=out_specs, check_vma=False)
```
